32 devices in a mesh: pod: 2 (over x), data: 4 (over z), model: 4 (over y, core).
Axes of the slice: x: 2, y: 2, z: 4, core: 2. Of those that a mesh axis runs over, the one named last changes fastest.
Arguments:
- x_in: bfloat16 [8, 1024, 2048], P(('pod', 'data'), 'model'), parts along dimension 0
- dy_in: bfloat16 [8, 1024, 2048], P(('pod', 'data'), 'model'), parts along dimension 0
- w_q: bfloat16 [2048, 16, 128], P(None, 'model')
- w_k: bfloat16 [2, 2048, 128], replicated
- w_v: bfloat16 [2, 2048, 128], replicated
- w_o: bfloat16 [16, 128, 2048], P('model')
Outputs:
- output 1: bfloat16 [8, 1024, 2048], P(('pod', 'data'), 'model'), parts along dimension 0
- output 2: float32 [4096, 16, 128], P(('pod', 'data'), 'model'), parts along dimension 0
- output 3: float32 [8192, 128], P(('pod', 'model', 'data')), parts along dimension 0
- output 4: float32 [8192, 128], P(('pod', 'model', 'data')), parts along dimension 0
- output 5: float32 [32, 128, 2048], P(('pod', 'model'), None, 'data'), parts along dimension 0
There are 2 independent parts. The reference program is written for one: setup_inputs(seed, part) draws one part's arguments, and reference() takes and returns one part's arrays. A program takes and returns all parts, laid end to end along the dimension named above; an argument that names none is the same for every part.
All inputs are finite; a program needn't handle non-finite values.
Results may differ from the reference program's by a relative error of at most 0.00935703.
Values are sent between devices in bfloat16 or wider.
A program may use at most 1 GiB of HBM per device.

```python
import jax
import jax.numpy as jnp
from jax import lax

NUM_SEQS = 4
SEQ_LEN = 1024
MODEL_DIM = 2048
Q_HEADS = 16
KV_HEADS = 2
HEAD_DIM = 128

GROUP_HEADS = Q_HEADS // KV_HEADS


def setup_inputs(seed: int = 0, part: int = 0) -> dict:
    shared_key = jax.random.key(seed)
    part_key = jax.random.fold_in(jax.random.key(seed + 1), part)
    key_x, key_dy = jax.random.split(part_key, 2)
    key_wq, key_wk, key_wv, key_wo = jax.random.split(shared_key, 4)
    act_shape = (NUM_SEQS, SEQ_LEN, MODEL_DIM)
    in_scale = MODEL_DIM ** -0.5
    out_scale = (Q_HEADS * HEAD_DIM) ** -0.5
    x_in = jax.random.normal(key_x, act_shape, jnp.float32)
    dy_in = jax.random.normal(key_dy, act_shape, jnp.float32)
    w_q = jax.random.normal(key_wq, (MODEL_DIM, Q_HEADS, HEAD_DIM), jnp.float32) * in_scale
    w_k = jax.random.normal(key_wk, (KV_HEADS, MODEL_DIM, HEAD_DIM), jnp.float32) * in_scale
    w_v = jax.random.normal(key_wv, (KV_HEADS, MODEL_DIM, HEAD_DIM), jnp.float32) * in_scale
    w_o = jax.random.normal(key_wo, (Q_HEADS, HEAD_DIM, MODEL_DIM), jnp.float32) * out_scale
    return {'x_in': x_in.astype(jnp.bfloat16), 'dy_in': dy_in.astype(jnp.bfloat16),
            'w_q': w_q.astype(jnp.bfloat16), 'w_k': w_k.astype(jnp.bfloat16),
            'w_v': w_v.astype(jnp.bfloat16), 'w_o': w_o.astype(jnp.bfloat16)}


def group_attention(operands):
    q_grp, k_one, v_one, dout_grp = operands
    score_scale = HEAD_DIM ** -0.5
    q_f32 = q_grp.astype(jnp.float32)
    k_f32 = k_one.astype(jnp.float32)
    v_f32 = v_one.astype(jnp.float32)
    dout_f32 = dout_grp.astype(jnp.float32)
    positions = jnp.arange(SEQ_LEN)
    causal = positions[:, None] >= positions[None, :]
    scores = jnp.einsum('qhe,ke->hqk', q_f32, k_f32) * score_scale
    attn_prob = jax.nn.softmax(jnp.where(causal, scores, -jnp.inf), axis=-1)
    prob_bf = attn_prob.astype(jnp.bfloat16).astype(jnp.float32)
    attn_out = jnp.einsum('hqk,ke->qhe', prob_bf, v_f32).astype(jnp.bfloat16)
    grad_prob = jnp.einsum('qhe,ke->hqk', dout_f32, v_f32)
    row_delta = jnp.einsum('qhe,qhe->hq', dout_f32, attn_out.astype(jnp.float32))
    grad_score = (attn_prob * (grad_prob - row_delta[:, :, None])).astype(jnp.bfloat16).astype(jnp.float32)
    grad_q = (jnp.einsum('hqk,ke->qhe', grad_score, k_f32) * score_scale).astype(jnp.bfloat16)
    grad_k = (jnp.einsum('hqk,qhe->ke', grad_score, q_f32) * score_scale).astype(jnp.bfloat16)
    grad_v = jnp.einsum('hqk,qhe->ke', prob_bf, dout_f32).astype(jnp.bfloat16)
    return attn_out, grad_q, grad_k, grad_v


def heads_to_items(per_head):
    return per_head.reshape(NUM_SEQS, SEQ_LEN, KV_HEADS, GROUP_HEADS, HEAD_DIM).transpose(0, 2, 1, 3, 4).reshape(NUM_SEQS * KV_HEADS, SEQ_LEN, GROUP_HEADS, HEAD_DIM)


def items_to_heads(per_item):
    return per_item.reshape(NUM_SEQS, KV_HEADS, SEQ_LEN, GROUP_HEADS, HEAD_DIM).transpose(0, 2, 1, 3, 4).reshape(NUM_SEQS, SEQ_LEN, Q_HEADS, HEAD_DIM)


def reference(x_in, dy_in, w_q, w_k, w_v, w_o):
    x_f32 = x_in.astype(jnp.float32)
    dy_f32 = dy_in.astype(jnp.float32)
    wq_f32 = w_q.astype(jnp.float32)
    wk_f32 = w_k.astype(jnp.float32)
    wv_f32 = w_v.astype(jnp.float32)
    wo_f32 = w_o.astype(jnp.float32)
    q_proj = jnp.einsum('std,dhe->sthe', x_f32, wq_f32).astype(jnp.bfloat16)
    k_proj = jnp.einsum('std,jde->sjte', x_f32, wk_f32).astype(jnp.bfloat16)
    v_proj = jnp.einsum('std,jde->sjte', x_f32, wv_f32).astype(jnp.bfloat16)
    dout_proj = jnp.einsum('std,hed->sthe', dy_f32, wo_f32).astype(jnp.bfloat16)
    item_count = NUM_SEQS * KV_HEADS
    attn_out, grad_q, grad_k, grad_v = lax.map(group_attention, (
        heads_to_items(q_proj), k_proj.reshape(item_count, SEQ_LEN, HEAD_DIM),
        v_proj.reshape(item_count, SEQ_LEN, HEAD_DIM), heads_to_items(dout_proj)))
    out_f32 = items_to_heads(attn_out).astype(jnp.float32)
    gq_f32 = items_to_heads(grad_q).astype(jnp.float32)
    gk_f32 = grad_k.reshape(NUM_SEQS, KV_HEADS, SEQ_LEN, HEAD_DIM).astype(jnp.float32)
    gv_f32 = grad_v.reshape(NUM_SEQS, KV_HEADS, SEQ_LEN, HEAD_DIM).astype(jnp.float32)
    dw_q = jnp.einsum('std,sthe->dhe', x_f32, gq_f32)
    dw_k = jnp.einsum('std,sjte->jde', x_f32, gk_f32).reshape(KV_HEADS * MODEL_DIM, HEAD_DIM)
    dw_v = jnp.einsum('std,sjte->jde', x_f32, gv_f32).reshape(KV_HEADS * MODEL_DIM, HEAD_DIM)
    dw_o = jnp.einsum('sthe,std->hed', out_f32, dy_f32)
    dx_f32 = (jnp.einsum('sthe,dhe->std', gq_f32, wq_f32)
              + jnp.einsum('sjte,jde->std', gk_f32, wk_f32)
              + jnp.einsum('sjte,jde->std', gv_f32, wv_f32))
    return dx_f32.astype(jnp.bfloat16), dw_q, dw_k, dw_v, dw_o
```

```python
import functools
import math

import jax
import jax.numpy as jnp
from jax import lax
from jax.experimental import pallas as pl
from jax.experimental.pallas import tpu as pltpu
from jax.sharding import PartitionSpec as P

MESH = pl.DeviceIdType.MESH
F32 = jnp.float32
BF16 = jnp.bfloat16

SEQ = 1024
BLK = 256
DIM = 2048
HD = 128
NH = 4
HE = NH * HD
QKV = HE + 2 * HD
CH = 512
KC = 256
NX = 2
XR = BLK // NX
NB = SEQ // BLK
CAUSAL_ROWS = BLK * NB * (NB + 1) // 2

S_XY, S_XF, S_XC = 0, 2, 4
S_DY, S_DF, S_DC = 5, 9, 13
S_WO, S_WQ = 14, 26
S_KV = 38
S_KP = 41
S_PX = 42
S_PY = 44
N_SEM = 46


def nn(a, b):
    return lax.dot_general(a, b, (((1,), (0,)), ((), ())), preferred_element_type=F32)


def nt(a, b):
    return lax.dot_general(a, b, (((1,), (1,)), ((), ())), preferred_element_type=F32)


def step_kernel(x_in, dy_in, wq_in, wk_in, wv_in, wo_in, dx_out, dwq_out, dwkv_out, dwo_out,
                xg, dyg, wqkv, wo, qkv, kt, vt, prob, pbuf, ot, dout, at, am, dkv, pw, pq, pkv,
                kvs, kvr, sring, rring, skv, rkv, sx, rx, sy, ry, pxo, pxm, dxo, ssem, rsem, lsem):
    pod = lax.axis_index("pod")
    z = lax.axis_index("data")
    m = lax.axis_index("model")
    y = m // 2
    c = m % 2
    core_m = 2 * y + 1 - c
    far_m = (m + 2) % 4
    diag_m = (core_m + 2) % 4
    core_dev = (pod, z, core_m)
    far_dev = (pod, z, far_m)
    right_dev = (pod, (z + 1) % 4, m)
    left_dev = (pod, (z + 3) % 4, m)

    def rows(block, n=BLK, off=0):
        return pl.ds(pl.multiple_of(block * BLK + off, n), n)

    def col(i):
        return pl.ds(pl.multiple_of(((z + 3 - i) % 4) * CH, CH), CH)

    def remote(src, dst, sem, dev):
        return pltpu.make_async_remote_copy(src_ref=src, dst_ref=dst, send_sem=ssem.at[sem], recv_sem=rsem.at[sem],
                                            device_id=dev, device_id_type=MESH)

    def head_rows(h):
        return pl.ds(pl.multiple_of(h * HD, HD), HD)

    loads = [
        pltpu.make_async_copy(x_in.at[0], xg.at[rows(m)], lsem.at[0]),
        pltpu.make_async_copy(dy_in.at[0], dyg.at[rows(m)], lsem.at[1]),
        pltpu.make_async_copy(wk_in.at[y], wqkv.at[:, pl.ds(HE, HD)], lsem.at[2]),
        pltpu.make_async_copy(wv_in.at[y], wqkv.at[:, pl.ds(HE + HD, HD)], lsem.at[3]),
        pltpu.make_async_copy(wq_in, wqkv.at[:, pl.ds(0, HE)], lsem.at[4]),
        pltpu.make_async_copy(wo_in, wo, lsem.at[5]),
    ]
    for ld in loads:
        ld.start()

    barrier = pltpu.get_barrier_semaphore()
    for dev in (far_dev, core_dev, right_dev, left_dev):
        pl.semaphore_signal(barrier, inc=1, device_id=dev, device_id_type=MESH)
    pl.semaphore_wait(barrier, 4)

    def x_far(i, block):
        r = rows(block, XR, i * XR)
        return remote(xg.at[r], xg.at[r], S_XY + i, far_dev)

    def x_fwd(i, block):
        r = rows(block, XR, i * XR)
        return remote(xg.at[r], xg.at[r], S_XF + i, core_dev)

    def x_core(block):
        return remote(xg.at[rows(block)], xg.at[rows(block)], S_XC, core_dev)

    def dy_far(i, block):
        return remote(dyg.at[rows(block), col(i)], dyg.at[rows(block), col(i)], S_DY + i, far_dev)

    def dy_fwd(i, block):
        return remote(dyg.at[rows(block), col(i)], dyg.at[rows(block), col(i)], S_DF + i, core_dev)

    def dy_core(block):
        return remote(dyg.at[rows(block)], dyg.at[rows(block)], S_DC, core_dev)

    loads[0].wait()
    for i in range(NX):
        x_far(i, m).start()
    x_core(m).start()
    loads[1].wait()
    for i in range(4):
        dy_far(i, m).start()
    dy_core(m).start()
    for ld in loads[2:]:
        ld.wait()

    def project(r):
        qkv[r, :] = nn(xg[r, :], wqkv[...]).astype(BF16)

    project(rows(m))
    x_core(core_m).wait_recv()
    project(rows(core_m))

    def x_piece(i, carry):
        x_far(i, far_m).wait_recv()
        x_fwd(i, far_m).start()
        project(rows(far_m, XR, i * XR))
        x_fwd(i, diag_m).wait_recv()
        project(rows(diag_m, XR, i * XR))
        return carry

    lax.fori_loop(0, NX, x_piece, 0)

    kt[...] = qkv[:, pl.ds(HE, HD)].T
    vt[...] = qkv[:, pl.ds(HE + HD, HD)].T
    dy_core(core_m).wait_recv()

    def take_dy(i):
        dy_far(i, far_m).wait_recv()
        dy_fwd(i, far_m).start()

    def ring_copy(base, which, hop, h):
        return remote(sring.at[which, hop, h], rring.at[which, hop, h], base + hop * 4 + h, right_dev)

    scale = HD ** -0.5
    exp_scale = scale * math.log2(math.e)
    diag_mask = lax.broadcasted_iota(jnp.int32, (BLK, BLK), 0) <= lax.broadcasted_iota(jnp.int32, (BLK, BLK), 1)

    def prow(qi, kj):
        return pl.ds(BLK * (qi * (qi + 1) // 2 + kj), BLK)

    def fwd_head(h, carry):
        hr = head_rows(h)
        for qi in range(NB):
            qb = qkv[pl.ds(qi * BLK, BLK), hr]
            mx = None
            for kj in range(qi + 1):
                s = nt(qkv[pl.ds(kj * BLK, BLK), pl.ds(HE, HD)], qb)
                if kj == qi:
                    s = jnp.where(diag_mask, s, -jnp.inf)
                prob[h, prow(qi, kj), :] = s
                bm = jnp.max(s, axis=0, keepdims=True)
                mx = bm if mx is None else jnp.maximum(mx, bm)
            tot = None
            for kj in range(qi + 1):
                e = jnp.exp2((prob[h, prow(qi, kj), :] - mx) * exp_scale)
                prob[h, prow(qi, kj), :] = e
                bs = jnp.sum(e, axis=0, keepdims=True)
                tot = bs if tot is None else tot + bs
            inv = 1.0 / tot
            for kj in range(qi + 1):
                p = prob[h, prow(qi, kj), :] * inv
                prob[h, prow(qi, kj), :] = p
                pbuf[pl.ds(kj * BLK, BLK), :] = p.astype(BF16)
            n = (qi + 1) * BLK
            ot[hr, pl.ds(qi * BLK, BLK)] = nn(vt[:, pl.ds(0, n)], pbuf[pl.ds(0, n), :]).astype(BF16)

        @pl.when(h == 0)
        def _():
            take_dy(0)
            dy_fwd(0, diag_m).wait_recv()

        sring[0, 0, h] = nn(ot[hr, :], dyg[:, col(0)]).astype(BF16)
        ring_copy(S_WO, 0, 0, h).start()
        return carry

    lax.fori_loop(0, NH, fwd_head, 0)

    def ring_service(base, which, own, hop, h):
        ring_copy(base, which, hop - 1, h).wait_recv()
        total = own[hop - 1, head_rows(h), :] + rring[which, hop - 1, h].astype(F32)
        sring[which, hop, h] = total.astype(BF16)
        ring_copy(base, which, hop, h).start()

    def ring_final(base, which, own, h):
        ring_copy(base, which, 2, h).wait_recv()
        own[2, head_rows(h), :] = own[2, head_rows(h), :] + rring[which, 2, h].astype(F32)

    def wo_own(i):
        pw[i - 1] = nn(ot[...], dyg[:, col(i)])

    def wq_own(i):
        pq[i - 1] = nn(at[pl.ds(0, HE), :], xg[:, col(i)])

    for i in range(1, 4):
        take_dy(i)
        dy_fwd(i, diag_m).wait_recv()
        wo_own(i)
        if i < 3:
            for h in range(2):
                ring_service(S_WO, 0, pw, 1, 2 * (i - 1) + h)

    def dout_block(b, carry):
        r = rows(b)
        dout[r, :] = nt(dyg[r, :], wo[...]).astype(BF16)
        return carry

    lax.fori_loop(0, NB, dout_block, 0)
    for h in range(2):
        ring_service(S_WO, 0, pw, 2, h)

    dkv[...] = jnp.zeros_like(dkv)

    def bwd_head(h, carry):
        hr = head_rows(h)
        for qi in range(NB):
            qr = pl.ds(qi * BLK, BLK)
            dob = dout[qr, hr]
            qb = qkv[qr, hr]
            delta = jnp.sum(dob.astype(F32).T * ot[hr, qr].astype(F32), axis=0, keepdims=True)
            for kj in range(qi + 1):
                kr = pl.ds(kj * BLK, BLK)
                p = prob[h, prow(qi, kj), :]
                dp = nt(qkv[kr, pl.ds(HE + HD, HD)], dob)
                ds = (p * (dp - delta)).astype(BF16)
                pbuf[kr, :] = ds
                dkv[kr, pl.ds(0, HD)] += nn(ds, qb)
                dkv[kr, pl.ds(HD, HD)] += nn(p.astype(BF16), dob)
            n = (qi + 1) * BLK
            dq = (nn(kt[:, pl.ds(0, n)], pbuf[pl.ds(0, n), :]) * scale).astype(BF16)
            at[hr, qr] = dq
            am[qr, hr] = dq.T

        @pl.when(h < 2)
        def _():
            ring_service(S_WO, 0, pw, 2, h + 2)

        sring[1, 0, h] = nn(at[hr, :], xg[:, col(0)]).astype(BF16)
        ring_copy(S_WQ, 1, 0, h).start()
        return carry

    lax.fori_loop(0, NH, bwd_head, 0)

    dkb = (dkv[:, pl.ds(0, HD)] * scale).astype(BF16)
    dvb = dkv[:, pl.ds(HD, HD)].astype(BF16)
    am[:, pl.ds(HE, HD)] = dkb
    am[:, pl.ds(HE + HD, HD)] = dvb
    at[pl.ds(HE, HD), :] = dkb.T
    at[pl.ds(HE + HD, HD), :] = dvb.T

    def dx_part(block, put):
        def piece(i, carry):
            cs = pl.ds(pl.multiple_of(i * CH, CH), CH)
            put(cs, nt(am[rows(block), :], wqkv[cs, :]))
            return carry

        lax.fori_loop(0, DIM // CH, piece, 0)

    def px_copy(i):
        return remote(sx.at[i], rx.at[i], S_PX + i, core_dev)

    def py_copy(i):
        r = pl.ds(i * (BLK // 2), BLK // 2)
        return remote(sy.at[r], ry.at[r], S_PY + i, far_dev)

    def put_sx(i):
        def put(cs, v):
            sx[i, :, cs] = v.astype(BF16)
        return put

    def put_ref(ref):
        def put(cs, v):
            ref[:, cs] = v
        return put

    dx_part(diag_m, put_sx(0))
    px_copy(0).start()
    dx_part(far_m, put_ref(pxm))
    px_copy(0).wait_recv()
    for i in range(2):
        r = pl.ds(i * (BLK // 2), BLK // 2)
        sy[r, :] = (pxm[r, :] + rx[0, r, :].astype(F32)).astype(BF16)
        py_copy(i).start()

    wq_own(1)
    for h in range(2):
        ring_service(S_WQ, 1, pq, 1, h)

    atk = at[pl.ds(HE, 2 * HD), :]
    half = DIM // 2
    kvs[...] = nn(atk, xg[:, pl.ds(pl.multiple_of((1 - c) * half, half), half)]).astype(BF16)
    kp_copy = remote(kvs, kvr, S_KP, core_dev)
    kp_copy.start()
    for h in range(2, 4):
        ring_service(S_WQ, 1, pq, 1, h)
    pkv[...] = nn(atk, xg[:, pl.ds(pl.multiple_of(c * half, half), half)])
    kp_copy.wait_recv()
    pkv[...] += kvr[...].astype(F32)

    def kcol(i):
        return pl.ds(pl.multiple_of(((z + 3 - i) % 4) * KC, KC), KC)

    def kv_copy(hop):
        return remote(skv.at[hop], rkv.at[hop], S_KV + hop, right_dev)

    skv[0] = pkv[:, kcol(0)].astype(BF16)
    kv_copy(0).start()

    wq_own(2)
    for h in range(2):
        ring_service(S_WQ, 1, pq, 2, h)
    dx_part(core_m, put_sx(1))
    px_copy(1).start()
    for h in range(2, 4):
        ring_service(S_WQ, 1, pq, 2, h)

    def kv_service(hop):
        kv_copy(hop - 1).wait_recv()
        skv[hop] = (pkv[:, kcol(hop)] + rkv[hop - 1].astype(F32)).astype(BF16)
        kv_copy(hop).start()

    kv_service(1)
    wq_own(3)
    dx_part(m, put_ref(pxo))
    px_copy(1).wait_recv()
    pxo[...] += rx[1].astype(F32)

    def wo_fin(h, carry):
        ring_final(S_WO, 0, pw, h)
        return carry

    lax.fori_loop(0, NH, wo_fin, 0)
    out_wo = pltpu.make_async_copy(pw.at[2], dwo_out, lsem.at[0])
    out_wo.start()
    kv_service(2)
    for i in range(2):
        r = pl.ds(i * (BLK // 2), BLK // 2)
        py_copy(i).wait_recv()
        dxo[r, :] = (pxo[r, :] + ry[r, :].astype(F32)).astype(BF16)
    out_dx = pltpu.make_async_copy(dxo, dx_out.at[0], lsem.at[1])
    out_dx.start()

    def wq_fin(h, carry):
        ring_final(S_WQ, 1, pq, h)
        return carry

    lax.fori_loop(0, NH, wq_fin, 0)
    out_wq = pltpu.make_async_copy(pq.at[2], dwq_out, lsem.at[2])
    out_wq.start()
    kv_copy(2).wait_recv()
    pkv[:, pl.ds(0, KC)] = pkv[:, kcol(3)] + rkv[2].astype(F32)
    out_kv = pltpu.make_async_copy(pkv.at[:, pl.ds(0, KC)], dwkv_out, lsem.at[3])
    out_kv.start()

    for i in range(NX):
        x_far(i, m).wait_send()
        x_fwd(i, far_m).wait_send()
    x_core(m).wait_send()
    for i in range(4):
        dy_far(i, m).wait_send()
        dy_fwd(i, far_m).wait_send()
    dy_core(m).wait_send()
    for base, which in ((S_WO, 0), (S_WQ, 1)):
        for hop in range(3):
            for h in range(NH):
                ring_copy(base, which, hop, h).wait_send()
    for hop in range(3):
        kv_copy(hop).wait_send()
    kp_copy.wait_send()
    for i in range(2):
        px_copy(i).wait_send()
        py_copy(i).wait_send()
    for cp in (out_wo, out_dx, out_wq, out_kv):
        cp.wait()


def solution(mesh):
    tok_spec = P(('pod', 'data'), 'model', None)

    def device_step(x_loc, dy_loc, w_q, w_k, w_v, w_o):
        any_spec = pl.BlockSpec(memory_space=pl.ANY)
        dx, dwq_t, dwkv_t, dwo = pl.pallas_call(
            step_kernel,
            out_shape=(jax.ShapeDtypeStruct((1, BLK, DIM), BF16), jax.ShapeDtypeStruct((HE, CH), F32),
                       jax.ShapeDtypeStruct((2 * HD, KC), F32), jax.ShapeDtypeStruct((HE, CH), F32)),
            in_specs=[any_spec] * 6,
            out_specs=[any_spec] * 4,
            scratch_shapes=[
                pltpu.VMEM((SEQ, DIM), BF16),
                pltpu.VMEM((SEQ, DIM), BF16),
                pltpu.VMEM((DIM, QKV), BF16),
                pltpu.VMEM((HE, DIM), BF16),
                pltpu.VMEM((SEQ, QKV), BF16),
                pltpu.VMEM((HD, SEQ), BF16),
                pltpu.VMEM((HD, SEQ), BF16),
                pltpu.VMEM((NH, CAUSAL_ROWS, BLK), F32),
                pltpu.VMEM((SEQ, BLK), BF16),
                pltpu.VMEM((HE, SEQ), BF16),
                pltpu.VMEM((SEQ, HE), BF16),
                pltpu.VMEM((QKV, SEQ), BF16),
                pltpu.VMEM((SEQ, QKV), BF16),
                pltpu.VMEM((SEQ, 2 * HD), F32),
                pltpu.VMEM((3, HE, CH), F32),
                pltpu.VMEM((3, HE, CH), F32),
                pltpu.VMEM((2 * HD, DIM // 2), F32),
                pltpu.VMEM((2 * HD, DIM // 2), BF16),
                pltpu.VMEM((2 * HD, DIM // 2), BF16),
                pltpu.VMEM((2, 3, NH, HD, CH), BF16),
                pltpu.VMEM((2, 3, NH, HD, CH), BF16),
                pltpu.VMEM((3, 2 * HD, KC), BF16),
                pltpu.VMEM((3, 2 * HD, KC), BF16),
                pltpu.VMEM((2, BLK, DIM), BF16),
                pltpu.VMEM((2, BLK, DIM), BF16),
                pltpu.VMEM((BLK, DIM), BF16),
                pltpu.VMEM((BLK, DIM), BF16),
                pltpu.VMEM((BLK, DIM), F32),
                pltpu.VMEM((BLK, DIM), F32),
                pltpu.VMEM((BLK, DIM), BF16),
                pltpu.SemaphoreType.DMA((N_SEM,)),
                pltpu.SemaphoreType.DMA((N_SEM,)),
                pltpu.SemaphoreType.DMA((6,)),
            ],
            compiler_params=pltpu.CompilerParams(collective_id=0, has_side_effects=True, vmem_limit_bytes=67043328),
        )(x_loc, dy_loc, w_q.reshape(DIM, HE), w_k, w_v, w_o.reshape(HE, DIM))
        dwq = dwq_t.T.reshape(CH, NH, HD)
        dwk = dwkv_t[:HD].T
        dwv = dwkv_t[HD:].T
        return dx, dwq, dwk, dwv, dwo.reshape(NH, HD, CH)

    kv_rows = P(('pod', 'model', 'data'), None)
    return jax.shard_map(device_step, mesh=mesh,
                         in_specs=(tok_spec, tok_spec, P(None, 'model', None), P(), P(), P('model', None, None)),
                         out_specs=(tok_spec, P(('pod', 'data'), 'model', None), kv_rows, kv_rows, P(('pod', 'model'), None, 'data')),
                         check_vma=False)
```

```python
import functools
import math

import jax
import jax.numpy as jnp
from jax import lax
from jax.experimental import pallas as pl
from jax.experimental.pallas import tpu as pltpu
from jax.sharding import PartitionSpec as P

MESH = pl.DeviceIdType.MESH
F32 = jnp.float32
BF16 = jnp.bfloat16

SEQ = 1024
BLK = 256
DIM = 2048
HD = 128
NH = 4
HE = NH * HD
QKV = HE + 2 * HD
CH = 512
SC = CH // 2
WR = 1024
KC = 256
NX = 4
XR = BLK // NX
NB = SEQ // BLK
CAUSAL_ROWS = BLK * NB * (NB + 1) // 2

S_XY, S_XF, S_XC = 0, 4, 8
S_DY, S_DF, S_DC = 9, 14, 19
S_WO, S_WQ = 20, 44
S_KV = 68
S_KP = 71
S_PX = 72
S_PY = 74
N_SEM = 76


def nn(a, b):
    return lax.dot_general(a, b, (((1,), (0,)), ((), ())), preferred_element_type=F32)


def nt(a, b):
    return lax.dot_general(a, b, (((1,), (1,)), ((), ())), preferred_element_type=F32)


def step_kernel(x_in, dy_in, wq_in, wk_in, wv_in, wo_in, dx_out, dwq_out, dwk_out, dwv_out, dwo_out,
                xg, dyg, wq8, wst, wqkv, wo, qkv, kt, vt, prob, pbuf, ot, dout, at, am, dkv, pw, pq, pkv,
                kvs, kvr, sring, rring, skv, rkv, sx, rx, sy, ry, pxo, dxo, wqo, kvo, ssem, rsem, lsem):
    pod = lax.axis_index("pod")
    z = lax.axis_index("data")
    m = lax.axis_index("model")
    y = m // 2
    c = m % 2
    core_m = 2 * y + 1 - c
    far_m = (m + 2) % 4
    diag_m = (core_m + 2) % 4
    core_dev = (pod, z, core_m)
    far_dev = (pod, z, far_m)
    right_dev = (pod, (z + 1) % 4, m)
    left_dev = (pod, (z + 3) % 4, m)

    def rows(block, n=BLK, off=0):
        return pl.ds(pl.multiple_of(block * BLK + off, n), n)

    def col(i):
        return pl.ds(pl.multiple_of(((z + 3 - i) % 4) * CH, CH), CH)

    def dcol(i):
        if i < 2:
            return pl.ds(pl.multiple_of(((z + 3) % 4) * CH + i * SC, SC), SC)
        return col(i - 1)

    def remote(src, dst, sem, dev):
        return pltpu.make_async_remote_copy(src_ref=src, dst_ref=dst, send_sem=ssem.at[sem], recv_sem=rsem.at[sem],
                                            device_id=dev, device_id_type=MESH)

    def head_rows(h):
        return pl.ds(pl.multiple_of(h * HD, HD), HD)

    loads = [
        pltpu.make_async_copy(x_in.at[0], xg.at[rows(m)], lsem.at[0]),
        pltpu.make_async_copy(dy_in.at[0], dyg.at[rows(m)], lsem.at[1]),
        pltpu.make_async_copy(wk_in.at[y], wqkv.at[:, pl.ds(HE, HD)], lsem.at[2]),
        pltpu.make_async_copy(wv_in.at[y], wqkv.at[:, pl.ds(HE + HD, HD)], lsem.at[3]),
        pltpu.make_async_copy(wq_in, wq8, lsem.at[4]),
        pltpu.make_async_copy(wo_in, wo, lsem.at[5]),
    ]
    for ld in loads:
        ld.start()

    barrier = pltpu.get_barrier_semaphore()
    for dev in (far_dev, core_dev, right_dev, left_dev):
        pl.semaphore_signal(barrier, inc=1, device_id=dev, device_id_type=MESH)
    pl.semaphore_wait(barrier, 4)

    def x_far(i, block):
        r = rows(block, XR, i * XR)
        return remote(xg.at[r], xg.at[r], S_XY + i, far_dev)

    def x_fwd(i, block):
        r = rows(block, XR, i * XR)
        return remote(xg.at[r], xg.at[r], S_XF + i, core_dev)

    def x_core(block):
        return remote(xg.at[rows(block)], xg.at[rows(block)], S_XC, core_dev)

    def dy_far(i, block):
        return remote(dyg.at[rows(block), dcol(i)], dyg.at[rows(block), dcol(i)], S_DY + i, far_dev)

    def dy_fwd(i, block):
        return remote(dyg.at[rows(block), dcol(i)], dyg.at[rows(block), dcol(i)], S_DF + i, core_dev)

    def dy_core(block):
        return remote(dyg.at[rows(block)], dyg.at[rows(block)], S_DC, core_dev)

    loads[0].wait()
    for i in range(NX):
        x_far(i, m).start()
    x_core(m).start()
    loads[1].wait()
    for i in range(5):
        dy_far(i, m).start()
    dy_core(m).start()
    for ld in loads[2:]:
        ld.wait()

    def wq_block(i, carry):
        wst[...] = wq8[pl.ds(pl.multiple_of(i * WR, WR), WR), :].astype(F32)
        for h in range(NH):
            wqkv[pl.ds(pl.multiple_of(i * (WR // NH), WR // NH), WR // NH), pl.ds(h * HD, HD)] = wst[pl.ds(h, WR // NH, stride=NH), :].astype(BF16)
        return carry

    lax.fori_loop(0, DIM * NH // WR, wq_block, 0)

    def project(r):
        qkv[r, :] = nn(xg[r, :], wqkv[...]).astype(BF16)

    def flip(block):
        r = rows(block)
        kt[:, r] = qkv[r, pl.ds(HE, HD)].T
        vt[:, r] = qkv[r, pl.ds(HE + HD, HD)].T

    project(rows(m))
    x_core(core_m).wait_recv()
    project(rows(core_m))
    flip(m)
    flip(core_m)

    def x_piece(i, carry):
        x_far(i, far_m).wait_recv()
        x_fwd(i, far_m).start()
        project(rows(far_m, XR, i * XR))
        x_fwd(i, diag_m).wait_recv()
        project(rows(diag_m, XR, i * XR))
        return carry

    lax.fori_loop(0, NX, x_piece, 0)

    flip(far_m)
    flip(diag_m)
    dy_core(core_m).wait_recv()

    def take_dy(i):
        dy_far(i, far_m).wait_recv()
        dy_fwd(i, far_m).start()

    def ring_copy(base, which, hop, s, h):
        return remote(sring.at[which, hop, s, h], rring.at[which, hop, s, h], base + hop * 8 + s * 4 + h, right_dev)

    def half_col(s):
        return pl.ds(s * SC, SC)

    def wo_first(s, h):
        sring[0, 0, s, h] = nn(ot[head_rows(h), :], dyg[:, dcol(s)]).astype(BF16)
        ring_copy(S_WO, 0, 0, s, h).start()

    scale = HD ** -0.5
    exp_scale = scale * math.log2(math.e)
    diag_mask = lax.broadcasted_iota(jnp.int32, (BLK, BLK), 0) <= lax.broadcasted_iota(jnp.int32, (BLK, BLK), 1)

    def prow(qi, kj):
        return pl.ds(BLK * (qi * (qi + 1) // 2 + kj), BLK)

    def fwd_head(h, carry):
        hr = head_rows(h)
        for qi in range(NB):
            qb = qkv[pl.ds(qi * BLK, BLK), hr]
            mx = None
            for kj in range(qi + 1):
                s = nt(qkv[pl.ds(kj * BLK, BLK), pl.ds(HE, HD)], qb)
                if kj == qi:
                    s = jnp.where(diag_mask, s, -jnp.inf)
                prob[h, prow(qi, kj), :] = s
                bm = jnp.max(s, axis=0, keepdims=True)
                mx = bm if mx is None else jnp.maximum(mx, bm)
            tot = None
            for kj in range(qi + 1):
                e = jnp.exp2((prob[h, prow(qi, kj), :] - mx) * exp_scale)
                prob[h, prow(qi, kj), :] = e
                bs = jnp.sum(e, axis=0, keepdims=True)
                tot = bs if tot is None else tot + bs
            inv = 1.0 / tot
            for kj in range(qi + 1):
                p = prob[h, prow(qi, kj), :] * inv
                prob[h, prow(qi, kj), :] = p
                pbuf[pl.ds(kj * BLK, BLK), :] = p.astype(BF16)
            n = (qi + 1) * BLK
            ot[hr, pl.ds(qi * BLK, BLK)] = nn(vt[:, pl.ds(0, n)], pbuf[pl.ds(0, n), :]).astype(BF16)

        @pl.when(h == 0)
        def _():
            take_dy(0)
            dy_fwd(0, diag_m).wait_recv()

        wo_first(0, h)

        @pl.when(h == 1)
        def _():
            take_dy(1)
            dy_fwd(1, diag_m).wait_recv()
            wo_first(1, 0)

        @pl.when(h >= 1)
        def _():
            wo_first(1, h)

        return carry

    lax.fori_loop(0, NH, fwd_head, 0)

    def ring_service(base, which, own, hop, h):
        for s in range(2):
            ring_copy(base, which, hop - 1, s, h).wait_recv()
            total = own[hop - 1, head_rows(h), half_col(s)] + rring[which, hop - 1, s, h].astype(F32)
            sring[which, hop, s, h] = total.astype(BF16)
            ring_copy(base, which, hop, s, h).start()

    def ring_final(base, which, own, h, s):
        ring_copy(base, which, 2, s, h).wait_recv()
        return own[2, head_rows(h), half_col(s)] + rring[which, 2, s, h].astype(F32)

    def wo_own(i):
        pw[i - 1] = nn(ot[...], dyg[:, col(i)])

    def wq_own(i):
        pq[i - 1] = nn(at[pl.ds(0, HE), :], xg[:, col(i)])

    for i in range(1, 4):
        take_dy(i + 1)
        dy_fwd(i + 1, diag_m).wait_recv()
        wo_own(i)
        if i < 3:
            for h in range(2):
                ring_service(S_WO, 0, pw, 1, 2 * (i - 1) + h)

    def dout_block(b, carry):
        r = rows(b)
        dout[r, :] = nt(dyg[r, :], wo[...]).astype(BF16)
        return carry

    lax.fori_loop(0, NB, dout_block, 0)
    for h in range(2):
        ring_service(S_WO, 0, pw, 2, h)

    dkv[...] = jnp.zeros_like(dkv)

    def bwd_head(h, carry):
        hr = head_rows(h)
        for qi in range(NB):
            qr = pl.ds(qi * BLK, BLK)
            dob = dout[qr, hr]
            qb = qkv[qr, hr]
            delta = jnp.sum(dob.astype(F32).T * ot[hr, qr].astype(F32), axis=0, keepdims=True)
            for kj in range(qi + 1):
                kr = pl.ds(kj * BLK, BLK)
                p = prob[h, prow(qi, kj), :]
                dp = nt(qkv[kr, pl.ds(HE + HD, HD)], dob)
                ds = (p * (dp - delta)).astype(BF16)
                pbuf[kr, :] = ds
                dkv[kr, pl.ds(0, HD)] += nn(ds, qb)
                dkv[kr, pl.ds(HD, HD)] += nn(p.astype(BF16), dob)
            n = (qi + 1) * BLK
            dq = (nn(kt[:, pl.ds(0, n)], pbuf[pl.ds(0, n), :]) * scale).astype(BF16)
            at[hr, qr] = dq
            am[qr, hr] = dq.T

        @pl.when(h < 2)
        def _():
            ring_service(S_WO, 0, pw, 2, h + 2)

        first = nn(at[hr, :], xg[:, col(0)]).astype(BF16)
        for s in range(2):
            sring[1, 0, s, h] = first[:, s * SC:(s + 1) * SC]
            ring_copy(S_WQ, 1, 0, s, h).start()
        return carry

    lax.fori_loop(0, NH, bwd_head, 0)

    dkb = (dkv[:, pl.ds(0, HD)] * scale).astype(BF16)
    dvb = dkv[:, pl.ds(HD, HD)].astype(BF16)
    am[:, pl.ds(HE, HD)] = dkb
    am[:, pl.ds(HE + HD, HD)] = dvb
    at[pl.ds(HE, HD), :] = dkb.T
    at[pl.ds(HE + HD, HD), :] = dvb.T

    def dx_part(block, put):
        def piece(i, carry):
            cs = pl.ds(pl.multiple_of(i * CH, CH), CH)
            put(cs, nt(am[rows(block), :], wqkv[cs, :]))
            return carry

        lax.fori_loop(0, DIM // CH, piece, 0)

    def px_copy(i):
        return remote(sx.at[i], rx.at[i], S_PX + i, core_dev)

    def py_copy(i):
        r = pl.ds(i * (BLK // 2), BLK // 2)
        return remote(sy.at[r], ry.at[r], S_PY + i, far_dev)

    def put_sx(i):
        def put(cs, v):
            sx[i, :, cs] = v.astype(BF16)
        return put

    def put_ref(ref):
        def put(cs, v):
            ref[:, cs] = v
        return put

    half = DIM // 2

    def kv_half(which):
        return nn(at[pl.ds(HE, 2 * HD), :], xg[:, pl.ds(pl.multiple_of(which * half, half), half)])

    def kcol(i):
        return pl.ds(pl.multiple_of(((z + 3 - i) % 4) * KC, KC), KC)

    def kv_copy(hop):
        return remote(skv.at[hop], rkv.at[hop], S_KV + hop, right_dev)

    def kv_service(hop):
        kv_copy(hop - 1).wait_recv()
        skv[hop] = (pkv[:, kcol(hop)] + rkv[hop - 1].astype(F32)).astype(BF16)
        kv_copy(hop).start()

    kvs[...] = kv_half(1 - c).astype(BF16)
    kp_copy = remote(kvs, kvr, S_KP, core_dev)
    kp_copy.start()
    dx_part(diag_m, put_sx(0))
    px_copy(0).start()
    pkv[...] = kv_half(c)
    kp_copy.wait_recv()
    pkv[...] += kvr[...].astype(F32)
    skv[0] = pkv[:, kcol(0)].astype(BF16)
    kv_copy(0).start()
    dx_part(far_m, put_ref(pxo))
    px_copy(0).wait_recv()
    for i in range(2):
        r = pl.ds(i * (BLK // 2), BLK // 2)
        sy[r, :] = (pxo[r, :] + rx[0, r, :].astype(F32)).astype(BF16)
        py_copy(i).start()

    wq_own(1)
    for h in range(NH):
        ring_service(S_WQ, 1, pq, 1, h)
    kv_service(1)
    dx_part(core_m, put_sx(1))
    px_copy(1).start()
    wq_own(2)
    for h in range(2):
        ring_service(S_WQ, 1, pq, 2, h)
    kv_service(2)
    for h in range(2, NH):
        ring_service(S_WQ, 1, pq, 2, h)
    wq_own(3)
    dx_part(m, put_ref(pxo))
    px_copy(1).wait_recv()
    pxo[...] += rx[1].astype(F32)

    for h in range(NH):
        for s in range(2):
            pw[2, head_rows(h), half_col(s)] = ring_final(S_WO, 0, pw, h, s)
    out_wo = pltpu.make_async_copy(pw.at[2], dwo_out, lsem.at[0])
    out_wo.start()
    for i in range(2):
        r = pl.ds(i * (BLK // 2), BLK // 2)
        py_copy(i).wait_recv()
        dxo[r, :] = (pxo[r, :] + ry[r, :].astype(F32)).astype(BF16)
    out_dx = pltpu.make_async_copy(dxo, dx_out.at[0], lsem.at[1])
    out_dx.start()

    def wq_fin(h):
        for s in range(2):
            wqo[pl.ds(s * SC * NH + h, SC, stride=NH), :] = ring_final(S_WQ, 1, pq, h, s).T

    for h in range(2):
        wq_fin(h)
    kv_copy(2).wait_recv()
    kv_sum = pkv[:, kcol(3)] + rkv[2].astype(F32)
    kvo[0] = kv_sum[:HD].T
    kvo[1] = kv_sum[HD:].T
    out_k = pltpu.make_async_copy(kvo.at[0], dwk_out, lsem.at[3])
    out_k.start()
    out_v = pltpu.make_async_copy(kvo.at[1], dwv_out, lsem.at[4])
    out_v.start()
    for h in range(2, NH):
        wq_fin(h)
    out_wq = pltpu.make_async_copy(wqo, dwq_out, lsem.at[2])
    out_wq.start()

    for i in range(NX):
        x_far(i, m).wait_send()
        x_fwd(i, far_m).wait_send()
    x_core(m).wait_send()
    for i in range(5):
        dy_far(i, m).wait_send()
        dy_fwd(i, far_m).wait_send()
    dy_core(m).wait_send()
    for base, which in ((S_WO, 0), (S_WQ, 1)):
        for hop in range(3):
            for h in range(NH):
                for s in range(2):
                    ring_copy(base, which, hop, s, h).wait_send()
    for hop in range(3):
        kv_copy(hop).wait_send()
    kp_copy.wait_send()
    for i in range(2):
        px_copy(i).wait_send()
        py_copy(i).wait_send()
    for cp in (out_wo, out_dx, out_wq, out_k, out_v):
        cp.wait()


def solution(mesh):
    tok_spec = P(('pod', 'data'), 'model', None)

    def device_step(x_loc, dy_loc, w_q, w_k, w_v, w_o):
        any_spec = pl.BlockSpec(memory_space=pl.ANY)
        dx, dwq, dwk, dwv, dwo = pl.pallas_call(
            step_kernel,
            out_shape=(jax.ShapeDtypeStruct((1, BLK, DIM), BF16), jax.ShapeDtypeStruct((CH * NH, HD), F32),
                       jax.ShapeDtypeStruct((KC, HD), F32), jax.ShapeDtypeStruct((KC, HD), F32),
                       jax.ShapeDtypeStruct((HE, CH), F32)),
            in_specs=[any_spec] * 6,
            out_specs=[any_spec] * 5,
            scratch_shapes=[
                pltpu.VMEM((SEQ, DIM), BF16),
                pltpu.VMEM((SEQ, DIM), BF16),
                pltpu.VMEM((DIM * NH, HD), BF16),
                pltpu.VMEM((WR, HD), F32),
                pltpu.VMEM((DIM, QKV), BF16),
                pltpu.VMEM((HE, DIM), BF16),
                pltpu.VMEM((SEQ, QKV), BF16),
                pltpu.VMEM((HD, SEQ), BF16),
                pltpu.VMEM((HD, SEQ), BF16),
                pltpu.VMEM((NH, CAUSAL_ROWS, BLK), F32),
                pltpu.VMEM((SEQ, BLK), BF16),
                pltpu.VMEM((HE, SEQ), BF16),
                pltpu.VMEM((SEQ, HE), BF16),
                pltpu.VMEM((QKV, SEQ), BF16),
                pltpu.VMEM((SEQ, QKV), BF16),
                pltpu.VMEM((SEQ, 2 * HD), F32),
                pltpu.VMEM((3, HE, CH), F32),
                pltpu.VMEM((3, HE, CH), F32),
                pltpu.VMEM((2 * HD, DIM // 2), F32),
                pltpu.VMEM((2 * HD, DIM // 2), BF16),
                pltpu.VMEM((2 * HD, DIM // 2), BF16),
                pltpu.VMEM((2, 3, 2, NH, HD, SC), BF16),
                pltpu.VMEM((2, 3, 2, NH, HD, SC), BF16),
                pltpu.VMEM((3, 2 * HD, KC), BF16),
                pltpu.VMEM((3, 2 * HD, KC), BF16),
                pltpu.VMEM((2, BLK, DIM), BF16),
                pltpu.VMEM((2, BLK, DIM), BF16),
                pltpu.VMEM((BLK, DIM), BF16),
                pltpu.VMEM((BLK, DIM), BF16),
                pltpu.VMEM((BLK, DIM), F32),
                pltpu.VMEM((BLK, DIM), BF16),
                pltpu.VMEM((CH * NH, HD), F32),
                pltpu.VMEM((2, KC, HD), F32),
                pltpu.SemaphoreType.DMA((N_SEM,)),
                pltpu.SemaphoreType.DMA((N_SEM,)),
                pltpu.SemaphoreType.DMA((6,)),
            ],
            compiler_params=pltpu.CompilerParams(collective_id=0, has_side_effects=True, vmem_limit_bytes=67043328),
        )(x_loc, dy_loc, w_q.reshape(DIM * NH, HD), w_k, w_v, w_o.reshape(HE, DIM))
        return dx, dwq.reshape(CH, NH, HD), dwk, dwv, dwo.reshape(NH, HD, CH)

    kv_rows = P(('pod', 'model', 'data'), None)
    return jax.shard_map(device_step, mesh=mesh,
                         in_specs=(tok_spec, tok_spec, P(None, 'model', None), P(), P(), P('model', None, None)),
                         out_specs=(tok_spec, P(('pod', 'data'), 'model', None), kv_rows, kv_rows, P(('pod', 'model'), None, 'data')),
                         check_vma=False)
```

```python
import functools
import math

import jax
import jax.numpy as jnp
from jax import lax
from jax.experimental import pallas as pl
from jax.experimental.pallas import tpu as pltpu
from jax.sharding import PartitionSpec as P

MESH = pl.DeviceIdType.MESH
F32 = jnp.float32
BF16 = jnp.bfloat16

SEQ = 1024
BLK = 256
DIM = 2048
HD = 128
NH = 4
HE = NH * HD
QKV = HE + 2 * HD
CH = 512
SC = CH // 2
WR = 1024
KC = 256
NX = 4
XR = BLK // NX
NB = SEQ // BLK
CAUSAL_ROWS = BLK * NB * (NB + 1) // 2

S_XY, S_XF, S_XC = 0, 4, 8
S_DY, S_DF, S_DC = 9, 14, 19
S_WO, S_WQ = 20, 44
S_KV = 68
S_KP = 71
S_PX = 72
S_PY = 74
N_SEM = 76
OWN = ((0, 1, 2), (3, 0, 1))
VMEM_LIMIT = 63 * 2 ** 20 - 3328 * 1024


def nn(a, b):
    return lax.dot_general(a, b, (((1,), (0,)), ((), ())), preferred_element_type=F32)


def nt(a, b):
    return lax.dot_general(a, b, (((1,), (1,)), ((), ())), preferred_element_type=F32)


def step_kernel(x_in, dy_in, wq_in, wk_in, wv_in, wo_in, dxo, wqo, dko, dvo, woo,
                xg, dyg, wq8, wst, wqkv, wo, qkv, kt, vt, prob, pbuf, ot, dout, at, am, dkv, pw, pkv,
                kvs, kvr, sring, rring, skv, rkv, sx, rx, sy, ry, pxo, ssem, rsem, lsem):
    pod = lax.axis_index("pod")
    z = lax.axis_index("data")
    m = lax.axis_index("model")
    y = m // 2
    c = m % 2
    core_m = 2 * y + 1 - c
    far_m = (m + 2) % 4
    diag_m = (core_m + 2) % 4
    core_dev = (pod, z, core_m)
    far_dev = (pod, z, far_m)
    right_dev = (pod, (z + 1) % 4, m)
    left_dev = (pod, (z + 3) % 4, m)

    def rows(block, n=BLK, off=0):
        return pl.ds(pl.multiple_of(block * BLK + off, n), n)

    def col(i):
        return pl.ds(pl.multiple_of(((z + 3 - i) % 4) * CH, CH), CH)

    def dcol(i):
        if i < 2:
            return pl.ds(pl.multiple_of(((z + 3) % 4) * CH + i * SC, SC), SC)
        return col(i - 1)

    def remote(src, dst, sem, dev):
        return pltpu.make_async_remote_copy(src_ref=src, dst_ref=dst, send_sem=ssem.at[sem], recv_sem=rsem.at[sem],
                                            device_id=dev, device_id_type=MESH)

    def head_rows(h):
        return pl.ds(pl.multiple_of(h * HD, HD), HD)

    loads = [
        pltpu.make_async_copy(x_in.at[0], xg.at[rows(m)], lsem.at[0]),
        pltpu.make_async_copy(dy_in.at[0], dyg.at[rows(m)], lsem.at[1]),
        pltpu.make_async_copy(wk_in.at[y], wqkv.at[:, pl.ds(HE, HD)], lsem.at[2]),
        pltpu.make_async_copy(wv_in.at[y], wqkv.at[:, pl.ds(HE + HD, HD)], lsem.at[3]),
        pltpu.make_async_copy(wq_in, wq8, lsem.at[4]),
        pltpu.make_async_copy(wo_in, wo, lsem.at[5]),
    ]
    for ld in loads:
        ld.start()

    barrier = pltpu.get_barrier_semaphore()
    for dev in (far_dev, core_dev, right_dev, left_dev):
        pl.semaphore_signal(barrier, inc=1, device_id=dev, device_id_type=MESH)
    pl.semaphore_wait(barrier, 4)

    def x_far(i, block):
        r = rows(block, XR, i * XR)
        return remote(xg.at[r], xg.at[r], S_XY + i, far_dev)

    def x_fwd(i, block):
        r = rows(block, XR, i * XR)
        return remote(xg.at[r], xg.at[r], S_XF + i, core_dev)

    def x_core(block):
        return remote(xg.at[rows(block)], xg.at[rows(block)], S_XC, core_dev)

    def dy_far(i, block):
        return remote(dyg.at[rows(block), dcol(i)], dyg.at[rows(block), dcol(i)], S_DY + i, far_dev)

    def dy_fwd(i, block):
        return remote(dyg.at[rows(block), dcol(i)], dyg.at[rows(block), dcol(i)], S_DF + i, core_dev)

    def dy_core(block):
        return remote(dyg.at[rows(block)], dyg.at[rows(block)], S_DC, core_dev)

    loads[0].wait()
    for i in range(NX):
        x_far(i, m).start()
    x_core(m).start()
    loads[1].wait()
    for i in range(5):
        dy_far(i, m).start()
    dy_core(m).start()
    for ld in loads[2:]:
        ld.wait()

    def wq_block(i, carry):
        wst[...] = wq8[pl.ds(pl.multiple_of(i * WR, WR), WR), :].astype(F32)
        for h in range(NH):
            wqkv[pl.ds(pl.multiple_of(i * (WR // NH), WR // NH), WR // NH), pl.ds(h * HD, HD)] = wst[pl.ds(h, WR // NH, stride=NH), :].astype(BF16)
        return carry

    lax.fori_loop(0, DIM * NH // WR, wq_block, 0)

    def project(r):
        qkv[r, :] = nn(xg[r, :], wqkv[...]).astype(BF16)

    def flip(block):
        r = rows(block)
        kt[:, r] = qkv[r, pl.ds(HE, HD)].T
        vt[:, r] = qkv[r, pl.ds(HE + HD, HD)].T

    project(rows(m))
    x_core(core_m).wait_recv()
    project(rows(core_m))
    flip(m)
    flip(core_m)

    def x_piece(i, carry):
        x_far(i, far_m).wait_recv()
        x_fwd(i, far_m).start()
        project(rows(far_m, XR, i * XR))
        x_fwd(i, diag_m).wait_recv()
        project(rows(diag_m, XR, i * XR))
        return carry

    lax.fori_loop(0, NX, x_piece, 0)

    flip(far_m)
    flip(diag_m)
    dy_core(core_m).wait_recv()

    def take_dy(i):
        dy_far(i, far_m).wait_recv()
        dy_fwd(i, far_m).start()

    take_dy(0)

    def ring_copy(base, which, hop, s, h):
        return remote(sring.at[which, hop, s, h], rring.at[which, hop, s, h], base + hop * 8 + s * 4 + h, right_dev)

    def half_col(s):
        return pl.ds(s * SC, SC)

    def wo_first(s, h):
        sring[0, 0, s, h] = nn(ot[head_rows(h), :], dyg[:, dcol(s)]).astype(BF16)
        ring_copy(S_WO, 0, 0, s, h).start()

    scale = HD ** -0.5
    exp_scale = scale * math.log2(math.e)
    diag_mask = lax.broadcasted_iota(jnp.int32, (BLK, BLK), 0) <= lax.broadcasted_iota(jnp.int32, (BLK, BLK), 1)

    def prow(qi, kj):
        return pl.ds(BLK * (qi * (qi + 1) // 2 + kj), BLK)

    def fwd_head(h, carry):
        hr = head_rows(h)
        for qi in range(NB):
            qb = qkv[pl.ds(qi * BLK, BLK), hr]
            mx = None
            for kj in range(qi + 1):
                s = nt(qkv[pl.ds(kj * BLK, BLK), pl.ds(HE, HD)], qb)
                if kj == qi:
                    s = jnp.where(diag_mask, s, -jnp.inf)
                prob[h, prow(qi, kj), :] = s
                bm = jnp.max(s, axis=0, keepdims=True)
                mx = bm if mx is None else jnp.maximum(mx, bm)
            tot = None
            for kj in range(qi + 1):
                e = jnp.exp2((prob[h, prow(qi, kj), :] - mx) * exp_scale)
                prob[h, prow(qi, kj), :] = e
                bs = jnp.sum(e, axis=0, keepdims=True)
                tot = bs if tot is None else tot + bs
            inv = 1.0 / tot
            for kj in range(qi + 1):
                p = prob[h, prow(qi, kj), :] * inv
                prob[h, prow(qi, kj), :] = p
                pbuf[pl.ds(kj * BLK, BLK), :] = p.astype(BF16)
            n = (qi + 1) * BLK
            ot[hr, pl.ds(qi * BLK, BLK)] = nn(vt[:, pl.ds(0, n)], pbuf[pl.ds(0, n), :]).astype(BF16)

        @pl.when(h == 0)
        def _():
            dy_fwd(0, diag_m).wait_recv()

        wo_first(0, h)

        @pl.when(h == 0)
        def _():
            take_dy(1)

        @pl.when(h == 1)
        def _():
            dy_fwd(1, diag_m).wait_recv()
            wo_first(1, 0)
            take_dy(2)

        @pl.when(h >= 1)
        def _():
            wo_first(1, h)

        return carry

    lax.fori_loop(0, NH, fwd_head, 0)

    def ring_service(base, which, hop, h):
        for s in range(2):
            ring_copy(base, which, hop - 1, s, h).wait_recv()
            total = pw[OWN[which][hop - 1], head_rows(h), half_col(s)] + rring[which, hop - 1, s, h].astype(F32)
            sring[which, hop, s, h] = total.astype(BF16)
            ring_copy(base, which, hop, s, h).start()

    def ring_final(base, which, h, s):
        ring_copy(base, which, 2, s, h).wait_recv()
        return pw[OWN[which][2], head_rows(h), half_col(s)] + rring[which, 2, s, h].astype(F32)

    def wo_own(i):
        pw[i - 1] = nn(ot[...], dyg[:, col(i)])

    def wq_own(i):
        pw[OWN[1][i - 1]] = nn(at[pl.ds(0, HE), :], xg[:, col(i)])

    for i in range(1, 4):
        if i > 1:
            take_dy(i + 1)
        dy_fwd(i + 1, diag_m).wait_recv()
        wo_own(i)
        if i < 3:
            for h in range(2):
                ring_service(S_WO, 0, 1, 2 * (i - 1) + h)

    def dout_block(b, carry):
        r = rows(b)
        dout[r, :] = nt(dyg[r, :], wo[...]).astype(BF16)
        return carry

    lax.fori_loop(0, NB, dout_block, 0)
    for h in range(2):
        ring_service(S_WO, 0, 2, h)

    dkv[...] = jnp.zeros_like(dkv)

    def bwd_head(h, carry):
        hr = head_rows(h)
        for qi in range(NB):
            qr = pl.ds(qi * BLK, BLK)
            dob = dout[qr, hr]
            qb = qkv[qr, hr]
            delta = jnp.sum(dob.astype(F32).T * ot[hr, qr].astype(F32), axis=0, keepdims=True)
            for kj in range(qi + 1):
                kr = pl.ds(kj * BLK, BLK)
                p = prob[h, prow(qi, kj), :]
                dp = nt(qkv[kr, pl.ds(HE + HD, HD)], dob)
                ds = (p * (dp - delta)).astype(BF16)
                pbuf[kr, :] = ds
                dkv[kr, pl.ds(0, HD)] += nn(ds, qb)
                dkv[kr, pl.ds(HD, HD)] += nn(p.astype(BF16), dob)
            n = (qi + 1) * BLK
            dq = (nn(kt[:, pl.ds(0, n)], pbuf[pl.ds(0, n), :]) * scale).astype(BF16)
            at[hr, qr] = dq
            am[qr, hr] = dq.T

        @pl.when(h < 2)
        def _():
            ring_service(S_WO, 0, 2, h + 2)

        first = nn(at[hr, :], xg[:, col(0)]).astype(BF16)
        for s in range(2):
            sring[1, 0, s, h] = first[:, s * SC:(s + 1) * SC]
            ring_copy(S_WQ, 1, 0, s, h).start()
        return carry

    lax.fori_loop(0, NH, bwd_head, 0)

    dkb = (dkv[:, pl.ds(0, HD)] * scale).astype(BF16)
    dvb = dkv[:, pl.ds(HD, HD)].astype(BF16)
    am[:, pl.ds(HE, HD)] = dkb
    am[:, pl.ds(HE + HD, HD)] = dvb
    at[pl.ds(HE, HD), :] = dkb.T
    at[pl.ds(HE + HD, HD), :] = dvb.T

    def dx_part(block, put):
        def piece(i, carry):
            cs = pl.ds(pl.multiple_of(i * CH, CH), CH)
            put(cs, nt(am[rows(block), :], wqkv[cs, :]))
            return carry

        lax.fori_loop(0, DIM // CH, piece, 0)

    def px_copy(i):
        return remote(sx.at[i], rx.at[i], S_PX + i, core_dev)

    def py_copy(i):
        r = pl.ds(i * (BLK // 2), BLK // 2)
        return remote(sy.at[r], ry.at[r], S_PY + i, far_dev)

    def put_sx(i):
        def put(cs, v):
            sx[i, :, cs] = v.astype(BF16)
        return put

    def put_ref(ref):
        def put(cs, v):
            ref[:, cs] = v
        return put

    half = DIM // 2

    def kv_half(which):
        return nn(at[pl.ds(HE, 2 * HD), :], xg[:, pl.ds(pl.multiple_of(which * half, half), half)])

    def kcol(i):
        return pl.ds(pl.multiple_of(((z + 3 - i) % 4) * KC, KC), KC)

    def kv_copy(hop):
        return remote(skv.at[hop], rkv.at[hop], S_KV + hop, right_dev)

    def kv_service(hop):
        kv_copy(hop - 1).wait_recv()
        skv[hop] = (pkv[:, kcol(hop)] + rkv[hop - 1].astype(F32)).astype(BF16)
        kv_copy(hop).start()

    kvs[...] = kv_half(1 - c).astype(BF16)
    kp_copy = remote(kvs, kvr, S_KP, core_dev)
    kp_copy.start()
    dx_part(diag_m, put_sx(0))
    px_copy(0).start()
    pkv[...] = kv_half(c)
    kp_copy.wait_recv()
    pkv[...] += kvr[...].astype(F32)
    skv[0] = pkv[:, kcol(0)].astype(BF16)
    kv_copy(0).start()
    dx_part(far_m, put_ref(pxo))
    px_copy(0).wait_recv()
    for i in range(2):
        r = pl.ds(i * (BLK // 2), BLK // 2)
        sy[r, :] = (pxo[r, :] + rx[0, r, :].astype(F32)).astype(BF16)
        py_copy(i).start()

    wq_own(1)
    for h in range(NH):
        ring_service(S_WQ, 1, 1, h)
    kv_service(1)
    dx_part(core_m, put_sx(1))
    px_copy(1).start()
    wq_own(2)
    for h in range(2):
        ring_service(S_WQ, 1, 2, h)
    kv_service(2)
    for h in range(2, NH):
        ring_service(S_WQ, 1, 2, h)
    wq_own(3)
    dx_part(m, put_ref(pxo))
    px_copy(1).wait_recv()
    pxo[...] += rx[1].astype(F32)

    for h in range(NH):
        for s in range(2):
            woo[head_rows(h), half_col(s)] = ring_final(S_WO, 0, h, s)
    for i in range(2):
        r = pl.ds(i * (BLK // 2), BLK // 2)
        py_copy(i).wait_recv()
        dxo[r, :] = (pxo[r, :] + ry[r, :].astype(F32)).astype(BF16)

    def wq_fin(h):
        for s in range(2):
            wqo[pl.ds(s * SC * NH + h, SC, stride=NH), :] = ring_final(S_WQ, 1, h, s).T

    for h in range(2):
        wq_fin(h)
    kv_copy(2).wait_recv()
    kv_sum = pkv[:, kcol(3)] + rkv[2].astype(F32)
    dko[...] = kv_sum[:HD].T
    dvo[...] = kv_sum[HD:].T
    for h in range(2, NH):
        wq_fin(h)

    for i in range(NX):
        x_far(i, m).wait_send()
        x_fwd(i, far_m).wait_send()
    x_core(m).wait_send()
    for i in range(5):
        dy_far(i, m).wait_send()
        dy_fwd(i, far_m).wait_send()
    dy_core(m).wait_send()
    for base, which in ((S_WO, 0), (S_WQ, 1)):
        for hop in range(3):
            for h in range(NH):
                for s in range(2):
                    ring_copy(base, which, hop, s, h).wait_send()
    for hop in range(3):
        kv_copy(hop).wait_send()
    kp_copy.wait_send()
    for i in range(2):
        px_copy(i).wait_send()
        py_copy(i).wait_send()


def solution(mesh):
    tok_spec = P(('pod', 'data'), 'model', None)

    def device_step(x_loc, dy_loc, w_q, w_k, w_v, w_o):
        any_spec = pl.BlockSpec(memory_space=pl.ANY)
        vmem_spec = pl.BlockSpec(memory_space=pltpu.VMEM)
        outs = (((BLK, DIM), BF16), ((CH * NH, HD), F32), ((KC, HD), F32), ((KC, HD), F32), ((HE, CH), F32))
        dx, dwq, dwk, dwv, dwo = pl.pallas_call(
            step_kernel,
            out_shape=tuple(pltpu.VMEM(shape, dtype) for shape, dtype in outs),
            in_specs=[any_spec] * 6,
            out_specs=[vmem_spec] * 5,
            scratch_shapes=[
                pltpu.VMEM((SEQ, DIM), BF16),
                pltpu.VMEM((SEQ, DIM), BF16),
                pltpu.VMEM((DIM * NH, HD), BF16),
                pltpu.VMEM((WR, HD), F32),
                pltpu.VMEM((DIM, QKV), BF16),
                pltpu.VMEM((HE, DIM), BF16),
                pltpu.VMEM((SEQ, QKV), BF16),
                pltpu.VMEM((HD, SEQ), BF16),
                pltpu.VMEM((HD, SEQ), BF16),
                pltpu.VMEM((NH, CAUSAL_ROWS, BLK), F32),
                pltpu.VMEM((SEQ, BLK), BF16),
                pltpu.VMEM((HE, SEQ), BF16),
                pltpu.VMEM((SEQ, HE), BF16),
                pltpu.VMEM((QKV, SEQ), BF16),
                pltpu.VMEM((SEQ, QKV), BF16),
                pltpu.VMEM((SEQ, 2 * HD), F32),
                pltpu.VMEM((4, HE, CH), F32),
                pltpu.VMEM((2 * HD, DIM // 2), F32),
                pltpu.VMEM((2 * HD, DIM // 2), BF16),
                pltpu.VMEM((2 * HD, DIM // 2), BF16),
                pltpu.VMEM((2, 3, 2, NH, HD, SC), BF16),
                pltpu.VMEM((2, 3, 2, NH, HD, SC), BF16),
                pltpu.VMEM((3, 2 * HD, KC), BF16),
                pltpu.VMEM((3, 2 * HD, KC), BF16),
                pltpu.VMEM((2, BLK, DIM), BF16),
                pltpu.VMEM((2, BLK, DIM), BF16),
                pltpu.VMEM((BLK, DIM), BF16),
                pltpu.VMEM((BLK, DIM), BF16),
                pltpu.VMEM((BLK, DIM), F32),
                pltpu.SemaphoreType.DMA((N_SEM,)),
                pltpu.SemaphoreType.DMA((N_SEM,)),
                pltpu.SemaphoreType.DMA((6,)),
            ],
            compiler_params=pltpu.CompilerParams(collective_id=0, has_side_effects=True, vmem_limit_bytes=VMEM_LIMIT),
        )(x_loc, dy_loc, w_q.reshape(DIM * NH, HD), w_k, w_v, w_o.reshape(HE, DIM))
        return dx.reshape(1, BLK, DIM), dwq.reshape(CH, NH, HD), dwk, dwv, dwo.reshape(NH, HD, CH)

    kv_rows = P(('pod', 'model', 'data'), None)
    return jax.shard_map(device_step, mesh=mesh,
                         in_specs=(tok_spec, tok_spec, P(None, 'model', None), P(), P(), P('model', None, None)),
                         out_specs=(tok_spec, P(('pod', 'data'), 'model', None), kv_rows, kv_rows, P(('pod', 'model'), None, 'data')),
                         check_vma=False)
```

```python
import functools
import math

import jax
import jax.numpy as jnp
from jax import lax
from jax.experimental import pallas as pl
from jax.experimental.pallas import tpu as pltpu
from jax.sharding import PartitionSpec as P

MESH = pl.DeviceIdType.MESH
F32 = jnp.float32
BF16 = jnp.bfloat16

SEQ = 1024
BLK = 256
DIM = 2048
HD = 128
NH = 4
HE = NH * HD
QKV = HE + 2 * HD
CH = 512
SC = CH // 2
WR = 1024
KC = 256
NX = 4
XR = BLK // NX
NB = SEQ // BLK
CAUSAL_ROWS = BLK * NB * (NB + 1) // 2

S_XY, S_XF, S_XC = 0, 4, 8
S_DY, S_DF, S_DC = 9, 14, 19
S_WO, S_WQ = 20, 44
S_KV = 68
S_KP = 71
S_PX = 72
S_PY = 74
N_SEM = 76
OWN = ((0, 1, 2), (3, 0, 1))
VMEM_LIMIT = 63 * 2 ** 20 - 3328 * 1024


def nn(a, b):
    return lax.dot_general(a, b, (((1,), (0,)), ((), ())), preferred_element_type=F32)


def nt(a, b):
    return lax.dot_general(a, b, (((1,), (1,)), ((), ())), preferred_element_type=F32)


def step_kernel(x_in, dy_in, wq_in, wk_in, wv_in, wo_in, dxo, wqo, dko, dvo, woo,
                xg, dyg, wq8, wst, wqkv, wo, qkv, kt, vt, prob, pbuf, ot, dout, at, am, dkv, pw, pkv,
                kvs, kvr, sring, rring, skv, rkv, sx, rx, sy, ry, pxo, ssem, rsem, lsem):
    pod = lax.axis_index("pod")
    z = lax.axis_index("data")
    m = lax.axis_index("model")
    y = m // 2
    c = m % 2
    core_m = 2 * y + 1 - c
    far_m = (m + 2) % 4
    diag_m = (core_m + 2) % 4
    core_dev = (pod, z, core_m)
    far_dev = (pod, z, far_m)
    right_dev = (pod, (z + 1) % 4, m)
    left_dev = (pod, (z + 3) % 4, m)

    def rows(block, n=BLK, off=0):
        return pl.ds(pl.multiple_of(block * BLK + off, n), n)

    def col(i):
        return pl.ds(pl.multiple_of(((z + 3 - i) % 4) * CH, CH), CH)

    def dcol(i):
        if i < 2:
            return pl.ds(pl.multiple_of(((z + 3) % 4) * CH + i * SC, SC), SC)
        return col(i - 1)

    def remote(src, dst, sem, dev):
        return pltpu.make_async_remote_copy(src_ref=src, dst_ref=dst, send_sem=ssem.at[sem], recv_sem=rsem.at[sem],
                                            device_id=dev, device_id_type=MESH)

    def head_rows(h):
        return pl.ds(pl.multiple_of(h * HD, HD), HD)

    loads = [
        pltpu.make_async_copy(x_in.at[0], xg.at[rows(m)], lsem.at[0]),
        pltpu.make_async_copy(dy_in.at[0], dyg.at[rows(m)], lsem.at[1]),
        pltpu.make_async_copy(wk_in.at[y], wqkv.at[:, pl.ds(HE, HD)], lsem.at[2]),
        pltpu.make_async_copy(wv_in.at[y], wqkv.at[:, pl.ds(HE + HD, HD)], lsem.at[3]),
        pltpu.make_async_copy(wq_in, wq8, lsem.at[4]),
        pltpu.make_async_copy(wo_in, wo, lsem.at[5]),
    ]
    for ld in loads:
        ld.start()

    barrier = pltpu.get_barrier_semaphore()
    for dev in (far_dev, core_dev, right_dev, left_dev):
        pl.semaphore_signal(barrier, inc=1, device_id=dev, device_id_type=MESH)
    pl.semaphore_wait(barrier, 4)

    def x_far(i, block):
        r = rows(block, XR, i * XR)
        return remote(xg.at[r], xg.at[r], S_XY + i, far_dev)

    def x_fwd(i, block):
        r = rows(block, XR, i * XR)
        return remote(xg.at[r], xg.at[r], S_XF + i, core_dev)

    def x_core(block):
        return remote(xg.at[rows(block)], xg.at[rows(block)], S_XC, core_dev)

    def dy_far(i, block):
        return remote(dyg.at[rows(block), dcol(i)], dyg.at[rows(block), dcol(i)], S_DY + i, far_dev)

    def dy_fwd(i, block):
        return remote(dyg.at[rows(block), dcol(i)], dyg.at[rows(block), dcol(i)], S_DF + i, core_dev)

    def dy_core(block):
        return remote(dyg.at[rows(block)], dyg.at[rows(block)], S_DC, core_dev)

    loads[0].wait()
    for i in range(NX):
        x_far(i, m).start()
    x_core(m).start()
    loads[1].wait()
    for i in range(5):
        dy_far(i, m).start()
    dy_core(m).start()
    for ld in loads[2:]:
        ld.wait()

    def wq_block(i, carry):
        wst[...] = wq8[pl.ds(pl.multiple_of(i * WR, WR), WR), :].astype(F32)
        for h in range(NH):
            wqkv[pl.ds(pl.multiple_of(i * (WR // NH), WR // NH), WR // NH), pl.ds(h * HD, HD)] = wst[pl.ds(h, WR // NH, stride=NH), :].astype(BF16)
        return carry

    lax.fori_loop(0, DIM * NH // WR, wq_block, 0)

    def project(r):
        qkv[r, :] = nn(xg[r, :], wqkv[...]).astype(BF16)

    def flip(block):
        r = rows(block)
        kt[:, r] = qkv[r, pl.ds(HE, HD)].T
        vt[:, r] = qkv[r, pl.ds(HE + HD, HD)].T

    project(rows(m))
    x_core(core_m).wait_recv()
    project(rows(core_m))
    flip(m)
    flip(core_m)

    def x_piece(i, carry):
        x_far(i, far_m).wait_recv()
        x_fwd(i, far_m).start()
        project(rows(far_m, XR, i * XR))
        x_fwd(i, diag_m).wait_recv()
        project(rows(diag_m, XR, i * XR))
        return carry

    lax.fori_loop(0, NX, x_piece, 0)

    flip(far_m)
    flip(diag_m)
    dy_core(core_m).wait_recv()

    def take_dy(i):
        dy_far(i, far_m).wait_recv()
        dy_fwd(i, far_m).start()

    take_dy(0)

    def ring_copy(base, which, hop, s, h):
        return remote(sring.at[which, hop, s, h], rring.at[which, hop, s, h], base + hop * 8 + s * 4 + h, right_dev)

    def half_col(s):
        return pl.ds(s * SC, SC)

    def wo_first(s, h):
        sring[0, 0, s, h] = nn(ot[head_rows(h), :], dyg[:, dcol(s)]).astype(BF16)
        ring_copy(S_WO, 0, 0, s, h).start()

    scale = HD ** -0.5
    exp_scale = scale * math.log2(math.e)
    diag_mask = lax.broadcasted_iota(jnp.int32, (BLK, BLK), 0) <= lax.broadcasted_iota(jnp.int32, (BLK, BLK), 1)

    def prow(qi, kj):
        return pl.ds(BLK * (qi * (qi + 1) // 2 + kj), BLK)

    def fwd_head(h, carry):
        hr = head_rows(h)
        for qi in range(NB):
            qb = qkv[pl.ds(qi * BLK, BLK), hr]
            mx = None
            for kj in range(qi + 1):
                s = nt(qkv[pl.ds(kj * BLK, BLK), pl.ds(HE, HD)], qb)
                if kj == qi:
                    s = jnp.where(diag_mask, s, -jnp.inf)
                prob[h, prow(qi, kj), :] = s
                bm = jnp.max(s, axis=0, keepdims=True)
                mx = bm if mx is None else jnp.maximum(mx, bm)
            tot = None
            for kj in range(qi + 1):
                e = jnp.exp2((prob[h, prow(qi, kj), :] - mx) * exp_scale)
                prob[h, prow(qi, kj), :] = e
                bs = jnp.sum(e, axis=0, keepdims=True)
                tot = bs if tot is None else tot + bs
            inv = 1.0 / tot
            for kj in range(qi + 1):
                p = prob[h, prow(qi, kj), :] * inv
                prob[h, prow(qi, kj), :] = p
                pbuf[pl.ds(kj * BLK, BLK), :] = p.astype(BF16)
            n = (qi + 1) * BLK
            ot[hr, pl.ds(qi * BLK, BLK)] = nn(vt[:, pl.ds(0, n)], pbuf[pl.ds(0, n), :]).astype(BF16)

        @pl.when(h == 0)
        def _():
            dy_fwd(0, diag_m).wait_recv()

        wo_first(0, h)

        @pl.when(h == 0)
        def _():
            take_dy(1)

        @pl.when(h == 1)
        def _():
            dy_fwd(1, diag_m).wait_recv()
            wo_first(1, 0)
            take_dy(2)

        @pl.when(h >= 1)
        def _():
            wo_first(1, h)

        return carry

    lax.fori_loop(0, NH, fwd_head, 0)

    def ring_service(base, which, hop, h):
        for s in range(2):
            ring_copy(base, which, hop - 1, s, h).wait_recv()
            total = pw[OWN[which][hop - 1], head_rows(h), half_col(s)] + rring[which, hop - 1, s, h].astype(F32)
            sring[which, hop, s, h] = total.astype(BF16)
            ring_copy(base, which, hop, s, h).start()

    def ring_final(base, which, h, s):
        ring_copy(base, which, 2, s, h).wait_recv()
        return pw[OWN[which][2], head_rows(h), half_col(s)] + rring[which, 2, s, h].astype(F32)

    def wo_own(i):
        pw[i - 1] = nn(ot[...], dyg[:, col(i)])

    def wq_own(i):
        pw[OWN[1][i - 1]] = nn(at[pl.ds(0, HE), :], xg[:, col(i)])

    for i in range(1, 4):
        if i > 1:
            take_dy(i + 1)
        dy_fwd(i + 1, diag_m).wait_recv()
        wo_own(i)
        if i < 3:
            for h in range(2):
                ring_service(S_WO, 0, 1, 2 * (i - 1) + h)

    def dout_block(b, carry):
        r = rows(b)
        dout[r, :] = nt(dyg[r, :], wo[...]).astype(BF16)
        return carry

    lax.fori_loop(0, NB, dout_block, 0)
    for h in range(2):
        ring_service(S_WO, 0, 2, h)

    dkv[...] = jnp.zeros_like(dkv)

    def bwd_head(h, carry):
        hr = head_rows(h)
        for qi in range(NB):
            qr = pl.ds(qi * BLK, BLK)
            dob = dout[qr, hr]
            qb = qkv[qr, hr]
            delta = jnp.sum(dob.astype(F32).T * ot[hr, qr].astype(F32), axis=0, keepdims=True)
            for kj in range(qi + 1):
                kr = pl.ds(kj * BLK, BLK)
                p = prob[h, prow(qi, kj), :]
                dp = nt(qkv[kr, pl.ds(HE + HD, HD)], dob)
                ds = (p * (dp - delta)).astype(BF16)
                pbuf[kr, :] = ds
                dkv[kr, pl.ds(0, HD)] += nn(ds, qb)
                dkv[kr, pl.ds(HD, HD)] += nn(p.astype(BF16), dob)
            n = (qi + 1) * BLK
            dq = (nn(kt[:, pl.ds(0, n)], pbuf[pl.ds(0, n), :]) * scale).astype(BF16)
            at[hr, qr] = dq
            am[qr, hr] = dq.T

        @pl.when(h < 2)
        def _():
            ring_service(S_WO, 0, 2, h + 2)

        first = nn(at[hr, :], xg[:, col(0)]).astype(BF16)
        for s in range(2):
            sring[1, 0, s, h] = first[:, s * SC:(s + 1) * SC]
            ring_copy(S_WQ, 1, 0, s, h).start()
        return carry

    lax.fori_loop(0, NH, bwd_head, 0)

    dkb = (dkv[:, pl.ds(0, HD)] * scale).astype(BF16)
    dvb = dkv[:, pl.ds(HD, HD)].astype(BF16)
    am[:, pl.ds(HE, HD)] = dkb
    am[:, pl.ds(HE + HD, HD)] = dvb
    at[pl.ds(HE, HD), :] = dkb.T
    at[pl.ds(HE + HD, HD), :] = dvb.T

    def dx_part(block, put):
        def piece(i, carry):
            cs = pl.ds(pl.multiple_of(i * CH, CH), CH)
            put(cs, nt(am[rows(block), :], wqkv[cs, :]))
            return carry

        lax.fori_loop(0, DIM // CH, piece, 0)

    def px_copy(i):
        return remote(sx.at[i], rx.at[i], S_PX + i, core_dev)

    def py_copy(i):
        r = pl.ds(i * (BLK // 2), BLK // 2)
        return remote(sy.at[r], ry.at[r], S_PY + i, far_dev)

    def put_sx(i):
        def put(cs, v):
            sx[i, :, cs] = v.astype(BF16)
        return put

    def put_ref(ref):
        def put(cs, v):
            ref[:, cs] = v
        return put

    half = DIM // 2

    def kv_half(which):
        return nn(at[pl.ds(HE, 2 * HD), :], xg[:, pl.ds(pl.multiple_of(which * half, half), half)])

    def kcol(i):
        return pl.ds(pl.multiple_of(((z + 3 - i) % 4) * KC, KC), KC)

    def kv_copy(hop):
        return remote(skv.at[hop], rkv.at[hop], S_KV + hop, right_dev)

    def kv_service(hop):
        kv_copy(hop - 1).wait_recv()
        skv[hop] = (pkv[:, kcol(hop)] + rkv[hop - 1].astype(F32)).astype(BF16)
        kv_copy(hop).start()

    kvs[...] = kv_half(1 - c).astype(BF16)
    kp_copy = remote(kvs, kvr, S_KP, core_dev)
    kp_copy.start()
    dx_part(diag_m, put_sx(0))
    px_copy(0).start()
    pkv[...] = kv_half(c)
    kp_copy.wait_recv()
    pkv[...] += kvr[...].astype(F32)
    skv[0] = pkv[:, kcol(0)].astype(BF16)
    kv_copy(0).start()
    dx_part(far_m, put_ref(pxo))
    px_copy(0).wait_recv()
    for i in range(2):
        r = pl.ds(i * (BLK // 2), BLK // 2)
        sy[r, :] = (pxo[r, :] + rx[0, r, :].astype(F32)).astype(BF16)
        py_copy(i).start()

    wq_own(1)
    for h in range(NH):
        ring_service(S_WQ, 1, 1, h)
    kv_service(1)
    dx_part(core_m, put_sx(1))
    px_copy(1).start()
    wq_own(2)
    for h in range(2):
        ring_service(S_WQ, 1, 2, h)
    kv_service(2)
    for h in range(2, NH):
        ring_service(S_WQ, 1, 2, h)
    wq_own(3)
    dx_part(m, put_ref(pxo))
    px_copy(1).wait_recv()
    pxo[...] += rx[1].astype(F32)

    for h in range(NH):
        for s in range(2):
            woo[head_rows(h), half_col(s)] = ring_final(S_WO, 0, h, s)
    for i in range(2):
        r = pl.ds(i * (BLK // 2), BLK // 2)
        py_copy(i).wait_recv()
        dxo[r, :] = (pxo[r, :] + ry[r, :].astype(F32)).astype(BF16)

    def wq_fin(h):
        for s in range(2):
            wqo[pl.ds(s * SC * NH + h, SC, stride=NH), :] = ring_final(S_WQ, 1, h, s).T

    for h in range(2):
        wq_fin(h)
    kv_copy(2).wait_recv()
    kv_sum = pkv[:, kcol(3)] + rkv[2].astype(F32)
    dko[...] = kv_sum[:HD].T
    dvo[...] = kv_sum[HD:].T
    for h in range(2, NH):
        wq_fin(h)

    for i in range(NX):
        x_far(i, m).wait_send()
        x_fwd(i, far_m).wait_send()
    x_core(m).wait_send()
    for i in range(5):
        dy_far(i, m).wait_send()
        dy_fwd(i, far_m).wait_send()
    dy_core(m).wait_send()
    for base, which in ((S_WO, 0), (S_WQ, 1)):
        for hop in range(3):
            for h in range(NH):
                for s in range(2):
                    ring_copy(base, which, hop, s, h).wait_send()
    for hop in range(3):
        kv_copy(hop).wait_send()
    kp_copy.wait_send()
    for i in range(2):
        px_copy(i).wait_send()
        py_copy(i).wait_send()


def store_kernel(*refs):
    n = len(refs) // 2
    sem = refs[-1]
    copies = [pltpu.make_async_copy(refs[i], refs[n + i], sem.at[i]) for i in range(n)]
    for cp in copies:
        cp.start()
    for cp in copies:
        cp.wait()


def solution(mesh):
    tok_spec = P(('pod', 'data'), 'model', None)

    def device_step(x_loc, dy_loc, w_q, w_k, w_v, w_o):
        any_spec = pl.BlockSpec(memory_space=pl.ANY)
        vmem_spec = pl.BlockSpec(memory_space=pltpu.VMEM)
        outs = (((BLK, DIM), BF16), ((CH * NH, HD), F32), ((KC, HD), F32), ((KC, HD), F32), ((HE, CH), F32))
        dx, dwq, dwk, dwv, dwo = pl.pallas_call(
            step_kernel,
            out_shape=tuple(pltpu.VMEM(shape, dtype) for shape, dtype in outs),
            in_specs=[any_spec] * 6,
            out_specs=[vmem_spec] * 5,
            scratch_shapes=[
                pltpu.VMEM((SEQ, DIM), BF16),
                pltpu.VMEM((SEQ, DIM), BF16),
                pltpu.VMEM((DIM * NH, HD), BF16),
                pltpu.VMEM((WR, HD), F32),
                pltpu.VMEM((DIM, QKV), BF16),
                pltpu.VMEM((HE, DIM), BF16),
                pltpu.VMEM((SEQ, QKV), BF16),
                pltpu.VMEM((HD, SEQ), BF16),
                pltpu.VMEM((HD, SEQ), BF16),
                pltpu.VMEM((NH, CAUSAL_ROWS, BLK), F32),
                pltpu.VMEM((SEQ, BLK), BF16),
                pltpu.VMEM((HE, SEQ), BF16),
                pltpu.VMEM((SEQ, HE), BF16),
                pltpu.VMEM((QKV, SEQ), BF16),
                pltpu.VMEM((SEQ, QKV), BF16),
                pltpu.VMEM((SEQ, 2 * HD), F32),
                pltpu.VMEM((4, HE, CH), F32),
                pltpu.VMEM((2 * HD, DIM // 2), F32),
                pltpu.VMEM((2 * HD, DIM // 2), BF16),
                pltpu.VMEM((2 * HD, DIM // 2), BF16),
                pltpu.VMEM((2, 3, 2, NH, HD, SC), BF16),
                pltpu.VMEM((2, 3, 2, NH, HD, SC), BF16),
                pltpu.VMEM((3, 2 * HD, KC), BF16),
                pltpu.VMEM((3, 2 * HD, KC), BF16),
                pltpu.VMEM((2, BLK, DIM), BF16),
                pltpu.VMEM((2, BLK, DIM), BF16),
                pltpu.VMEM((BLK, DIM), BF16),
                pltpu.VMEM((BLK, DIM), BF16),
                pltpu.VMEM((BLK, DIM), F32),
                pltpu.SemaphoreType.DMA((N_SEM,)),
                pltpu.SemaphoreType.DMA((N_SEM,)),
                pltpu.SemaphoreType.DMA((6,)),
            ],
            compiler_params=pltpu.CompilerParams(collective_id=0, has_side_effects=True, vmem_limit_bytes=VMEM_LIMIT),
        )(x_loc, dy_loc, w_q.reshape(DIM * NH, HD), w_k, w_v, w_o.reshape(HE, DIM))
        dx, dwq, dwk, dwv, dwo = pl.pallas_call(
            store_kernel,
            out_shape=tuple(jax.ShapeDtypeStruct(shape, dtype) for shape, dtype in outs),
            in_specs=[any_spec] * 5,
            out_specs=[any_spec] * 5,
            scratch_shapes=[pltpu.SemaphoreType.DMA((5,))],
            compiler_params=pltpu.CompilerParams(vmem_limit_bytes=2 ** 20),
        )(dx, dwq, dwk, dwv, dwo)
        return dx.reshape(1, BLK, DIM), dwq.reshape(CH, NH, HD), dwk, dwv, dwo.reshape(NH, HD, CH)

    kv_rows = P(('pod', 'model', 'data'), None)
    return jax.shard_map(device_step, mesh=mesh,
                         in_specs=(tok_spec, tok_spec, P(None, 'model', None), P(), P(), P('model', None, None)),
                         out_specs=(tok_spec, P(('pod', 'data'), 'model', None), kv_rows, kv_rows, P(('pod', 'model'), None, 'data')),
                         check_vma=False)
```

```python
import functools
import math

import jax
import jax.numpy as jnp
from jax import lax
from jax.experimental import pallas as pl
from jax.experimental.pallas import tpu as pltpu
from jax.sharding import PartitionSpec as P

MESH = pl.DeviceIdType.MESH
F32 = jnp.float32
BF16 = jnp.bfloat16

SEQ = 1024
BLK = 256
DIM = 2048
HD = 128
NH = 4
HE = NH * HD
QKV = HE + 2 * HD
CH = 512
SC = CH // 2
WR = 1024
KC = 256
NX = 4
XR = BLK // NX
NB = SEQ // BLK
CAUSAL_ROWS = BLK * NB * (NB + 1) // 2

S_XY, S_XF, S_XC = 0, 4, 8
S_DY, S_DF, S_DC = 9, 14, 19
S_WO, S_WQ = 20, 44
S_KV = 68
S_KP = 71
S_PX = 72
S_PY = 74
S_XN, S_XNC, S_XNF, S_XNG = 76, 77, 78, 79
S_A = 80
N_SEM = 83
AH = 3
OWN = ((0, 1, 2), (3, 0, 1))
VMEM_LIMIT = 63 * 2 ** 20 - 3328 * 1024


def nn(a, b):
    return lax.dot_general(a, b, (((1,), (0,)), ((), ())), preferred_element_type=F32)


def nt(a, b):
    return lax.dot_general(a, b, (((1,), (1,)), ((), ())), preferred_element_type=F32)


def step_kernel(x_in, dy_in, wq_in, wk_in, wv_in, wo_in, dxo, wqo, dko, dvo, woo,
                xg, dyg, wq8, wst, wqkv, wo, qkv, kt, vt, prob, pbuf, ot, dout, at, am, dkv, pw, pkv,
                kvs, kvr, sring, rring, skv, rkv, sx, rx, sy, ry, xn, abuf, ssem, rsem, lsem):
    pod = lax.axis_index("pod")
    z = lax.axis_index("data")
    m = lax.axis_index("model")
    y = m // 2
    c = m % 2
    core_m = 2 * y + 1 - c
    far_m = (m + 2) % 4
    diag_m = (core_m + 2) % 4
    core_dev = (pod, z, core_m)
    far_dev = (pod, z, far_m)
    right_dev = (pod, (z + 1) % 4, m)
    left_dev = (pod, (z + 3) % 4, m)

    inner = ((z + 1) // 2) % 2
    edge_nb = (pod, 1 + z // 3, m)
    q_e = 3 * (z // 2)
    q_oe = 3 - q_e
    q_o = 3 - z
    edge_dev = (pod, q_e, m)
    other_dev = (pod, q_o, m)
    x_off = CH * (1 - z // 2)

    def rows(block, n=BLK, off=0):
        return pl.ds(pl.multiple_of(block * BLK + off, n), n)

    def col(i):
        return pl.ds(pl.multiple_of(((z + 3 - i) % 4) * CH, CH), CH)

    def dcol(i):
        if i < 2:
            return pl.ds(pl.multiple_of(((z + 3) % 4) * CH + i * SC, SC), SC)
        return col(i - 1)

    def remote(src, dst, sem, dev):
        return pltpu.make_async_remote_copy(src_ref=src, dst_ref=dst, send_sem=ssem.at[sem], recv_sem=rsem.at[sem],
                                            device_id=dev, device_id_type=MESH)

    def head_rows(h):
        return pl.ds(pl.multiple_of(h * HD, HD), HD)

    loads = [
        pltpu.make_async_copy(x_in.at[0], xg.at[rows(m)], lsem.at[0]),
        pltpu.make_async_copy(dy_in.at[0], dyg.at[rows(m)], lsem.at[1]),
        pltpu.make_async_copy(wk_in.at[y], wqkv.at[:, pl.ds(HE, HD)], lsem.at[2]),
        pltpu.make_async_copy(wv_in.at[y], wqkv.at[:, pl.ds(HE + HD, HD)], lsem.at[3]),
        pltpu.make_async_copy(wo_in, wo, lsem.at[4]),
    ]
    def wq_load(i):
        return pltpu.make_async_copy(wq_in.at[pl.ds(pl.multiple_of(i * WR, WR), WR)], wq8.at[i % 2], lsem.at[5 + i % 2])

    for ld in loads:
        ld.start()
    wq_load(0).start()
    wq_load(1).start()

    barrier = pltpu.get_barrier_semaphore()
    for dev in (far_dev, core_dev, right_dev, left_dev):
        pl.semaphore_signal(barrier, inc=1, device_id=dev, device_id_type=MESH)
    pl.semaphore_wait(barrier, 4)

    def x_far(i, block):
        r = rows(block, XR, i * XR)
        return remote(xg.at[r], xg.at[r], S_XY + i, far_dev)

    def x_fwd(i, block):
        r = rows(block, XR, i * XR)
        return remote(xg.at[r], xg.at[r], S_XF + i, core_dev)

    def x_core(block):
        return remote(xg.at[rows(block)], xg.at[rows(block)], S_XC, core_dev)

    def dy_far(i, block):
        return remote(dyg.at[rows(block), dcol(i)], dyg.at[rows(block), dcol(i)], S_DY + i, far_dev)

    def dy_fwd(i, block):
        return remote(dyg.at[rows(block), dcol(i)], dyg.at[rows(block), dcol(i)], S_DF + i, core_dev)

    def dy_core(block):
        return remote(dyg.at[rows(block)], dyg.at[rows(block)], S_DC, core_dev)

    def xn_edge(block):
        return remote(xg.at[rows(block), pl.ds(pl.multiple_of(x_off, CH), 3 * CH)], xn.at[rows(block)], S_XN, edge_nb)

    def xn_send(block, sem, dev):
        return remote(xn.at[rows(block)], xn.at[rows(block)], sem, dev)

    loads[0].wait()
    for i in range(NX):
        x_far(i, m).start()

    @pl.when(inner == 0)
    def _():
        xn_edge(m).start()

    x_core(m).start()
    loads[1].wait()
    for i in range(5):
        dy_far(i, m).start()
    dy_core(m).start()
    for ld in loads[2:]:
        ld.wait()

    def wq_block(i, carry):
        wq_load(i).wait()
        wst[...] = wq8[i % 2].astype(F32)

        @pl.when(i + 2 < DIM * NH // WR)
        def _():
            wq_load(i + 2).start()

        for h in range(NH):
            wqkv[pl.ds(pl.multiple_of(i * (WR // NH), WR // NH), WR // NH), pl.ds(h * HD, HD)] = wst[pl.ds(h, WR // NH, stride=NH), :].astype(BF16)
        return carry

    lax.fori_loop(0, DIM * NH // WR, wq_block, 0)

    def project(r):
        qkv[r, :] = nn(xg[r, :], wqkv[...]).astype(BF16)

    def flip(block):
        r = rows(block)
        kt[:, r] = qkv[r, pl.ds(HE, HD)].T
        vt[:, r] = qkv[r, pl.ds(HE + HD, HD)].T

    project(rows(m))
    x_core(core_m).wait_recv()
    project(rows(core_m))
    flip(m)
    flip(core_m)

    def x_piece(i, carry):
        x_far(i, far_m).wait_recv()
        x_fwd(i, far_m).start()
        project(rows(far_m, XR, i * XR))
        x_fwd(i, diag_m).wait_recv()
        project(rows(diag_m, XR, i * XR))
        return carry

    lax.fori_loop(0, NX, x_piece, 0)

    flip(far_m)
    flip(diag_m)
    dy_core(core_m).wait_recv()

    def take_dy(i):
        dy_far(i, far_m).wait_recv()
        dy_fwd(i, far_m).start()

    def ring_copy(base, which, hop, s, h):
        return remote(sring.at[which, hop, s, h], rring.at[which, hop, s, h], base + hop * 8 + s * 4 + h, right_dev)

    def half_col(s):
        return pl.ds(s * SC, SC)

    def wo_first(s, h):
        sring[0, 0, s, h] = nn(ot[head_rows(h), :], dyg[:, dcol(s)]).astype(BF16)
        ring_copy(S_WO, 0, 0, s, h).start()

    @pl.when(inner == 1)
    def _():
        xn_edge(m).wait_recv()
        xn_send(m, S_XNF, far_dev).start()
        xn_send(m, S_XNC, core_dev).start()

    scale = HD ** -0.5
    exp_scale = scale * math.log2(math.e)
    diag_mask = lax.broadcasted_iota(jnp.int32, (BLK, BLK), 0) <= lax.broadcasted_iota(jnp.int32, (BLK, BLK), 1)

    def prow(qi, kj):
        return pl.ds(BLK * (qi * (qi + 1) // 2 + kj), BLK)

    def fwd_head(h, carry):
        hr = head_rows(h)
        for qi in range(NB):
            qb = qkv[pl.ds(qi * BLK, BLK), hr]
            mx = None
            for kj in range(qi + 1):
                s = nt(qkv[pl.ds(kj * BLK, BLK), pl.ds(HE, HD)], qb)
                if kj == qi:
                    s = jnp.where(diag_mask, s, -jnp.inf)
                prob[h, prow(qi, kj), :] = s
                bm = jnp.max(s, axis=0, keepdims=True)
                mx = bm if mx is None else jnp.maximum(mx, bm)
            tot = None
            for kj in range(qi + 1):
                e = jnp.exp2((prob[h, prow(qi, kj), :] - mx) * exp_scale)
                prob[h, prow(qi, kj), :] = e
                bs = jnp.sum(e, axis=0, keepdims=True)
                tot = bs if tot is None else tot + bs
            inv = 1.0 / tot
            for kj in range(qi + 1):
                p = prob[h, prow(qi, kj), :] * inv
                prob[h, prow(qi, kj), :] = p
                pbuf[pl.ds(kj * BLK, BLK), :] = p.astype(BF16)
            n = (qi + 1) * BLK
            ot[hr, pl.ds(qi * BLK, BLK)] = nn(vt[:, pl.ds(0, n)], pbuf[pl.ds(0, n), :]).astype(BF16)
            for at_h, at_q, piece in ((0, 2, 0), (1, 1, 1), (3, 0, 2)):
                if qi == at_q:
                    @pl.when(h == at_h)
                    def _(piece=piece):
                        take_dy(piece)

        @pl.when(h == 0)
        def _():
            dy_fwd(0, diag_m).wait_recv()

        wo_first(0, h)

        @pl.when(h == 1)
        def _():
            dy_fwd(1, diag_m).wait_recv()
            wo_first(1, 0)

        @pl.when(h >= 1)
        def _():
            wo_first(1, h)

        return carry

    lax.fori_loop(0, NH, fwd_head, 0)

    def ring_service(base, which, hop, h):
        for s in range(2):
            ring_copy(base, which, hop - 1, s, h).wait_recv()
            total = pw[OWN[which][hop - 1], head_rows(h), half_col(s)] + rring[which, hop - 1, s, h].astype(F32)
            sring[which, hop, s, h] = total.astype(BF16)
            ring_copy(base, which, hop, s, h).start()

    def ring_final(base, which, h, s):
        ring_copy(base, which, 2, s, h).wait_recv()
        return pw[OWN[which][2], head_rows(h), half_col(s)] + rring[which, 2, s, h].astype(F32)

    def wo_own(i):
        pw[i - 1] = nn(ot[...], dyg[:, col(i)])

    ring_rows = pl.ds(AH * HD, (NH - AH) * HD)

    def wq_own(i, r):
        pw[OWN[1][i - 1], r, :] = nn(at[r, :], xg[:, col(i)])

    def a_copy(h):
        r = head_rows(h)
        return remote(at.at[r], abuf.at[r], S_A + h, edge_nb)

    def swap_copy(k, s, h):
        return remote(sring.at[1, k, s, h], rring.at[1, k, s, h], S_WQ + k * 8 + s * 4 + h, other_dev)

    def outer_copy(s, h):
        return remote(sring.at[1, 2, s, h], rring.at[1, 2, s, h], S_WQ + 16 + s * 4 + h, edge_dev)

    def xcol(q):
        return pl.ds(pl.multiple_of(q * CH, CH), CH)

    def ncol(q):
        return pl.ds(pl.multiple_of(q * CH - x_off, CH), CH)

    def spot(k, s, h, n):
        return 1 + k // 2, pl.ds(((k % 2) * 2 + s) * AH * HD + h * HD, n * HD)

    def roles():
        for k, q in enumerate((q_oe, q_o, q_e)):
            v = nn(at[pl.ds(0, AH * HD), :], xg[:, xcol(q)])
            for s in range(2):
                j, r = spot(k, s, 0, AH)
                prob[j, r, :] = v[:, s * SC:(s + 1) * SC]

    def combine(h):
        a_copy(h).wait_recv()
        for k, q in enumerate((q_oe, q_o)):
            v = nn(abuf[head_rows(h), :], xn[:, ncol(q)])
            for s in range(2):
                j, r = spot(k, s, h, 1)
                sring[1, k, s, h] = (prob[j, r, :] + v[:, s * SC:(s + 1) * SC]).astype(BF16)
                swap_copy(k, s, h).start()

    def outer(h):
        for s in range(2):
            swap_copy(0, s, h).wait_recv()
            j, r = spot(2, s, h, 1)
            sring[1, 2, s, h] = (prob[j, r, :] + rring[1, 0, s, h].astype(F32)).astype(BF16)
            outer_copy(s, h).start()

    for i in range(1, 4):
        if i > 1:
            take_dy(i + 1)
        dy_fwd(i + 1, diag_m).wait_recv()
        wo_own(i)
        if i < 3:
            for h in range(2):
                ring_service(S_WO, 0, 1, 2 * (i - 1) + h)

    def dout_block(b, carry):
        r = rows(b)
        dout[r, :] = nt(dyg[r, :], wo[...]).astype(BF16)
        return carry

    lax.fori_loop(0, NB, dout_block, 0)
    for h in range(2):
        ring_service(S_WO, 0, 2, h)

    dkv[...] = jnp.zeros_like(dkv)

    def bwd_head(h, carry):
        hr = head_rows(h)
        for qi in range(NB):
            qr = pl.ds(qi * BLK, BLK)
            dob = dout[qr, hr]
            qb = qkv[qr, hr]
            delta = jnp.sum(dob.astype(F32).T * ot[hr, qr].astype(F32), axis=0, keepdims=True)
            for kj in range(qi + 1):
                kr = pl.ds(kj * BLK, BLK)
                p = prob[h, prow(qi, kj), :]
                dp = nt(qkv[kr, pl.ds(HE + HD, HD)], dob)
                ds = (p * (dp - delta)).astype(BF16)
                pbuf[kr, :] = ds
                dkv[kr, pl.ds(0, HD)] += nn(ds, qb)
                dkv[kr, pl.ds(HD, HD)] += nn(p.astype(BF16), dob)
            n = (qi + 1) * BLK
            dq = (nn(kt[:, pl.ds(0, n)], pbuf[pl.ds(0, n), :]) * scale).astype(BF16)
            at[hr, qr] = dq
            am[qr, hr] = dq.T

        @pl.when((h < 2) & (inner == 1))
        def _():
            ring_service(S_WO, 0, 2, h + 2)

        @pl.when((h < AH) & (inner == 0))
        def _():
            a_copy(h).start()

        @pl.when(h >= AH)
        def _():
            first = nn(at[hr, :], xg[:, col(0)]).astype(BF16)
            for s in range(2):
                sring[1, 0, s, h] = first[:, s * SC:(s + 1) * SC]
                ring_copy(S_WQ, 1, 0, s, h).start()

        return carry

    lax.fori_loop(0, NH, bwd_head, 0)

    @pl.when(inner == 0)
    def _():
        for h in range(2, NH):
            ring_service(S_WO, 0, 2, h)

    dkb = (dkv[:, pl.ds(0, HD)] * scale).astype(BF16)
    dvb = dkv[:, pl.ds(HD, HD)].astype(BF16)
    am[:, pl.ds(HE, HD)] = dkb
    am[:, pl.ds(HE + HD, HD)] = dvb
    at[pl.ds(HE, HD), :] = dkb.T
    at[pl.ds(HE + HD, HD), :] = dvb.T

    def dx_part(block, put):
        def piece(i, carry):
            cs = pl.ds(pl.multiple_of(i * CH, CH), CH)
            put(i, cs, nt(am[rows(block), :], wqkv[cs, :]))
            return carry

        lax.fori_loop(0, DIM // CH, piece, 0)

    def px_copy(i):
        return remote(sx.at[i], rx.at[i], S_PX + i, core_dev)

    def py_copy(i):
        r = pl.ds(i * (BLK // 2), BLK // 2)
        return remote(sy.at[r], ry.at[r], S_PY + i, far_dev)

    def put_sx(j):
        def put(i, cs, v):
            sx[j, :, cs] = v.astype(BF16)
        return put

    def pxo(i, s):
        return prob.at[0, pl.ds(pl.multiple_of((2 * i + s) * BLK, BLK), BLK)]

    def put_own(i, cs, v):
        for s in range(2):
            pxo(i, s)[...] = v[:, s * SC:(s + 1) * SC]

    half = DIM // 2

    def kv_half(which):
        return nn(at[pl.ds(HE, 2 * HD), :], xg[:, pl.ds(pl.multiple_of(which * half, half), half)])

    def kcol(i):
        return pl.ds(pl.multiple_of(((z + 3 - i) % 4) * KC, KC), KC)

    def kv_copy(hop):
        return remote(skv.at[hop], rkv.at[hop], S_KV + hop, right_dev)

    def kv_service(hop):
        kv_copy(hop - 1).wait_recv()
        skv[hop] = (pkv[:, kcol(hop)] + rkv[hop - 1].astype(F32)).astype(BF16)
        kv_copy(hop).start()

    kvs[...] = kv_half(1 - c).astype(BF16)
    kp_copy = remote(kvs, kvr, S_KP, core_dev)
    kp_copy.start()
    dx_part(diag_m, put_sx(0))
    px_copy(0).start()
    pkv[...] = kv_half(c)
    kp_copy.wait_recv()
    pkv[...] += kvr[...].astype(F32)
    skv[0] = pkv[:, kcol(0)].astype(BF16)
    kv_copy(0).start()

    @pl.when(inner == 1)
    def _():
        xn_send(far_m, S_XNF, far_dev).wait_recv()
        xn_send(far_m, S_XNG, core_dev).start()
        roles()

    dx_part(far_m, put_own)
    px_copy(0).wait_recv()
    for i in range(2):
        r = pl.ds(i * (BLK // 2), BLK // 2)
        for j in range(DIM // SC):
            cs = pl.ds(j * SC, SC)
            own = prob[0, pl.ds(j * BLK + i * (BLK // 2), BLK // 2), :]
            sy[r, cs] = (own + rx[0, r, cs].astype(F32)).astype(BF16)
        py_copy(i).start()

    @pl.when(inner == 1)
    def _():
        xn_send(core_m, S_XNC, core_dev).wait_recv()
        xn_send(diag_m, S_XNG, core_dev).wait_recv()
        combine(0)
        combine(1)
        outer(0)
        combine(2)
        outer(1)

    for i in (1, 2):
        wq_own(i, ring_rows)
    wq_own(3, pl.ds(0, HE))
    dx_part(core_m, put_sx(1))
    px_copy(1).start()
    dx_part(m, put_own)
    for h in range(NH):
        for s in range(2):
            woo[head_rows(h), half_col(s)] = ring_final(S_WO, 0, h, s)

    for h in range(AH, NH):
        ring_service(S_WQ, 1, 1, h)

    @pl.when(inner == 1)
    def _():
        outer(2)

    kv_service(1)

    @pl.when(inner == 1)
    def _():
        pw[OWN[1][2], pl.ds(0, AH * HD), :] += nn(abuf[...], xn[:, ncol(z)])

    for h in range(AH, NH):
        ring_service(S_WQ, 1, 2, h)
    kv_service(2)

    px_copy(1).wait_recv()
    for i in range(2):
        r = pl.ds(i * (BLK // 2), BLK // 2)
        py_copy(i).wait_recv()
        for j in range(DIM // SC):
            cs = pl.ds(j * SC, SC)
            own = prob[0, pl.ds(j * BLK + i * (BLK // 2), BLK // 2), :]
            dxo[r, cs] = (own + rx[1, r, cs].astype(F32) + ry[r, cs].astype(F32)).astype(BF16)

    def wq_put(h, s, v):
        wqo[pl.ds(s * SC * NH + h, SC, stride=NH), :] = v.T

    @pl.when(inner == 1)
    def _():
        for h in range(AH):
            for s in range(2):
                swap_copy(1, s, h).wait_recv()
                wq_put(h, s, pw[OWN[1][2], head_rows(h), half_col(s)] + rring[1, 1, s, h].astype(F32))

    @pl.when(inner == 0)
    def _():
        for h in range(AH):
            for s in range(2):
                outer_copy(s, h).wait_recv()
                wq_put(h, s, pw[OWN[1][2], head_rows(h), half_col(s)] + rring[1, 2, s, h].astype(F32))

    for h in range(AH, NH):
        for s in range(2):
            wq_put(h, s, ring_final(S_WQ, 1, h, s))
    kv_copy(2).wait_recv()
    kv_sum = pkv[:, kcol(3)] + rkv[2].astype(F32)
    dko[...] = kv_sum[:HD].T
    dvo[...] = kv_sum[HD:].T

    for i in range(NX):
        x_far(i, m).wait_send()
        x_fwd(i, far_m).wait_send()
    x_core(m).wait_send()
    for i in range(5):
        dy_far(i, m).wait_send()
        dy_fwd(i, far_m).wait_send()
    dy_core(m).wait_send()
    for hop in range(3):
        for s in range(2):
            for h in range(NH):
                ring_copy(S_WO, 0, hop, s, h).wait_send()
            for h in range(AH, NH):
                ring_copy(S_WQ, 1, hop, s, h).wait_send()

    @pl.when(inner == 0)
    def _():
        xn_edge(m).wait_send()
        for h in range(AH):
            a_copy(h).wait_send()

    @pl.when(inner == 1)
    def _():
        xn_send(m, S_XNF, far_dev).wait_send()
        xn_send(m, S_XNC, core_dev).wait_send()
        xn_send(far_m, S_XNG, core_dev).wait_send()
        for h in range(AH):
            for s in range(2):
                for k in range(2):
                    swap_copy(k, s, h).wait_send()
                outer_copy(s, h).wait_send()

    for hop in range(3):
        kv_copy(hop).wait_send()
    kp_copy.wait_send()
    for i in range(2):
        px_copy(i).wait_send()
        py_copy(i).wait_send()


def store_kernel(*refs):
    n = len(refs) // 2
    sem = refs[-1]
    copies = [pltpu.make_async_copy(refs[i], refs[n + i], sem.at[i]) for i in range(n)]
    for cp in copies:
        cp.start()
    for cp in copies:
        cp.wait()


def solution(mesh):
    tok_spec = P(('pod', 'data'), 'model', None)

    def device_step(x_loc, dy_loc, w_q, w_k, w_v, w_o):
        any_spec = pl.BlockSpec(memory_space=pl.ANY)
        vmem_spec = pl.BlockSpec(memory_space=pltpu.VMEM)
        outs = (((BLK, DIM), BF16), ((CH * NH, HD), F32), ((KC, HD), F32), ((KC, HD), F32), ((HE, CH), F32))
        dx, dwq, dwk, dwv, dwo = pl.pallas_call(
            step_kernel,
            out_shape=tuple(pltpu.VMEM(shape, dtype) for shape, dtype in outs),
            in_specs=[any_spec] * 6,
            out_specs=[vmem_spec] * 5,
            scratch_shapes=[
                pltpu.VMEM((SEQ, DIM), BF16),
                pltpu.VMEM((SEQ, DIM), BF16),
                pltpu.VMEM((2, WR, HD), BF16),
                pltpu.VMEM((WR, HD), F32),
                pltpu.VMEM((DIM, QKV), BF16),
                pltpu.VMEM((HE, DIM), BF16),
                pltpu.VMEM((SEQ, QKV), BF16),
                pltpu.VMEM((HD, SEQ), BF16),
                pltpu.VMEM((HD, SEQ), BF16),
                pltpu.VMEM((NH, CAUSAL_ROWS, BLK), F32),
                pltpu.VMEM((SEQ, BLK), BF16),
                pltpu.VMEM((HE, SEQ), BF16),
                pltpu.VMEM((SEQ, HE), BF16),
                pltpu.VMEM((QKV, SEQ), BF16),
                pltpu.VMEM((SEQ, QKV), BF16),
                pltpu.VMEM((SEQ, 2 * HD), F32),
                pltpu.VMEM((4, HE, CH), F32),
                pltpu.VMEM((2 * HD, DIM // 2), F32),
                pltpu.VMEM((2 * HD, DIM // 2), BF16),
                pltpu.VMEM((2 * HD, DIM // 2), BF16),
                pltpu.VMEM((2, 3, 2, NH, HD, SC), BF16),
                pltpu.VMEM((2, 3, 2, NH, HD, SC), BF16),
                pltpu.VMEM((3, 2 * HD, KC), BF16),
                pltpu.VMEM((3, 2 * HD, KC), BF16),
                pltpu.VMEM((2, BLK, DIM), BF16),
                pltpu.VMEM((2, BLK, DIM), BF16),
                pltpu.VMEM((BLK, DIM), BF16),
                pltpu.VMEM((BLK, DIM), BF16),
                pltpu.VMEM((SEQ, 3 * CH), BF16),
                pltpu.VMEM((AH * HD, SEQ), BF16),
                pltpu.SemaphoreType.DMA((N_SEM,)),
                pltpu.SemaphoreType.DMA((N_SEM,)),
                pltpu.SemaphoreType.DMA((7,)),
            ],
            compiler_params=pltpu.CompilerParams(collective_id=0, has_side_effects=True, vmem_limit_bytes=VMEM_LIMIT),
        )(x_loc, dy_loc, w_q.reshape(DIM * NH, HD), w_k, w_v, w_o.reshape(HE, DIM))
        dx, dwq, dwk, dwv, dwo = pl.pallas_call(
            store_kernel,
            out_shape=tuple(jax.ShapeDtypeStruct(shape, dtype) for shape, dtype in outs),
            in_specs=[any_spec] * 5,
            out_specs=[any_spec] * 5,
            scratch_shapes=[pltpu.SemaphoreType.DMA((5,))],
            compiler_params=pltpu.CompilerParams(vmem_limit_bytes=2 ** 20),
        )(dx, dwq, dwk, dwv, dwo)
        return dx.reshape(1, BLK, DIM), dwq.reshape(CH, NH, HD), dwk, dwv, dwo.reshape(NH, HD, CH)

    kv_rows = P(('pod', 'model', 'data'), None)
    return jax.shard_map(device_step, mesh=mesh,
                         in_specs=(tok_spec, tok_spec, P(None, 'model', None), P(), P(), P('model', None, None)),
                         out_specs=(tok_spec, P(('pod', 'data'), 'model', None), kv_rows, kv_rows, P(('pod', 'model'), None, 'data')),
                         check_vma=False)
```

```python
import functools
import math

import jax
import jax.numpy as jnp
from jax import lax
from jax.experimental import pallas as pl
from jax.experimental.pallas import tpu as pltpu
from jax.sharding import PartitionSpec as P

MESH = pl.DeviceIdType.MESH
F32 = jnp.float32
BF16 = jnp.bfloat16

SEQ = 1024
BLK = 256
DIM = 2048
HD = 128
NH = 4
HE = NH * HD
QKV = HE + 2 * HD
CH = 512
SC = CH // 2
WR = 1024
KC = 256
NX = 4
XR = BLK // NX
NB = SEQ // BLK
CAUSAL_ROWS = BLK * NB * (NB + 1) // 2

S_XY, S_XF, S_XC = 0, 4, 8
S_DY, S_DF, S_DC = 9, 14, 19
S_KP = 20
S_PX = 21
S_PY = 23
S_XN, S_XNC, S_XNF, S_XNG = 25, 26, 27, 28
S_A = 29
S_WO = 33
S_WQ = 81
S_KV = 105
N_SEM = 111
VMEM_LIMIT = 63 * 2 ** 20 - 3328 * 1024


def nn(a, b):
    return lax.dot_general(a, b, (((1,), (0,)), ((), ())), preferred_element_type=F32)


def nt(a, b):
    return lax.dot_general(a, b, (((1,), (1,)), ((), ())), preferred_element_type=F32)


def step_kernel(x_in, dy_in, wq_in, wk_in, wv_in, wo_in, dxo, wqo, dko, dvo, woo,
                xg, dyg, wq8, wst, wqkv, wo, qkv, kt, vt, prob, pbuf, ot, dout, at, am, dkv, pw, pkv,
                kvs, kvr, so, ro, sq, rq, skv, rkv, sx, rx, sy, ry, xn, abuf, ssem, rsem, lsem):
    pod = lax.axis_index("pod")
    z = lax.axis_index("data")
    m = lax.axis_index("model")
    y = m // 2
    c = m % 2
    core_m = 2 * y + 1 - c
    far_m = (m + 2) % 4
    diag_m = (core_m + 2) % 4
    core_dev = (pod, z, core_m)
    far_dev = (pod, z, far_m)

    inner = ((z + 1) // 2) % 2
    pair_dev = (pod, z + 1 - 2 * (z % 2), m)
    other_dev = (pod, 3 - z, m)
    x_off = CH * (1 - z // 2)

    def rows(block, n=BLK, off=0):
        return pl.ds(pl.multiple_of(block * BLK + off, n), n)

    def chunk(i):
        return i + (1 - z // 2) * (3 - 2 * i)

    def col(i):
        return pl.ds(pl.multiple_of(chunk(i) * CH, CH), CH)

    def dcol(i):
        if i < 2:
            return pl.ds(pl.multiple_of(chunk(0) * CH + i * SC, SC), SC)
        return col(i - 1)

    def remote(src, dst, sem, dev):
        return pltpu.make_async_remote_copy(src_ref=src, dst_ref=dst, send_sem=ssem.at[sem], recv_sem=rsem.at[sem],
                                            device_id=dev, device_id_type=MESH)

    def head_rows(h):
        return pl.ds(pl.multiple_of(h * HD, HD), HD)

    loads = [
        pltpu.make_async_copy(x_in.at[0], xg.at[rows(m)], lsem.at[0]),
        pltpu.make_async_copy(dy_in.at[0], dyg.at[rows(m)], lsem.at[1]),
        pltpu.make_async_copy(wk_in.at[y], wqkv.at[:, pl.ds(HE, HD)], lsem.at[2]),
        pltpu.make_async_copy(wv_in.at[y], wqkv.at[:, pl.ds(HE + HD, HD)], lsem.at[3]),
        pltpu.make_async_copy(wo_in, wo, lsem.at[4]),
    ]
    def wq_load(i):
        return pltpu.make_async_copy(wq_in.at[pl.ds(pl.multiple_of(i * WR, WR), WR)], wq8.at[i % 2], lsem.at[5 + i % 2])

    for ld in loads:
        ld.start()
    wq_load(0).start()
    wq_load(1).start()

    barrier = pltpu.get_barrier_semaphore()
    for dev in (far_dev, core_dev, pair_dev):
        pl.semaphore_signal(barrier, inc=1, device_id=dev, device_id_type=MESH)

    @pl.when(inner == 1)
    def _():
        pl.semaphore_signal(barrier, inc=1, device_id=other_dev, device_id_type=MESH)

    pl.semaphore_wait(barrier, 3 + inner)

    def x_far(i, block):
        r = rows(block, XR, i * XR)
        return remote(xg.at[r], xg.at[r], S_XY + i, far_dev)

    def x_fwd(i, block):
        r = rows(block, XR, i * XR)
        return remote(xg.at[r], xg.at[r], S_XF + i, core_dev)

    def x_core(block):
        return remote(xg.at[rows(block)], xg.at[rows(block)], S_XC, core_dev)

    def dy_far(i, block):
        return remote(dyg.at[rows(block), dcol(i)], dyg.at[rows(block), dcol(i)], S_DY + i, far_dev)

    def dy_fwd(i, block):
        return remote(dyg.at[rows(block), dcol(i)], dyg.at[rows(block), dcol(i)], S_DF + i, core_dev)

    def dy_core(block):
        return remote(dyg.at[rows(block)], dyg.at[rows(block)], S_DC, core_dev)

    def xn_edge(block):
        return remote(xg.at[rows(block), pl.ds(pl.multiple_of(x_off, CH), 3 * CH)], xn.at[rows(block)], S_XN, pair_dev)

    def xn_send(block, sem, dev):
        return remote(xn.at[rows(block)], xn.at[rows(block)], sem, dev)

    loads[0].wait()
    for i in range(NX):
        x_far(i, m).start()

    @pl.when(inner == 0)
    def _():
        xn_edge(m).start()

    x_core(m).start()
    loads[1].wait()
    for i in range(5):
        dy_far(i, m).start()
    dy_core(m).start()
    for ld in loads[2:]:
        ld.wait()

    def wq_block(i, carry):
        wq_load(i).wait()
        wst[...] = wq8[i % 2].astype(F32)

        @pl.when(i + 2 < DIM * NH // WR)
        def _():
            wq_load(i + 2).start()

        for h in range(NH):
            wqkv[pl.ds(pl.multiple_of(i * (WR // NH), WR // NH), WR // NH), pl.ds(h * HD, HD)] = wst[pl.ds(h, WR // NH, stride=NH), :].astype(BF16)
        return carry

    lax.fori_loop(0, DIM * NH // WR, wq_block, 0)

    def project(r):
        qkv[r, :] = nn(xg[r, :], wqkv[...]).astype(BF16)

    def flip(block):
        r = rows(block)
        kt[:, r] = qkv[r, pl.ds(HE, HD)].T
        vt[:, r] = qkv[r, pl.ds(HE + HD, HD)].T

    project(rows(m))
    x_core(core_m).wait_recv()
    project(rows(core_m))
    flip(m)
    flip(core_m)

    def x_piece(i, carry):
        x_far(i, far_m).wait_recv()
        x_fwd(i, far_m).start()
        project(rows(far_m, XR, i * XR))
        x_fwd(i, diag_m).wait_recv()
        project(rows(diag_m, XR, i * XR))
        return carry

    lax.fori_loop(0, NX, x_piece, 0)

    flip(far_m)
    flip(diag_m)
    dy_core(core_m).wait_recv()

    def take_dy(i):
        dy_far(i, far_m).wait_recv()
        dy_fwd(i, far_m).start()

    def wo_sem(slot, s, h):
        return S_WO + slot * 8 + s * 4 + h

    def wo_edge(k, s, h):
        return remote(so.at[k, s, h], ro.at[k, s, h], wo_sem(k, s, h), pair_dev)

    def wo_swap(k, s, h):
        return remote(so.at[k, s, h], ro.at[3 + k, s, h], wo_sem(3 + k, s, h), other_dev)

    def wo_back(s, h):
        return remote(so.at[2, s, h], ro.at[3, s, h], wo_sem(5, s, h), pair_dev)

    def half_col(s):
        return pl.ds(s * SC, SC)

    def wo_first(s, h):
        v = nn(ot[head_rows(h), :], dyg[:, dcol(s)])

        @pl.when(inner == 0)
        def _():
            so[0, s, h] = v.astype(BF16)
            wo_edge(0, s, h).start()

        @pl.when(inner == 1)
        def _():
            pw[0, head_rows(h), half_col(s)] = v

    @pl.when(inner == 1)
    def _():
        xn_edge(m).wait_recv()
        xn_send(m, S_XNF, far_dev).start()
        xn_send(m, S_XNC, core_dev).start()

    scale = HD ** -0.5
    exp_scale = scale * math.log2(math.e)
    diag_mask = lax.broadcasted_iota(jnp.int32, (BLK, BLK), 0) <= lax.broadcasted_iota(jnp.int32, (BLK, BLK), 1)

    def prow(qi, kj):
        return pl.ds(BLK * (qi * (qi + 1) // 2 + kj), BLK)

    def fwd_head(h, carry):
        hr = head_rows(h)
        for qi in range(NB):
            qb = qkv[pl.ds(qi * BLK, BLK), hr]
            mx = None
            for kj in range(qi + 1):
                s = nt(qkv[pl.ds(kj * BLK, BLK), pl.ds(HE, HD)], qb)
                if kj == qi:
                    s = jnp.where(diag_mask, s, -jnp.inf)
                prob[h, prow(qi, kj), :] = s
                bm = jnp.max(s, axis=0, keepdims=True)
                mx = bm if mx is None else jnp.maximum(mx, bm)
            tot = None
            for kj in range(qi + 1):
                e = jnp.exp2((prob[h, prow(qi, kj), :] - mx) * exp_scale)
                prob[h, prow(qi, kj), :] = e
                bs = jnp.sum(e, axis=0, keepdims=True)
                tot = bs if tot is None else tot + bs
            inv = 1.0 / tot
            for kj in range(qi + 1):
                p = prob[h, prow(qi, kj), :] * inv
                prob[h, prow(qi, kj), :] = p
                pbuf[pl.ds(kj * BLK, BLK), :] = p.astype(BF16)
            n = (qi + 1) * BLK
            ot[hr, pl.ds(qi * BLK, BLK)] = nn(vt[:, pl.ds(0, n)], pbuf[pl.ds(0, n), :]).astype(BF16)
            for at_h, at_q, piece in ((0, 2, 0), (1, 1, 1), (3, 0, 2)):
                if qi == at_q:
                    @pl.when(h == at_h)
                    def _(piece=piece):
                        take_dy(piece)

        @pl.when(h == 0)
        def _():
            dy_fwd(0, diag_m).wait_recv()

        wo_first(0, h)

        @pl.when(h == 1)
        def _():
            dy_fwd(1, diag_m).wait_recv()
            wo_first(1, 0)

        @pl.when(h >= 1)
        def _():
            wo_first(1, h)

        return carry

    lax.fori_loop(0, NH, fwd_head, 0)

    def wo_pass(k, h):
        for s in range(2):
            wo_edge(k, s, h).wait_recv()
            so[k, s, h] = (pw[k, head_rows(h), half_col(s)] + ro[k, s, h].astype(F32)).astype(BF16)
            wo_swap(k, s, h).start()

    def wo_return(h):
        for s in range(2):
            wo_swap(0, s, h).wait_recv()
            so[2, s, h] = (pw[3, head_rows(h), half_col(s)] + ro[3, s, h].astype(F32)).astype(BF16)
            wo_back(s, h).start()

    def wo_send(k):
        for h in range(NH):
            for s in range(2):
                so[k, s, h] = pw[k, head_rows(h), half_col(s)].astype(BF16)
                wo_edge(k, s, h).start()

    for i in range(1, 4):
        if i > 1:
            take_dy(i + 1)
        dy_fwd(i + 1, diag_m).wait_recv()
        pw[i] = nn(ot[...], dyg[:, col(i)])
        if i < 3:
            @pl.when(inner == 0)
            def _(i=i):
                wo_send(i)

            @pl.when(inner == 1)
            def _(i=i):
                for h in (2 * i - 2, 2 * i - 1):
                    wo_pass(0, h)

    def a_copy(h):
        r = head_rows(h)
        return remote(at.at[r], abuf.at[r], S_A + h, pair_dev)

    def wq_swap(k, s, h):
        return remote(sq.at[k, s, h], rq.at[k, s, h], S_WQ + k * 8 + s * 4 + h, other_dev)

    def wq_back(s, h):
        return remote(sq.at[2, s, h], rq.at[2, s, h], S_WQ + 16 + s * 4 + h, pair_dev)

    def ncol(k):
        return pl.ds(pl.multiple_of(chunk(k) * CH - x_off, CH), CH)

    def spot(k, s, h=0, n=1):
        return prob.at[1 + k // 2, pl.ds(((k % 2) * 2 + s) * HE + h * HD, n * HD)]

    def wq_own(k, q):
        v = nn(at[pl.ds(0, HE), :], xg[:, pl.ds(pl.multiple_of(q * CH, CH), CH)])
        for s in range(2):
            spot(k, s, 0, NH)[...] = v[:, s * SC:(s + 1) * SC]

    def combine(h):
        a_copy(h).wait_recv()
        for k in range(2):
            v = nn(abuf[head_rows(h), :], xn[:, ncol(k)])
            for s in range(2):
                sq[k, s, h] = (spot(k, s, h)[...] + v[:, s * SC:(s + 1) * SC]).astype(BF16)
                wq_swap(k, s, h).start()

    def outer(h):
        for s in range(2):
            wq_swap(0, s, h).wait_recv()
            sq[2, s, h] = (spot(3, s, h)[...] + rq[0, s, h].astype(F32)).astype(BF16)
            wq_back(s, h).start()

    def dout_block(b, carry):
        r = rows(b)
        dout[r, :] = nt(dyg[r, :], wo[...]).astype(BF16)
        return carry

    lax.fori_loop(0, NB, dout_block, 0)

    dkv[...] = jnp.zeros_like(dkv)

    def bwd_head(h, carry):
        hr = head_rows(h)
        for qi in range(NB):
            qr = pl.ds(qi * BLK, BLK)
            dob = dout[qr, hr]
            qb = qkv[qr, hr]
            delta = jnp.sum(dob.astype(F32).T * ot[hr, qr].astype(F32), axis=0, keepdims=True)
            for kj in range(qi + 1):
                kr = pl.ds(kj * BLK, BLK)
                p = prob[h, prow(qi, kj), :]
                dp = nt(qkv[kr, pl.ds(HE + HD, HD)], dob)
                ds = (p * (dp - delta)).astype(BF16)
                pbuf[kr, :] = ds
                dkv[kr, pl.ds(0, HD)] += nn(ds, qb)
                dkv[kr, pl.ds(HD, HD)] += nn(p.astype(BF16), dob)
            n = (qi + 1) * BLK
            dq = (nn(kt[:, pl.ds(0, n)], pbuf[pl.ds(0, n), :]) * scale).astype(BF16)
            at[hr, qr] = dq
            am[qr, hr] = dq.T

        @pl.when(inner == 0)
        def _():
            a_copy(h).start()

        @pl.when(inner == 1)
        def _():
            wo_pass(1, h)
            wo_return(h)

        return carry

    lax.fori_loop(0, NH, bwd_head, 0)

    dkb = (dkv[:, pl.ds(0, HD)] * scale).astype(BF16)
    dvb = dkv[:, pl.ds(HD, HD)].astype(BF16)
    am[:, pl.ds(HE, HD)] = dkb
    am[:, pl.ds(HE + HD, HD)] = dvb
    at[pl.ds(HE, HD), :] = dkb.T
    at[pl.ds(HE + HD, HD), :] = dvb.T

    def dx_part(block, put):
        def piece(i, carry):
            cs = pl.ds(pl.multiple_of(i * CH, CH), CH)
            put(i, cs, nt(am[rows(block), :], wqkv[cs, :]))
            return carry

        lax.fori_loop(0, DIM // CH, piece, 0)

    def px_copy(i):
        return remote(sx.at[i], rx.at[i], S_PX + i, core_dev)

    def py_copy(i):
        r = pl.ds(i * (BLK // 2), BLK // 2)
        return remote(sy.at[r], ry.at[r], S_PY + i, far_dev)

    def put_sx(j):
        def put(i, cs, v):
            sx[j, :, cs] = v.astype(BF16)
        return put

    def pxo(i, s):
        return prob.at[0, pl.ds(pl.multiple_of((2 * i + s) * BLK, BLK), BLK)]

    def put_own(i, cs, v):
        for s in range(2):
            pxo(i, s)[...] = v[:, s * SC:(s + 1) * SC]

    half = DIM // 2

    def kv_half(which):
        return nn(at[pl.ds(HE, 2 * HD), :], xg[:, pl.ds(pl.multiple_of(which * half, half), half)])

    def kcol(k):
        return pl.ds(pl.multiple_of(chunk(k) * KC, KC), KC)

    def kv_edge(k):
        return remote(skv.at[k], rkv.at[k], S_KV + k, pair_dev)

    def kv_swap(k):
        return remote(skv.at[k], rkv.at[3 + k], S_KV + 3 + k, other_dev)

    def kv_back():
        return remote(skv.at[2], rkv.at[3], S_KV + 5, pair_dev)

    def kv_pass(k):
        kv_edge(k).wait_recv()
        skv[k] = (pkv[:, kcol(k)] + rkv[k].astype(F32)).astype(BF16)
        kv_swap(k).start()

    kvs[...] = kv_half(1 - c).astype(BF16)
    kp_copy = remote(kvs, kvr, S_KP, core_dev)
    kp_copy.start()
    dx_part(diag_m, put_sx(0))
    px_copy(0).start()
    pkv[...] = kv_half(c)
    kp_copy.wait_recv()
    pkv[...] += kvr[...].astype(F32)

    @pl.when(inner == 0)
    def _():
        for k in range(3):
            skv[k] = pkv[:, kcol(k)].astype(BF16)
            kv_edge(k).start()
    @pl.when(inner == 1)
    def _():
        xn_send(far_m, S_XNF, far_dev).wait_recv()
        xn_send(far_m, S_XNG, core_dev).start()
        wq_own(0, chunk(0))
        wq_own(1, chunk(1))

    dx_part(far_m, put_own)
    px_copy(0).wait_recv()
    for i in range(2):
        r = pl.ds(i * (BLK // 2), BLK // 2)
        for j in range(DIM // SC):
            cs = pl.ds(j * SC, SC)
            own = prob[0, pl.ds(j * BLK + i * (BLK // 2), BLK // 2), :]
            sy[r, cs] = (own + rx[0, r, cs].astype(F32)).astype(BF16)
        py_copy(i).start()

    @pl.when(inner == 1)
    def _():
        xn_send(core_m, S_XNC, core_dev).wait_recv()
        xn_send(diag_m, S_XNG, core_dev).wait_recv()
        combine(0)
        wq_own(3, chunk(3))
        combine(1)
        outer(0)

    dx_part(core_m, put_sx(1))
    px_copy(1).start()
    dx_part(m, put_own)
    wq_own(2, z)

    @pl.when(inner == 1)
    def _():
        combine(2)
        outer(1)
        combine(3)
        outer(2)
        kv_pass(0)
        v = nn(abuf[...], xn[:, ncol(2)])
        for s in range(2):
            spot(2, s, 0, NH)[...] += v[:, s * SC:(s + 1) * SC]
        outer(3)
        kv_pass(1)
        kv_swap(0).wait_recv()
        skv[2] = (pkv[:, kcol(3)] + rkv[3].astype(F32)).astype(BF16)
        kv_back().start()
        for h in range(NH):
            for s in range(2):
                wo_edge(2, s, h).wait_recv()
                wo_swap(1, s, h).wait_recv()
                woo[head_rows(h), half_col(s)] = pw[2, head_rows(h), half_col(s)] + ro[2, s, h].astype(F32) + ro[4, s, h].astype(F32)

    @pl.when(inner == 0)
    def _():
        for h in range(NH):
            for s in range(2):
                wo_back(s, h).wait_recv()
                woo[head_rows(h), half_col(s)] = pw[3, head_rows(h), half_col(s)] + ro[3, s, h].astype(F32)

    px_copy(1).wait_recv()
    for i in range(2):
        r = pl.ds(i * (BLK // 2), BLK // 2)
        py_copy(i).wait_recv()
        for j in range(DIM // SC):
            cs = pl.ds(j * SC, SC)
            own = prob[0, pl.ds(j * BLK + i * (BLK // 2), BLK // 2), :]
            dxo[r, cs] = (own + rx[1, r, cs].astype(F32) + ry[r, cs].astype(F32)).astype(BF16)

    def wq_put(h, s, got):
        wqo[pl.ds(s * SC * NH + h, SC, stride=NH), :] = (spot(2, s, h)[...] + got.astype(F32)).T

    def kv_put(v):
        dko[...] = v[:HD].T
        dvo[...] = v[HD:].T

    @pl.when(inner == 1)
    def _():
        for h in range(NH):
            for s in range(2):
                wq_swap(1, s, h).wait_recv()
                wq_put(h, s, rq[1, s, h])
        kv_edge(2).wait_recv()
        kv_swap(1).wait_recv()
        kv_put(pkv[:, kcol(2)] + rkv[2].astype(F32) + rkv[4].astype(F32))

    @pl.when(inner == 0)
    def _():
        for h in range(NH):
            for s in range(2):
                wq_back(s, h).wait_recv()
                wq_put(h, s, rq[2, s, h])
        kv_back().wait_recv()
        kv_put(pkv[:, kcol(3)] + rkv[3].astype(F32))

    for i in range(NX):
        x_far(i, m).wait_send()
        x_fwd(i, far_m).wait_send()
    x_core(m).wait_send()
    for i in range(5):
        dy_far(i, m).wait_send()
        dy_fwd(i, far_m).wait_send()
    dy_core(m).wait_send()
    @pl.when(inner == 0)
    def _():
        xn_edge(m).wait_send()
        for h in range(NH):
            a_copy(h).wait_send()
        for k in range(3):
            kv_edge(k).wait_send()
            for s in range(2):
                for h in range(NH):
                    wo_edge(k, s, h).wait_send()

    @pl.when(inner == 1)
    def _():
        xn_send(m, S_XNF, far_dev).wait_send()
        xn_send(m, S_XNC, core_dev).wait_send()
        xn_send(far_m, S_XNG, core_dev).wait_send()
        for k in range(2):
            kv_swap(k).wait_send()
        kv_back().wait_send()
        for s in range(2):
            for h in range(NH):
                for k in range(2):
                    wo_swap(k, s, h).wait_send()
                    wq_swap(k, s, h).wait_send()
                wo_back(s, h).wait_send()
                wq_back(s, h).wait_send()

    kp_copy.wait_send()
    for i in range(2):
        px_copy(i).wait_send()
        py_copy(i).wait_send()


def store_kernel(*refs):
    n = len(refs) // 2
    sem = refs[-1]
    copies = [pltpu.make_async_copy(refs[i], refs[n + i], sem.at[i]) for i in range(n)]
    for cp in copies:
        cp.start()
    for cp in copies:
        cp.wait()


def solution(mesh):
    tok_spec = P(('pod', 'data'), 'model', None)

    def device_step(x_loc, dy_loc, w_q, w_k, w_v, w_o):
        any_spec = pl.BlockSpec(memory_space=pl.ANY)
        vmem_spec = pl.BlockSpec(memory_space=pltpu.VMEM)
        outs = (((BLK, DIM), BF16), ((CH * NH, HD), F32), ((KC, HD), F32), ((KC, HD), F32), ((HE, CH), F32))
        dx, dwq, dwk, dwv, dwo = pl.pallas_call(
            step_kernel,
            out_shape=tuple(pltpu.VMEM(shape, dtype) for shape, dtype in outs),
            in_specs=[any_spec] * 6,
            out_specs=[vmem_spec] * 5,
            scratch_shapes=[
                pltpu.VMEM((SEQ, DIM), BF16),
                pltpu.VMEM((SEQ, DIM), BF16),
                pltpu.VMEM((2, WR, HD), BF16),
                pltpu.VMEM((WR, HD), F32),
                pltpu.VMEM((DIM, QKV), BF16),
                pltpu.VMEM((HE, DIM), BF16),
                pltpu.VMEM((SEQ, QKV), BF16),
                pltpu.VMEM((HD, SEQ), BF16),
                pltpu.VMEM((HD, SEQ), BF16),
                pltpu.VMEM((NH, CAUSAL_ROWS, BLK), F32),
                pltpu.VMEM((SEQ, BLK), BF16),
                pltpu.VMEM((HE, SEQ), BF16),
                pltpu.VMEM((SEQ, HE), BF16),
                pltpu.VMEM((QKV, SEQ), BF16),
                pltpu.VMEM((SEQ, QKV), BF16),
                pltpu.VMEM((SEQ, 2 * HD), F32),
                pltpu.VMEM((4, HE, CH), F32),
                pltpu.VMEM((2 * HD, DIM // 2), F32),
                pltpu.VMEM((2 * HD, DIM // 2), BF16),
                pltpu.VMEM((2 * HD, DIM // 2), BF16),
                pltpu.VMEM((3, 2, NH, HD, SC), BF16),
                pltpu.VMEM((5, 2, NH, HD, SC), BF16),
                pltpu.VMEM((3, 2, NH, HD, SC), BF16),
                pltpu.VMEM((3, 2, NH, HD, SC), BF16),
                pltpu.VMEM((3, 2 * HD, KC), BF16),
                pltpu.VMEM((5, 2 * HD, KC), BF16),
                pltpu.VMEM((2, BLK, DIM), BF16),
                pltpu.VMEM((2, BLK, DIM), BF16),
                pltpu.VMEM((BLK, DIM), BF16),
                pltpu.VMEM((BLK, DIM), BF16),
                pltpu.VMEM((SEQ, 3 * CH), BF16),
                pltpu.VMEM((HE, SEQ), BF16),
                pltpu.SemaphoreType.DMA((N_SEM,)),
                pltpu.SemaphoreType.DMA((N_SEM,)),
                pltpu.SemaphoreType.DMA((7,)),
            ],
            compiler_params=pltpu.CompilerParams(collective_id=0, has_side_effects=True, vmem_limit_bytes=VMEM_LIMIT),
        )(x_loc, dy_loc, w_q.reshape(DIM * NH, HD), w_k, w_v, w_o.reshape(HE, DIM))
        dx, dwq, dwk, dwv, dwo = pl.pallas_call(
            store_kernel,
            out_shape=tuple(jax.ShapeDtypeStruct(shape, dtype) for shape, dtype in outs),
            in_specs=[any_spec] * 5,
            out_specs=[any_spec] * 5,
            scratch_shapes=[pltpu.SemaphoreType.DMA((5,))],
            compiler_params=pltpu.CompilerParams(vmem_limit_bytes=2 ** 20),
        )(dx, dwq, dwk, dwv, dwo)
        return dx.reshape(1, BLK, DIM), dwq.reshape(CH, NH, HD), dwk, dwv, dwo.reshape(NH, HD, CH)

    kv_rows = P(('pod', 'model', 'data'), None)
    return jax.shard_map(device_step, mesh=mesh,
                         in_specs=(tok_spec, tok_spec, P(None, 'model', None), P(), P(), P('model', None, None)),
                         out_specs=(tok_spec, P(('pod', 'data'), 'model', None), kv_rows, kv_rows, P(('pod', 'model'), None, 'data')),
                         check_vma=False)
```

```python
import functools
import math

import jax
import jax.numpy as jnp
from jax import lax
from jax.experimental import pallas as pl
from jax.experimental.pallas import tpu as pltpu
from jax.sharding import PartitionSpec as P

MESH = pl.DeviceIdType.MESH
F32 = jnp.float32
BF16 = jnp.bfloat16

SEQ = 1024
BLK = 256
DIM = 2048
HD = 128
NH = 4
HE = NH * HD
QKV = HE + 2 * HD
CH = 512
SC = CH // 2
WR = 1024
KC = 256
NX = 4
XR = BLK // NX
NB = SEQ // BLK
CAUSAL_ROWS = BLK * NB * (NB + 1) // 2

S_XY, S_XF, S_XC = 0, 4, 8
S_DY, S_DF, S_DC = 9, 14, 19
S_KP = 20
S_PX = 21
S_PY = 23
S_XN, S_XNC, S_XNF, S_XNG = 25, 26, 27, 28
S_A = 29
S_WO = 33
S_WQ = 81
S_KV = 105
N_SEM = 117
VMEM_LIMIT = 63 * 2 ** 20 - 3328 * 1024


def nn(a, b):
    return lax.dot_general(a, b, (((1,), (0,)), ((), ())), preferred_element_type=F32)


def nt(a, b):
    return lax.dot_general(a, b, (((1,), (1,)), ((), ())), preferred_element_type=F32)


def step_kernel(x_in, dy_in, wq_in, wk_in, wv_in, wo_in, dxo, wqo, dko, dvo, woo,
                xg, dyg, wq8, wst, wqkv, wo, qkv, kt, vt, prob, pbuf, ot, dout, at, am, dkv, pw, pkv,
                kvs, kvr, so, ro, sq, rq, skv, rkv, sx, rx, sy, ry, xn, abuf, ssem, rsem, lsem):
    pod = lax.axis_index("pod")
    z = lax.axis_index("data")
    m = lax.axis_index("model")
    y = m // 2
    c = m % 2
    core_m = 2 * y + 1 - c
    far_m = (m + 2) % 4
    diag_m = (core_m + 2) % 4
    core_dev = (pod, z, core_m)
    far_dev = (pod, z, far_m)

    inner = ((z + 1) // 2) % 2
    pair_dev = (pod, z + 1 - 2 * (z % 2), m)
    other_dev = (pod, 3 - z, m)
    x_off = CH * (1 - z // 2)

    def rows(block, n=BLK, off=0):
        return pl.ds(pl.multiple_of(block * BLK + off, n), n)

    def chunk(i):
        return i + (1 - z // 2) * (3 - 2 * i)

    def col(i):
        return pl.ds(pl.multiple_of(chunk(i) * CH, CH), CH)

    def dcol(i):
        if i < 2:
            return pl.ds(pl.multiple_of(chunk(0) * CH + i * SC, SC), SC)
        return col(i - 1)

    def remote(src, dst, sem, dev):
        return pltpu.make_async_remote_copy(src_ref=src, dst_ref=dst, send_sem=ssem.at[sem], recv_sem=rsem.at[sem],
                                            device_id=dev, device_id_type=MESH)

    def head_rows(h):
        return pl.ds(pl.multiple_of(h * HD, HD), HD)

    loads = [
        pltpu.make_async_copy(x_in.at[0], xg.at[rows(m)], lsem.at[0]),
        pltpu.make_async_copy(dy_in.at[0], dyg.at[rows(m)], lsem.at[1]),
        pltpu.make_async_copy(wk_in.at[y], wqkv.at[:, pl.ds(HE, HD)], lsem.at[2]),
        pltpu.make_async_copy(wv_in.at[y], wqkv.at[:, pl.ds(HE + HD, HD)], lsem.at[3]),
        pltpu.make_async_copy(wo_in, wo, lsem.at[4]),
    ]
    def wq_load(i):
        return pltpu.make_async_copy(wq_in.at[pl.ds(pl.multiple_of(i * WR, WR), WR)], wq8.at[i % 2], lsem.at[5 + i % 2])

    for ld in loads:
        ld.start()
    wq_load(0).start()
    wq_load(1).start()

    barrier = pltpu.get_barrier_semaphore()
    for dev in (far_dev, core_dev, pair_dev):
        pl.semaphore_signal(barrier, inc=1, device_id=dev, device_id_type=MESH)

    @pl.when(inner == 1)
    def _():
        pl.semaphore_signal(barrier, inc=1, device_id=other_dev, device_id_type=MESH)

    pl.semaphore_wait(barrier, 3 + inner)

    def x_far(i, block):
        r = rows(block, XR, i * XR)
        return remote(xg.at[r], xg.at[r], S_XY + i, far_dev)

    def x_fwd(i, block):
        r = rows(block, XR, i * XR)
        return remote(xg.at[r], xg.at[r], S_XF + i, core_dev)

    def x_core(block):
        return remote(xg.at[rows(block)], xg.at[rows(block)], S_XC, core_dev)

    def dy_far(i, block):
        return remote(dyg.at[rows(block), dcol(i)], dyg.at[rows(block), dcol(i)], S_DY + i, far_dev)

    def dy_fwd(i, block):
        return remote(dyg.at[rows(block), dcol(i)], dyg.at[rows(block), dcol(i)], S_DF + i, core_dev)

    def dy_core(block):
        return remote(dyg.at[rows(block)], dyg.at[rows(block)], S_DC, core_dev)

    def xn_edge(block):
        return remote(xg.at[rows(block), pl.ds(pl.multiple_of(x_off, CH), 3 * CH)], xn.at[rows(block)], S_XN, pair_dev)

    def xn_send(block, sem, dev):
        return remote(xn.at[rows(block)], xn.at[rows(block)], sem, dev)

    loads[0].wait()
    for i in range(NX):
        x_far(i, m).start()

    @pl.when(inner == 0)
    def _():
        xn_edge(m).start()

    x_core(m).start()
    loads[1].wait()
    for i in range(5):
        dy_far(i, m).start()
    dy_core(m).start()
    for ld in loads[2:]:
        ld.wait()

    def wq_block(i, carry):
        wq_load(i).wait()
        wst[...] = wq8[i % 2].astype(F32)

        @pl.when(i + 2 < DIM * NH // WR)
        def _():
            wq_load(i + 2).start()

        for h in range(NH):
            wqkv[pl.ds(pl.multiple_of(i * (WR // NH), WR // NH), WR // NH), pl.ds(h * HD, HD)] = wst[pl.ds(h, WR // NH, stride=NH), :].astype(BF16)
        return carry

    lax.fori_loop(0, DIM * NH // WR, wq_block, 0)

    def project(r):
        qkv[r, :] = nn(xg[r, :], wqkv[...]).astype(BF16)

    def flip(block):
        r = rows(block)
        kt[:, r] = qkv[r, pl.ds(HE, HD)].T
        vt[:, r] = qkv[r, pl.ds(HE + HD, HD)].T

    project(rows(m))
    x_core(core_m).wait_recv()
    project(rows(core_m))
    flip(m)
    flip(core_m)

    def x_piece(i, carry):
        x_far(i, far_m).wait_recv()
        x_fwd(i, far_m).start()
        project(rows(far_m, XR, i * XR))
        x_fwd(i, diag_m).wait_recv()
        project(rows(diag_m, XR, i * XR))
        return carry

    lax.fori_loop(0, NX, x_piece, 0)

    flip(far_m)
    flip(diag_m)
    dy_core(core_m).wait_recv()

    def take_dy(i):
        dy_far(i, far_m).wait_recv()
        dy_fwd(i, far_m).start()

    def wo_sem(slot, s, h):
        return S_WO + slot * 8 + s * 4 + h

    def wo_edge(k, s, h):
        return remote(so.at[k, s, h], ro.at[k, s, h], wo_sem(k, s, h), pair_dev)

    def wo_swap(k, s, h):
        return remote(so.at[k, s, h], ro.at[3 + k, s, h], wo_sem(3 + k, s, h), other_dev)

    def wo_back(s, h):
        return remote(so.at[2, s, h], ro.at[3, s, h], wo_sem(5, s, h), pair_dev)

    def half_col(s):
        return pl.ds(s * SC, SC)

    def wo_first(s, h):
        v = nn(ot[pl.ds(h * HD, HD), :], dyg[:, dcol(s)])

        @pl.when(inner == 0)
        def _():
            so[0, s, h] = v.astype(BF16)
            wo_edge(0, s, h).start()

        @pl.when(inner == 1)
        def _():
            pw[0, head_rows(h), half_col(s)] = v

    @pl.when(inner == 1)
    def _():
        xn_edge(m).wait_recv()
        xn_send(m, S_XNF, far_dev).start()
        xn_send(m, S_XNC, core_dev).start()

    scale = HD ** -0.5
    exp_scale = scale * math.log2(math.e)
    diag_mask = lax.broadcasted_iota(jnp.int32, (BLK, BLK), 0) <= lax.broadcasted_iota(jnp.int32, (BLK, BLK), 1)

    def prow(qi, kj):
        return pl.ds(BLK * (qi * (qi + 1) // 2 + kj), BLK)

    def fwd_head(h, first_q, last_q):
        hr = pl.ds(h * HD, HD)
        for qi in range(first_q, last_q):
            qb = qkv[pl.ds(qi * BLK, BLK), hr]
            mx = None
            for kj in range(qi + 1):
                s = nt(qkv[pl.ds(kj * BLK, BLK), pl.ds(HE, HD)], qb)
                if kj == qi:
                    s = jnp.where(diag_mask, s, -jnp.inf)
                prob[h, prow(qi, kj), :] = s
                bm = jnp.max(s, axis=0, keepdims=True)
                mx = bm if mx is None else jnp.maximum(mx, bm)
            tot = None
            for kj in range(qi + 1):
                e = jnp.exp2((prob[h, prow(qi, kj), :] - mx) * exp_scale)
                prob[h, prow(qi, kj), :] = e
                bs = jnp.sum(e, axis=0, keepdims=True)
                tot = bs if tot is None else tot + bs
            inv = 1.0 / tot
            for kj in range(qi + 1):
                p = prob[h, prow(qi, kj), :] * inv
                prob[h, prow(qi, kj), :] = p
                pbuf[pl.ds(kj * BLK, BLK), :] = p.astype(BF16)
            n = (qi + 1) * BLK
            ot[hr, pl.ds(qi * BLK, BLK)] = nn(vt[:, pl.ds(0, n)], pbuf[pl.ds(0, n), :]).astype(BF16)

    fwd_head(0, 0, 3)
    take_dy(0)
    fwd_head(0, 3, NB)
    dy_fwd(0, diag_m).wait_recv()
    wo_first(0, 0)
    fwd_head(1, 0, 3)
    take_dy(1)
    fwd_head(1, 3, NB)
    wo_first(0, 1)
    dy_fwd(1, diag_m).wait_recv()
    wo_first(1, 0)
    wo_first(1, 1)
    for h in range(2, NH):
        fwd_head(h, 0, 3)
        if h == 3:
            take_dy(2)
        fwd_head(h, 3, NB)
        for s in range(2):
            wo_first(s, h)

    def wo_pass(k, h):
        for s in range(2):
            wo_edge(k, s, h).wait_recv()
            so[k, s, h] = (pw[k, head_rows(h), half_col(s)] + ro[k, s, h].astype(F32)).astype(BF16)
            wo_swap(k, s, h).start()

    def wo_return(h):
        for s in range(2):
            wo_swap(0, s, h).wait_recv()
            so[2, s, h] = (pw[3, head_rows(h), half_col(s)] + ro[3, s, h].astype(F32)).astype(BF16)
            wo_back(s, h).start()

    def wo_send(k):
        for h in range(NH):
            for s in range(2):
                so[k, s, h] = pw[k, head_rows(h), half_col(s)].astype(BF16)
                wo_edge(k, s, h).start()

    for i in range(1, 4):
        if i > 1:
            take_dy(i + 1)
        dy_fwd(i + 1, diag_m).wait_recv()
        pw[i] = nn(ot[...], dyg[:, col(i)])
        if i < 3:
            @pl.when(inner == 0)
            def _(i=i):
                wo_send(i)

            @pl.when(inner == 1)
            def _(i=i):
                for h in (2 * i - 2, 2 * i - 1):
                    wo_pass(0, h)

    def a_copy(h):
        r = head_rows(h)
        return remote(at.at[r], abuf.at[r], S_A + h, pair_dev)

    def wq_swap(k, s, h):
        return remote(sq.at[k, s, h], rq.at[k, s, h], S_WQ + k * 8 + s * 4 + h, other_dev)

    def wq_back(s, h):
        return remote(sq.at[2, s, h], rq.at[2, s, h], S_WQ + 16 + s * 4 + h, pair_dev)

    def ncol(k):
        return pl.ds(pl.multiple_of(chunk(k) * CH - x_off, CH), CH)

    def spot(k, s, h=0, n=1):
        return prob.at[1 + k // 2, pl.ds(((k % 2) * 2 + s) * HE + h * HD, n * HD)]

    def wq_own(k, q):
        v = nn(at[pl.ds(0, HE), :], xg[:, pl.ds(pl.multiple_of(q * CH, CH), CH)])
        for s in range(2):
            spot(k, s, 0, NH)[...] = v[:, s * SC:(s + 1) * SC]

    def combine(h, ks=(0, 1)):
        if 0 in ks:
            a_copy(h).wait_recv()
        for k in ks:
            v = nn(abuf[head_rows(h), :], xn[:, ncol(k)])
            for s in range(2):
                sq[k, s, h] = (spot(k, s, h)[...] + v[:, s * SC:(s + 1) * SC]).astype(BF16)
                wq_swap(k, s, h).start()

    def outer(h):
        for s in range(2):
            wq_swap(0, s, h).wait_recv()
            sq[2, s, h] = (spot(3, s, h)[...] + rq[0, s, h].astype(F32)).astype(BF16)
            wq_back(s, h).start()

    def dout_block(b, carry):
        r = rows(b)
        dout[r, :] = nt(dyg[r, :], wo[...]).astype(BF16)
        return carry

    lax.fori_loop(0, NB, dout_block, 0)

    dkv[...] = jnp.zeros_like(dkv)

    def bwd_head(h, carry):
        hr = head_rows(h)
        for qi in range(NB):
            qr = pl.ds(qi * BLK, BLK)
            dob = dout[qr, hr]
            qb = qkv[qr, hr]
            delta = jnp.sum(dob.astype(F32).T * ot[hr, qr].astype(F32), axis=0, keepdims=True)
            for kj in range(qi + 1):
                kr = pl.ds(kj * BLK, BLK)
                p = prob[h, prow(qi, kj), :]
                dp = nt(qkv[kr, pl.ds(HE + HD, HD)], dob)
                ds = (p * (dp - delta)).astype(BF16)
                pbuf[kr, :] = ds
                dkv[kr, pl.ds(0, HD)] += nn(ds, qb)
                dkv[kr, pl.ds(HD, HD)] += nn(p.astype(BF16), dob)
            n = (qi + 1) * BLK
            dq = (nn(kt[:, pl.ds(0, n)], pbuf[pl.ds(0, n), :]) * scale).astype(BF16)
            at[hr, qr] = dq
            am[qr, hr] = dq.T

        @pl.when(inner == 0)
        def _():
            a_copy(h).start()

        @pl.when(inner == 1)
        def _():
            wo_pass(1, h)
            wo_return(h)

        return carry

    lax.fori_loop(0, NH, bwd_head, 0)

    dkb = (dkv[:, pl.ds(0, HD)] * scale).astype(BF16)
    dvb = dkv[:, pl.ds(HD, HD)].astype(BF16)
    am[:, pl.ds(HE, HD)] = dkb
    am[:, pl.ds(HE + HD, HD)] = dvb
    at[pl.ds(HE, HD), :] = dkb.T
    at[pl.ds(HE + HD, HD), :] = dvb.T

    def dx_part(block, put):
        def piece(i, carry):
            cs = pl.ds(pl.multiple_of(i * CH, CH), CH)
            put(i, cs, nt(am[rows(block), :], wqkv[cs, :]))
            return carry

        lax.fori_loop(0, DIM // CH, piece, 0)

    def px_copy(i):
        return remote(sx.at[i], rx.at[i], S_PX + i, core_dev)

    def py_copy(i):
        r = pl.ds(i * (BLK // 2), BLK // 2)
        return remote(sy.at[r], ry.at[r], S_PY + i, far_dev)

    def put_sx(j):
        def put(i, cs, v):
            sx[j, :, cs] = v.astype(BF16)
        return put

    def pxo(i, s):
        return prob.at[0, pl.ds(pl.multiple_of((2 * i + s) * BLK, BLK), BLK)]

    def put_own(i, cs, v):
        for s in range(2):
            pxo(i, s)[...] = v[:, s * SC:(s + 1) * SC]

    half = DIM // 2

    def kv_half(which):
        return nn(at[pl.ds(HE, 2 * HD), :], xg[:, pl.ds(pl.multiple_of(which * half, half), half)])

    def kcol(k):
        return pl.ds(pl.multiple_of(chunk(k) * KC, KC), KC)

    def kv_part(ref, slot, t):
        return ref.at[slot, pl.ds(t * HD, HD)]

    def kv_edge(k, t):
        return remote(kv_part(skv, k, t), kv_part(rkv, k, t), S_KV + 2 * k + t, pair_dev)

    def kv_swap(k, t):
        return remote(kv_part(skv, k, t), kv_part(rkv, 3 + k, t), S_KV + 2 * (3 + k) + t, other_dev)

    def kv_back(t):
        return remote(kv_part(skv, 2, t), kv_part(rkv, 3, t), S_KV + 10 + t, pair_dev)

    def kv_own(k, t):
        return pkv[pl.ds(t * HD, HD), kcol(k)]

    def kv_pass(k):
        for t in range(2):
            kv_edge(k, t).wait_recv()
            kv_part(skv, k, t)[...] = (kv_own(k, t) + kv_part(rkv, k, t)[...].astype(F32)).astype(BF16)
            kv_swap(k, t).start()

    kvs[...] = kv_half(1 - c).astype(BF16)
    kp_copy = remote(kvs, kvr, S_KP, core_dev)
    kp_copy.start()
    dx_part(diag_m, put_sx(0))
    px_copy(0).start()
    pkv[...] = kv_half(c)
    kp_copy.wait_recv()
    pkv[...] += kvr[...].astype(F32)

    @pl.when(inner == 0)
    def _():
        for k in range(3):
            for t in range(2):
                kv_part(skv, k, t)[...] = kv_own(k, t).astype(BF16)
                kv_edge(k, t).start()
    @pl.when(inner == 1)
    def _():
        xn_send(far_m, S_XNF, far_dev).wait_recv()
        xn_send(far_m, S_XNG, core_dev).start()
        wq_own(0, chunk(0))
        wq_own(1, chunk(1))

    dx_part(far_m, put_own)
    px_copy(0).wait_recv()
    for i in range(2):
        r = pl.ds(i * (BLK // 2), BLK // 2)
        for j in range(DIM // SC):
            cs = pl.ds(j * SC, SC)
            own = prob[0, pl.ds(j * BLK + i * (BLK // 2), BLK // 2), :]
            sy[r, cs] = (own + rx[0, r, cs].astype(F32)).astype(BF16)
        py_copy(i).start()

    @pl.when(inner == 1)
    def _():
        xn_send(core_m, S_XNC, core_dev).wait_recv()
        xn_send(diag_m, S_XNG, core_dev).wait_recv()
        combine(0)
        wq_own(3, chunk(3))
        combine(1)
        outer(0)

    dx_part(core_m, put_sx(1))
    px_copy(1).start()
    dx_part(m, put_own)
    wq_own(2, z)

    @pl.when(inner == 1)
    def _():
        combine(2)
        outer(1)
        combine(3, (0,))
        outer(2)
        v = nn(abuf[...], xn[:, ncol(2)])
        for s in range(2):
            spot(2, s, 0, NH)[...] += v[:, s * SC:(s + 1) * SC]
        kv_pass(0)
        combine(3, (1,))
        outer(3)
        kv_pass(1)
        for t in range(2):
            kv_swap(0, t).wait_recv()
            kv_part(skv, 2, t)[...] = (kv_own(3, t) + kv_part(rkv, 3, t)[...].astype(F32)).astype(BF16)
            kv_back(t).start()
        for h in range(NH):
            for s in range(2):
                wo_edge(2, s, h).wait_recv()
                wo_swap(1, s, h).wait_recv()
                woo[head_rows(h), half_col(s)] = pw[2, head_rows(h), half_col(s)] + ro[2, s, h].astype(F32) + ro[4, s, h].astype(F32)

    @pl.when(inner == 0)
    def _():
        for h in range(NH):
            for s in range(2):
                wo_back(s, h).wait_recv()
                woo[head_rows(h), half_col(s)] = pw[3, head_rows(h), half_col(s)] + ro[3, s, h].astype(F32)

    px_copy(1).wait_recv()
    for i in range(2):
        r = pl.ds(i * (BLK // 2), BLK // 2)
        py_copy(i).wait_recv()
        for j in range(DIM // SC):
            cs = pl.ds(j * SC, SC)
            own = prob[0, pl.ds(j * BLK + i * (BLK // 2), BLK // 2), :]
            dxo[r, cs] = (own + rx[1, r, cs].astype(F32) + ry[r, cs].astype(F32)).astype(BF16)

    def wq_put(h, s, got):
        wqo[pl.ds(s * SC * NH + h, SC, stride=NH), :] = (spot(2, s, h)[...] + got.astype(F32)).T

    kv_out = (dko, dvo)

    @pl.when(inner == 1)
    def _():
        for h in range(NH):
            for s in range(2):
                wq_swap(1, s, h).wait_recv()
                wq_put(h, s, rq[1, s, h])
        for t in range(2):
            kv_edge(2, t).wait_recv()
            kv_swap(1, t).wait_recv()
            kv_out[t][...] = (kv_own(2, t) + kv_part(rkv, 2, t)[...].astype(F32) + kv_part(rkv, 4, t)[...].astype(F32)).T

    @pl.when(inner == 0)
    def _():
        for h in range(NH):
            for s in range(2):
                wq_back(s, h).wait_recv()
                wq_put(h, s, rq[2, s, h])
        for t in range(2):
            kv_back(t).wait_recv()
            kv_out[t][...] = (kv_own(3, t) + kv_part(rkv, 3, t)[...].astype(F32)).T

    for i in range(NX):
        x_far(i, m).wait_send()
        x_fwd(i, far_m).wait_send()
    x_core(m).wait_send()
    for i in range(5):
        dy_far(i, m).wait_send()
        dy_fwd(i, far_m).wait_send()
    dy_core(m).wait_send()
    @pl.when(inner == 0)
    def _():
        xn_edge(m).wait_send()
        for h in range(NH):
            a_copy(h).wait_send()
        for k in range(3):
            for t in range(2):
                kv_edge(k, t).wait_send()
            for s in range(2):
                for h in range(NH):
                    wo_edge(k, s, h).wait_send()

    @pl.when(inner == 1)
    def _():
        xn_send(m, S_XNF, far_dev).wait_send()
        xn_send(m, S_XNC, core_dev).wait_send()
        xn_send(far_m, S_XNG, core_dev).wait_send()
        for t in range(2):
            for k in range(2):
                kv_swap(k, t).wait_send()
            kv_back(t).wait_send()
        for s in range(2):
            for h in range(NH):
                for k in range(2):
                    wo_swap(k, s, h).wait_send()
                    wq_swap(k, s, h).wait_send()
                wo_back(s, h).wait_send()
                wq_back(s, h).wait_send()

    kp_copy.wait_send()
    for i in range(2):
        px_copy(i).wait_send()
        py_copy(i).wait_send()


def store_kernel(*refs):
    n = len(refs) // 2
    sem = refs[-1]
    copies = [pltpu.make_async_copy(refs[i], refs[n + i], sem.at[i]) for i in range(n)]
    for cp in copies:
        cp.start()
    for cp in copies:
        cp.wait()


def solution(mesh):
    tok_spec = P(('pod', 'data'), 'model', None)

    def device_step(x_loc, dy_loc, w_q, w_k, w_v, w_o):
        any_spec = pl.BlockSpec(memory_space=pl.ANY)
        vmem_spec = pl.BlockSpec(memory_space=pltpu.VMEM)
        outs = (((BLK, DIM), BF16), ((CH * NH, HD), F32), ((KC, HD), F32), ((KC, HD), F32), ((HE, CH), F32))
        dx, dwq, dwk, dwv, dwo = pl.pallas_call(
            step_kernel,
            out_shape=tuple(pltpu.VMEM(shape, dtype) for shape, dtype in outs),
            in_specs=[any_spec] * 6,
            out_specs=[vmem_spec] * 5,
            scratch_shapes=[
                pltpu.VMEM((SEQ, DIM), BF16),
                pltpu.VMEM((SEQ, DIM), BF16),
                pltpu.VMEM((2, WR, HD), BF16),
                pltpu.VMEM((WR, HD), F32),
                pltpu.VMEM((DIM, QKV), BF16),
                pltpu.VMEM((HE, DIM), BF16),
                pltpu.VMEM((SEQ, QKV), BF16),
                pltpu.VMEM((HD, SEQ), BF16),
                pltpu.VMEM((HD, SEQ), BF16),
                pltpu.VMEM((NH, CAUSAL_ROWS, BLK), F32),
                pltpu.VMEM((SEQ, BLK), BF16),
                pltpu.VMEM((HE, SEQ), BF16),
                pltpu.VMEM((SEQ, HE), BF16),
                pltpu.VMEM((QKV, SEQ), BF16),
                pltpu.VMEM((SEQ, QKV), BF16),
                pltpu.VMEM((SEQ, 2 * HD), F32),
                pltpu.VMEM((4, HE, CH), F32),
                pltpu.VMEM((2 * HD, DIM // 2), F32),
                pltpu.VMEM((2 * HD, DIM // 2), BF16),
                pltpu.VMEM((2 * HD, DIM // 2), BF16),
                pltpu.VMEM((3, 2, NH, HD, SC), BF16),
                pltpu.VMEM((5, 2, NH, HD, SC), BF16),
                pltpu.VMEM((3, 2, NH, HD, SC), BF16),
                pltpu.VMEM((3, 2, NH, HD, SC), BF16),
                pltpu.VMEM((3, 2 * HD, KC), BF16),
                pltpu.VMEM((5, 2 * HD, KC), BF16),
                pltpu.VMEM((2, BLK, DIM), BF16),
                pltpu.VMEM((2, BLK, DIM), BF16),
                pltpu.VMEM((BLK, DIM), BF16),
                pltpu.VMEM((BLK, DIM), BF16),
                pltpu.VMEM((SEQ, 3 * CH), BF16),
                pltpu.VMEM((HE, SEQ), BF16),
                pltpu.SemaphoreType.DMA((N_SEM,)),
                pltpu.SemaphoreType.DMA((N_SEM,)),
                pltpu.SemaphoreType.DMA((7,)),
            ],
            compiler_params=pltpu.CompilerParams(collective_id=0, has_side_effects=True, vmem_limit_bytes=VMEM_LIMIT),
        )(x_loc, dy_loc, w_q.reshape(DIM * NH, HD), w_k, w_v, w_o.reshape(HE, DIM))
        dx, dwq, dwk, dwv, dwo = pl.pallas_call(
            store_kernel,
            out_shape=tuple(jax.ShapeDtypeStruct(shape, dtype) for shape, dtype in outs),
            in_specs=[any_spec] * 5,
            out_specs=[any_spec] * 5,
            scratch_shapes=[pltpu.SemaphoreType.DMA((5,))],
            compiler_params=pltpu.CompilerParams(vmem_limit_bytes=2 ** 20),
        )(dx, dwq, dwk, dwv, dwo)
        return dx.reshape(1, BLK, DIM), dwq.reshape(CH, NH, HD), dwk, dwv, dwo.reshape(NH, HD, CH)

    kv_rows = P(('pod', 'model', 'data'), None)
    return jax.shard_map(device_step, mesh=mesh,
                         in_specs=(tok_spec, tok_spec, P(None, 'model', None), P(), P(), P('model', None, None)),
                         out_specs=(tok_spec, P(('pod', 'data'), 'model', None), kv_rows, kv_rows, P(('pod', 'model'), None, 'data')),
                         check_vma=False)
```

```python
import functools
import math

import jax
import jax.numpy as jnp
from jax import lax
from jax.experimental import pallas as pl
from jax.experimental.pallas import tpu as pltpu
from jax.sharding import PartitionSpec as P

MESH = pl.DeviceIdType.MESH
F32 = jnp.float32
BF16 = jnp.bfloat16

SEQ = 1024
BLK = 256
DIM = 2048
HD = 128
NH = 4
HE = NH * HD
QKV = HE + 2 * HD
CH = 512
SC = CH // 2
WR = 1024
KC = 256
NX = 4
XR = BLK // NX
NB = SEQ // BLK
CAUSAL_ROWS = BLK * NB * (NB + 1) // 2

S_XY, S_XF, S_XC = 0, 4, 8
S_DY, S_DF, S_DC = 9, 14, 19
S_KP = 20
S_PX = 21
S_PY = 23
S_XN, S_XNC, S_XNF, S_XNG = 25, 26, 27, 28
S_A = 29
S_WO = 33
S_WQ = 81
S_KV = 105
S_XT, S_XU = 117, 121
N_SEM = 125
XT = XR // 4
VMEM_LIMIT = 63 * 2 ** 20 - 3328 * 1024


def nn(a, b):
    return lax.dot_general(a, b, (((1,), (0,)), ((), ())), preferred_element_type=F32)


def nt(a, b):
    return lax.dot_general(a, b, (((1,), (1,)), ((), ())), preferred_element_type=F32)


def step_kernel(x_in, dy_in, wq_in, wk_in, wv_in, wo_in, dxo, wqo, dko, dvo, woo,
                xg, dyg, wq8, wst, wqkv, wo, qkv, kt, vt, prob, pbuf, ot, dout, at, am, dkv, pw, pkv,
                kvs, kvr, so, ro, sq, rq, skv, rkv, sx, rx, sy, ry, xn, xta, xtb, abuf, ssem, rsem, lsem):
    pod = lax.axis_index("pod")
    z = lax.axis_index("data")
    m = lax.axis_index("model")
    y = m // 2
    c = m % 2
    core_m = 2 * y + 1 - c
    far_m = (m + 2) % 4
    diag_m = (core_m + 2) % 4
    core_dev = (pod, z, core_m)
    far_dev = (pod, z, far_m)

    inner = ((z + 1) // 2) % 2
    pair_dev = (pod, z + 1 - 2 * (z % 2), m)
    other_dev = (pod, 3 - z, m)
    x_off = CH * (1 - z // 2)

    def rows(block, n=BLK, off=0):
        return pl.ds(pl.multiple_of(block * BLK + off, n), n)

    def chunk(i):
        return i + (1 - z // 2) * (3 - 2 * i)

    def col(i):
        return pl.ds(pl.multiple_of(chunk(i) * CH, CH), CH)

    def dcol(i):
        if i < 2:
            return pl.ds(pl.multiple_of(chunk(0) * CH + i * SC, SC), SC)
        return col(i - 1)

    def remote(src, dst, sem, dev):
        return pltpu.make_async_remote_copy(src_ref=src, dst_ref=dst, send_sem=ssem.at[sem], recv_sem=rsem.at[sem],
                                            device_id=dev, device_id_type=MESH)

    def head_rows(h):
        return pl.ds(pl.multiple_of(h * HD, HD), HD)

    loads = [
        pltpu.make_async_copy(x_in.at[0], xg.at[rows(m)], lsem.at[0]),
        pltpu.make_async_copy(dy_in.at[0], dyg.at[rows(m)], lsem.at[1]),
        pltpu.make_async_copy(wk_in.at[y], wqkv.at[:, pl.ds(HE, HD)], lsem.at[2]),
        pltpu.make_async_copy(wv_in.at[y], wqkv.at[:, pl.ds(HE + HD, HD)], lsem.at[3]),
        pltpu.make_async_copy(wo_in, wo, lsem.at[4]),
    ]
    def wq_load(i):
        return pltpu.make_async_copy(wq_in.at[pl.ds(pl.multiple_of(i * WR, WR), WR)], wq8.at[i % 2], lsem.at[5 + i % 2])

    for ld in loads:
        ld.start()
    wq_load(0).start()
    wq_load(1).start()

    barrier = pltpu.get_barrier_semaphore()
    for dev in (far_dev, core_dev, pair_dev):
        pl.semaphore_signal(barrier, inc=1, device_id=dev, device_id_type=MESH)

    @pl.when(inner == 1)
    def _():
        pl.semaphore_signal(barrier, inc=1, device_id=other_dev, device_id_type=MESH)

    pl.semaphore_wait(barrier, 3 + inner)

    def x_far(i, block):
        r = rows(block, XR, i * XR)
        return remote(xg.at[r], xg.at[r], S_XY + i, far_dev)

    def x_fwd(i, block):
        r = rows(block, XR, i * XR)
        return remote(xg.at[r], xg.at[r], S_XF + i, core_dev)

    def x_core(block):
        return remote(xg.at[rows(block)], xg.at[rows(block)], S_XC, core_dev)

    def dy_far(i, block):
        return remote(dyg.at[rows(block), dcol(i)], dyg.at[rows(block), dcol(i)], S_DY + i, far_dev)

    def dy_fwd(i, block):
        return remote(dyg.at[rows(block), dcol(i)], dyg.at[rows(block), dcol(i)], S_DF + i, core_dev)

    def dy_core(block):
        return remote(dyg.at[rows(block)], dyg.at[rows(block)], S_DC, core_dev)

    def xn_edge(block):
        return remote(xg.at[rows(block), pl.ds(pl.multiple_of(x_off, CH), 3 * CH)], xn.at[rows(block)], S_XN, pair_dev)

    def xn_send(block, sem, dev):
        return remote(xn.at[rows(block)], xn.at[rows(block)], sem, dev)

    def xt_edge(j):
        return remote(xg.at[rows(m, XT, (NX - 1) * XR + j * XT)], xta.at[pl.ds(j * XT, XT)], S_XT + j, pair_dev)

    def xt_far(j):
        return remote(xta.at[pl.ds(j * XT, XT)], xtb.at[pl.ds(j * XT, XT)], S_XU + j, far_dev)

    def xt_back():
        return remote(xtb, xg.at[rows(far_m, XR, (NX - 1) * XR)], S_XY + NX - 1, pair_dev)

    loads[0].wait()
    x_far(0, m).start()

    @pl.when(inner == 0)
    def _():
        for j in range(4):
            xt_edge(j).start()
        xn_edge(m).start()
        for i in range(1, NX - 1):
            x_far(i, m).start()

    x_core(m).start()
    loads[1].wait()

    @pl.when(inner == 0)
    def _():
        for i in range(5):
            dy_far(i, m).start()

    dy_core(m).start()
    for ld in loads[2:]:
        ld.wait()

    def wq_block(i, carry):
        wq_load(i).wait()
        wst[...] = wq8[i % 2].astype(F32)

        @pl.when(i + 2 < DIM * NH // WR)
        def _():
            wq_load(i + 2).start()

        for h in range(NH):
            wqkv[pl.ds(pl.multiple_of(i * (WR // NH), WR // NH), WR // NH), pl.ds(h * HD, HD)] = wst[pl.ds(h, WR // NH, stride=NH), :].astype(BF16)
        return carry

    lax.fori_loop(0, DIM * NH // WR, wq_block, 0)

    @pl.when(inner == 1)
    def _():
        for j in range(4):
            xt_edge(j).wait_recv()
            xt_far(j).start()
        for i in range(1, NX):
            x_far(i, m).start()
        for i in range(5):
            dy_far(i, m).start()

    def project(r):
        qkv[r, :] = nn(xg[r, :], wqkv[...]).astype(BF16)

    def flip(block):
        r = rows(block)
        kt[:, r] = qkv[r, pl.ds(HE, HD)].T
        vt[:, r] = qkv[r, pl.ds(HE + HD, HD)].T

    project(rows(m))
    x_core(core_m).wait_recv()
    project(rows(core_m))
    flip(m)
    flip(core_m)

    @pl.when(inner == 1)
    def _():
        for j in range(4):
            xt_far(j).wait_recv()
        xt_back().start()

    def x_piece(i, carry):
        x_far(i, far_m).wait_recv()
        x_fwd(i, far_m).start()
        project(rows(far_m, XR, i * XR))
        x_fwd(i, diag_m).wait_recv()
        project(rows(diag_m, XR, i * XR))
        return carry

    lax.fori_loop(0, NX, x_piece, 0)

    flip(far_m)
    flip(diag_m)
    dy_core(core_m).wait_recv()

    def take_dy(i):
        dy_far(i, far_m).wait_recv()
        dy_fwd(i, far_m).start()

    def wo_sem(slot, s, h):
        return S_WO + slot * 8 + s * 4 + h

    def wo_edge(k, s, h):
        return remote(so.at[k, s, h], ro.at[k, s, h], wo_sem(k, s, h), pair_dev)

    def wo_swap(k, s, h):
        return remote(so.at[k, s, h], ro.at[3 + k, s, h], wo_sem(3 + k, s, h), other_dev)

    def wo_back(s, h):
        return remote(so.at[2, s, h], ro.at[3, s, h], wo_sem(5, s, h), pair_dev)

    def half_col(s):
        return pl.ds(s * SC, SC)

    def wo_first(s, h):
        v = nn(ot[pl.ds(h * HD, HD), :], dyg[:, dcol(s)])

        @pl.when(inner == 0)
        def _():
            so[0, s, h] = v.astype(BF16)
            wo_edge(0, s, h).start()

        @pl.when(inner == 1)
        def _():
            pw[0, head_rows(h), half_col(s)] = v

    @pl.when(inner == 1)
    def _():
        xn_edge(m).wait_recv()
        xn_send(m, S_XNF, far_dev).start()
        xn_send(m, S_XNC, core_dev).start()

    scale = HD ** -0.5
    exp_scale = scale * math.log2(math.e)
    diag_mask = lax.broadcasted_iota(jnp.int32, (BLK, BLK), 0) <= lax.broadcasted_iota(jnp.int32, (BLK, BLK), 1)

    def prow(qi, kj):
        return pl.ds(BLK * (qi * (qi + 1) // 2 + kj), BLK)

    def fwd_head(h, first_q, last_q):
        hr = pl.ds(h * HD, HD)
        for qi in range(first_q, last_q):
            qb = qkv[pl.ds(qi * BLK, BLK), hr]
            mx = None
            for kj in range(qi + 1):
                s = nt(qkv[pl.ds(kj * BLK, BLK), pl.ds(HE, HD)], qb)
                if kj == qi:
                    s = jnp.where(diag_mask, s, -jnp.inf)
                prob[h, prow(qi, kj), :] = s
                bm = jnp.max(s, axis=0, keepdims=True)
                mx = bm if mx is None else jnp.maximum(mx, bm)
            tot = None
            for kj in range(qi + 1):
                e = jnp.exp2((prob[h, prow(qi, kj), :] - mx) * exp_scale)
                prob[h, prow(qi, kj), :] = e
                bs = jnp.sum(e, axis=0, keepdims=True)
                tot = bs if tot is None else tot + bs
            inv = 1.0 / tot
            for kj in range(qi + 1):
                p = prob[h, prow(qi, kj), :] * inv
                prob[h, prow(qi, kj), :] = p
                pbuf[pl.ds(kj * BLK, BLK), :] = p.astype(BF16)
            n = (qi + 1) * BLK
            ot[hr, pl.ds(qi * BLK, BLK)] = nn(vt[:, pl.ds(0, n)], pbuf[pl.ds(0, n), :]).astype(BF16)

    fwd_head(0, 0, 3)
    take_dy(0)
    fwd_head(0, 3, NB)
    dy_fwd(0, diag_m).wait_recv()
    wo_first(0, 0)
    fwd_head(1, 0, 2)
    take_dy(1)
    fwd_head(1, 2, 3)
    dy_fwd(1, diag_m).wait_recv()
    wo_first(1, 0)
    fwd_head(1, 3, NB)
    wo_first(0, 1)
    wo_first(1, 1)
    for h in range(2, NH):
        fwd_head(h, 0, 3)
        if h == 3:
            take_dy(2)
        fwd_head(h, 3, NB)
        for s in range(2):
            wo_first(s, h)

    def wo_pass(k, h):
        for s in range(2):
            wo_edge(k, s, h).wait_recv()
            so[k, s, h] = (pw[k, head_rows(h), half_col(s)] + ro[k, s, h].astype(F32)).astype(BF16)
            wo_swap(k, s, h).start()

    def wo_return(h):
        for s in range(2):
            wo_swap(0, s, h).wait_recv()
            so[2, s, h] = (pw[3, head_rows(h), half_col(s)] + ro[3, s, h].astype(F32)).astype(BF16)
            wo_back(s, h).start()

    def wo_send(k):
        for h in range(NH):
            for s in range(2):
                so[k, s, h] = pw[k, head_rows(h), half_col(s)].astype(BF16)
                wo_edge(k, s, h).start()

    for i in range(1, 4):
        if i > 1:
            take_dy(i + 1)
        dy_fwd(i + 1, diag_m).wait_recv()
        pw[i] = nn(ot[...], dyg[:, col(i)])
        if i < 3:
            @pl.when(inner == 0)
            def _(i=i):
                wo_send(i)

            @pl.when(inner == 1)
            def _(i=i):
                for h in (2 * i - 2, 2 * i - 1):
                    wo_pass(0, h)

    def a_copy(h):
        r = head_rows(h)
        return remote(at.at[r], abuf.at[r], S_A + h, pair_dev)

    def wq_swap(k, s, h):
        return remote(sq.at[k, s, h], rq.at[k, s, h], S_WQ + k * 8 + s * 4 + h, other_dev)

    def wq_back(s, h):
        return remote(sq.at[2, s, h], rq.at[2, s, h], S_WQ + 16 + s * 4 + h, pair_dev)

    def ncol(k):
        return pl.ds(pl.multiple_of(chunk(k) * CH - x_off, CH), CH)

    def spot(k, s, h=0, n=1):
        return prob.at[1 + k // 2, pl.ds(((k % 2) * 2 + s) * HE + h * HD, n * HD)]

    def wq_own(k, q):
        v = nn(at[pl.ds(0, HE), :], xg[:, pl.ds(pl.multiple_of(q * CH, CH), CH)])
        for s in range(2):
            spot(k, s, 0, NH)[...] = v[:, s * SC:(s + 1) * SC]

    def combine(h, ks=(0, 1)):
        if 0 in ks:
            a_copy(h).wait_recv()
        for k in ks:
            v = nn(abuf[head_rows(h), :], xn[:, ncol(k)])
            for s in range(2):
                sq[k, s, h] = (spot(k, s, h)[...] + v[:, s * SC:(s + 1) * SC]).astype(BF16)
                wq_swap(k, s, h).start()

    def outer(h):
        for s in range(2):
            wq_swap(0, s, h).wait_recv()
            sq[2, s, h] = (spot(3, s, h)[...] + rq[0, s, h].astype(F32)).astype(BF16)
            wq_back(s, h).start()

    def dout_block(b, carry):
        r = rows(b)
        dout[r, :] = nt(dyg[r, :], wo[...]).astype(BF16)
        return carry

    lax.fori_loop(0, NB, dout_block, 0)

    dkv[...] = jnp.zeros_like(dkv)

    def bwd_head(h, carry):
        hr = head_rows(h)
        for qi in range(NB):
            qr = pl.ds(qi * BLK, BLK)
            dob = dout[qr, hr]
            qb = qkv[qr, hr]
            delta = jnp.sum(dob.astype(F32).T * ot[hr, qr].astype(F32), axis=0, keepdims=True)
            for kj in range(qi + 1):
                kr = pl.ds(kj * BLK, BLK)
                p = prob[h, prow(qi, kj), :]
                dp = nt(qkv[kr, pl.ds(HE + HD, HD)], dob)
                ds = (p * (dp - delta)).astype(BF16)
                pbuf[kr, :] = ds
                dkv[kr, pl.ds(0, HD)] += nn(ds, qb)
                dkv[kr, pl.ds(HD, HD)] += nn(p.astype(BF16), dob)
            n = (qi + 1) * BLK
            dq = (nn(kt[:, pl.ds(0, n)], pbuf[pl.ds(0, n), :]) * scale).astype(BF16)
            at[hr, qr] = dq
            am[qr, hr] = dq.T

        @pl.when(inner == 0)
        def _():
            a_copy(h).start()

        @pl.when(inner == 1)
        def _():
            wo_pass(1, h)
            wo_return(h)

        return carry

    lax.fori_loop(0, NH, bwd_head, 0)

    dkb = (dkv[:, pl.ds(0, HD)] * scale).astype(BF16)
    dvb = dkv[:, pl.ds(HD, HD)].astype(BF16)
    am[:, pl.ds(HE, HD)] = dkb
    am[:, pl.ds(HE + HD, HD)] = dvb
    at[pl.ds(HE, HD), :] = dkb.T
    at[pl.ds(HE + HD, HD), :] = dvb.T

    def dx_part(block, put):
        def piece(i, carry):
            cs = pl.ds(pl.multiple_of(i * CH, CH), CH)
            put(i, cs, nt(am[rows(block), :], wqkv[cs, :]))
            return carry

        lax.fori_loop(0, DIM // CH, piece, 0)

    def px_copy(i):
        return remote(sx.at[i], rx.at[i], S_PX + i, core_dev)

    def py_copy(i):
        r = pl.ds(i * (BLK // 2), BLK // 2)
        return remote(sy.at[r], ry.at[r], S_PY + i, far_dev)

    def put_sx(j):
        def put(i, cs, v):
            sx[j, :, cs] = v.astype(BF16)
        return put

    def pxo(i, s):
        return prob.at[0, pl.ds(pl.multiple_of((2 * i + s) * BLK, BLK), BLK)]

    def put_own(i, cs, v):
        for s in range(2):
            pxo(i, s)[...] = v[:, s * SC:(s + 1) * SC]

    half = DIM // 2

    def kv_half(which):
        return nn(at[pl.ds(HE, 2 * HD), :], xg[:, pl.ds(pl.multiple_of(which * half, half), half)])

    def kcol(k):
        return pl.ds(pl.multiple_of(chunk(k) * KC, KC), KC)

    def kv_part(ref, slot, t):
        return ref.at[slot, pl.ds(t * HD, HD)]

    def kv_edge(k, t):
        return remote(kv_part(skv, k, t), kv_part(rkv, k, t), S_KV + 2 * k + t, pair_dev)

    def kv_swap(k, t):
        return remote(kv_part(skv, k, t), kv_part(rkv, 3 + k, t), S_KV + 2 * (3 + k) + t, other_dev)

    def kv_back(t):
        return remote(kv_part(skv, 2, t), kv_part(rkv, 3, t), S_KV + 10 + t, pair_dev)

    def kv_own(k, t):
        return pkv[pl.ds(t * HD, HD), kcol(k)]

    def kv_pass(k):
        for t in range(2):
            kv_edge(k, t).wait_recv()
            kv_part(skv, k, t)[...] = (kv_own(k, t) + kv_part(rkv, k, t)[...].astype(F32)).astype(BF16)
            kv_swap(k, t).start()

    kvs[...] = kv_half(1 - c).astype(BF16)
    kp_copy = remote(kvs, kvr, S_KP, core_dev)
    kp_copy.start()
    dx_part(diag_m, put_sx(0))
    px_copy(0).start()
    pkv[...] = kv_half(c)
    kp_copy.wait_recv()
    pkv[...] += kvr[...].astype(F32)

    @pl.when(inner == 0)
    def _():
        for k in range(3):
            for t in range(2):
                kv_part(skv, k, t)[...] = kv_own(k, t).astype(BF16)
                kv_edge(k, t).start()
    @pl.when(inner == 1)
    def _():
        xn_send(far_m, S_XNF, far_dev).wait_recv()
        xn_send(far_m, S_XNG, core_dev).start()
        wq_own(0, chunk(0))
        wq_own(1, chunk(1))

    dx_part(far_m, put_own)
    px_copy(0).wait_recv()
    for i in range(2):
        r = pl.ds(i * (BLK // 2), BLK // 2)
        for j in range(DIM // SC):
            cs = pl.ds(j * SC, SC)
            own = prob[0, pl.ds(j * BLK + i * (BLK // 2), BLK // 2), :]
            sy[r, cs] = (own + rx[0, r, cs].astype(F32)).astype(BF16)
        py_copy(i).start()

    @pl.when(inner == 1)
    def _():
        xn_send(core_m, S_XNC, core_dev).wait_recv()
        xn_send(diag_m, S_XNG, core_dev).wait_recv()
        combine(0)
        wq_own(3, chunk(3))
        combine(1)
        outer(0)

    dx_part(core_m, put_sx(1))
    px_copy(1).start()
    dx_part(m, put_own)
    wq_own(2, z)

    @pl.when(inner == 1)
    def _():
        combine(2)
        outer(1)
        combine(3, (0,))
        outer(2)
        v = nn(abuf[...], xn[:, ncol(2)])
        for s in range(2):
            spot(2, s, 0, NH)[...] += v[:, s * SC:(s + 1) * SC]
        kv_pass(0)
        combine(3, (1,))
        outer(3)
        kv_pass(1)
        for t in range(2):
            kv_swap(0, t).wait_recv()
            kv_part(skv, 2, t)[...] = (kv_own(3, t) + kv_part(rkv, 3, t)[...].astype(F32)).astype(BF16)
            kv_back(t).start()
        for h in range(NH):
            for s in range(2):
                wo_edge(2, s, h).wait_recv()
                wo_swap(1, s, h).wait_recv()
                woo[head_rows(h), half_col(s)] = pw[2, head_rows(h), half_col(s)] + ro[2, s, h].astype(F32) + ro[4, s, h].astype(F32)

    @pl.when(inner == 0)
    def _():
        for h in range(NH):
            for s in range(2):
                wo_back(s, h).wait_recv()
                woo[head_rows(h), half_col(s)] = pw[3, head_rows(h), half_col(s)] + ro[3, s, h].astype(F32)

    px_copy(1).wait_recv()
    for i in range(2):
        r = pl.ds(i * (BLK // 2), BLK // 2)
        py_copy(i).wait_recv()
        for j in range(DIM // SC):
            cs = pl.ds(j * SC, SC)
            own = prob[0, pl.ds(j * BLK + i * (BLK // 2), BLK // 2), :]
            dxo[r, cs] = (own + rx[1, r, cs].astype(F32) + ry[r, cs].astype(F32)).astype(BF16)

    def wq_put(h, s, got):
        wqo[pl.ds(s * SC * NH + h, SC, stride=NH), :] = (spot(2, s, h)[...] + got.astype(F32)).T

    kv_out = (dko, dvo)

    @pl.when(inner == 1)
    def _():
        for h in range(NH):
            for s in range(2):
                wq_swap(1, s, h).wait_recv()
                wq_put(h, s, rq[1, s, h])
        for t in range(2):
            kv_edge(2, t).wait_recv()
            kv_swap(1, t).wait_recv()
            kv_out[t][...] = (kv_own(2, t) + kv_part(rkv, 2, t)[...].astype(F32) + kv_part(rkv, 4, t)[...].astype(F32)).T

    @pl.when(inner == 0)
    def _():
        for h in range(NH):
            for s in range(2):
                wq_back(s, h).wait_recv()
                wq_put(h, s, rq[2, s, h])
        for t in range(2):
            kv_back(t).wait_recv()
            kv_out[t][...] = (kv_own(3, t) + kv_part(rkv, 3, t)[...].astype(F32)).T

    for i in range(NX - 1):
        x_far(i, m).wait_send()
    for i in range(NX):
        x_fwd(i, far_m).wait_send()
    x_core(m).wait_send()
    for i in range(5):
        dy_far(i, m).wait_send()
        dy_fwd(i, far_m).wait_send()
    dy_core(m).wait_send()
    @pl.when(inner == 0)
    def _():
        for j in range(4):
            xt_edge(j).wait_send()
        xn_edge(m).wait_send()
        for h in range(NH):
            a_copy(h).wait_send()
        for k in range(3):
            for t in range(2):
                kv_edge(k, t).wait_send()
            for s in range(2):
                for h in range(NH):
                    wo_edge(k, s, h).wait_send()

    @pl.when(inner == 1)
    def _():
        x_far(NX - 1, m).wait_send()
        for j in range(4):
            xt_far(j).wait_send()
        xt_back().wait_send()
        xn_send(m, S_XNF, far_dev).wait_send()
        xn_send(m, S_XNC, core_dev).wait_send()
        xn_send(far_m, S_XNG, core_dev).wait_send()
        for t in range(2):
            for k in range(2):
                kv_swap(k, t).wait_send()
            kv_back(t).wait_send()
        for s in range(2):
            for h in range(NH):
                for k in range(2):
                    wo_swap(k, s, h).wait_send()
                    wq_swap(k, s, h).wait_send()
                wo_back(s, h).wait_send()
                wq_back(s, h).wait_send()

    kp_copy.wait_send()
    for i in range(2):
        px_copy(i).wait_send()
        py_copy(i).wait_send()


def store_kernel(*refs):
    n = len(refs) // 2
    sem = refs[-1]
    copies = [pltpu.make_async_copy(refs[i], refs[n + i], sem.at[i]) for i in range(n)]
    for cp in copies:
        cp.start()
    for cp in copies:
        cp.wait()


def solution(mesh):
    tok_spec = P(('pod', 'data'), 'model', None)

    def device_step(x_loc, dy_loc, w_q, w_k, w_v, w_o):
        any_spec = pl.BlockSpec(memory_space=pl.ANY)
        vmem_spec = pl.BlockSpec(memory_space=pltpu.VMEM)
        outs = (((BLK, DIM), BF16), ((CH * NH, HD), F32), ((KC, HD), F32), ((KC, HD), F32), ((HE, CH), F32))
        dx, dwq, dwk, dwv, dwo = pl.pallas_call(
            step_kernel,
            out_shape=tuple(pltpu.VMEM(shape, dtype) for shape, dtype in outs),
            in_specs=[any_spec] * 6,
            out_specs=[vmem_spec] * 5,
            scratch_shapes=[
                pltpu.VMEM((SEQ, DIM), BF16),
                pltpu.VMEM((SEQ, DIM), BF16),
                pltpu.VMEM((2, WR, HD), BF16),
                pltpu.VMEM((WR, HD), F32),
                pltpu.VMEM((DIM, QKV), BF16),
                pltpu.VMEM((HE, DIM), BF16),
                pltpu.VMEM((SEQ, QKV), BF16),
                pltpu.VMEM((HD, SEQ), BF16),
                pltpu.VMEM((HD, SEQ), BF16),
                pltpu.VMEM((NH, CAUSAL_ROWS, BLK), F32),
                pltpu.VMEM((SEQ, BLK), BF16),
                pltpu.VMEM((HE, SEQ), BF16),
                pltpu.VMEM((SEQ, HE), BF16),
                pltpu.VMEM((QKV, SEQ), BF16),
                pltpu.VMEM((SEQ, QKV), BF16),
                pltpu.VMEM((SEQ, 2 * HD), F32),
                pltpu.VMEM((4, HE, CH), F32),
                pltpu.VMEM((2 * HD, DIM // 2), F32),
                pltpu.VMEM((2 * HD, DIM // 2), BF16),
                pltpu.VMEM((2 * HD, DIM // 2), BF16),
                pltpu.VMEM((3, 2, NH, HD, SC), BF16),
                pltpu.VMEM((5, 2, NH, HD, SC), BF16),
                pltpu.VMEM((3, 2, NH, HD, SC), BF16),
                pltpu.VMEM((3, 2, NH, HD, SC), BF16),
                pltpu.VMEM((3, 2 * HD, KC), BF16),
                pltpu.VMEM((5, 2 * HD, KC), BF16),
                pltpu.VMEM((2, BLK, DIM), BF16),
                pltpu.VMEM((2, BLK, DIM), BF16),
                pltpu.VMEM((BLK, DIM), BF16),
                pltpu.VMEM((BLK, DIM), BF16),
                pltpu.VMEM((SEQ, 3 * CH), BF16),
                pltpu.VMEM((XR, DIM), BF16),
                pltpu.VMEM((XR, DIM), BF16),
                pltpu.VMEM((HE, SEQ), BF16),
                pltpu.SemaphoreType.DMA((N_SEM,)),
                pltpu.SemaphoreType.DMA((N_SEM,)),
                pltpu.SemaphoreType.DMA((7,)),
            ],
            compiler_params=pltpu.CompilerParams(collective_id=0, has_side_effects=True, vmem_limit_bytes=VMEM_LIMIT),
        )(x_loc, dy_loc, w_q.reshape(DIM * NH, HD), w_k, w_v, w_o.reshape(HE, DIM))
        dx, dwq, dwk, dwv, dwo = pl.pallas_call(
            store_kernel,
            out_shape=tuple(jax.ShapeDtypeStruct(shape, dtype) for shape, dtype in outs),
            in_specs=[any_spec] * 5,
            out_specs=[any_spec] * 5,
            scratch_shapes=[pltpu.SemaphoreType.DMA((5,))],
            compiler_params=pltpu.CompilerParams(vmem_limit_bytes=2 ** 20),
        )(dx, dwq, dwk, dwv, dwo)
        return dx.reshape(1, BLK, DIM), dwq.reshape(CH, NH, HD), dwk, dwv, dwo.reshape(NH, HD, CH)

    kv_rows = P(('pod', 'model', 'data'), None)
    return jax.shard_map(device_step, mesh=mesh,
                         in_specs=(tok_spec, tok_spec, P(None, 'model', None), P(), P(), P('model', None, None)),
                         out_specs=(tok_spec, P(('pod', 'data'), 'model', None), kv_rows, kv_rows, P(('pod', 'model'), None, 'data')),
                         check_vma=False)
```

```python
import functools
import math

import jax
import jax.numpy as jnp
from jax import lax
from jax.experimental import pallas as pl
from jax.experimental.pallas import tpu as pltpu
from jax.sharding import PartitionSpec as P

MESH = pl.DeviceIdType.MESH
F32 = jnp.float32
BF16 = jnp.bfloat16

SEQ = 1024
BLK = 256
DIM = 2048
HD = 128
NH = 4
HE = NH * HD
QKV = HE + 2 * HD
CH = 512
SC = CH // 2
WR = 1024
KC = 256
NX = 8
XR = BLK // NX
NB = SEQ // BLK
CAUSAL_ROWS = BLK * NB * (NB + 1) // 2

S_XY, S_XF, S_XC = 0, 8, 16
S_DY, S_DF, S_DC = 17, 22, 27
S_KP = 28
S_PX = 29
S_PY = 31
S_XN, S_XNC, S_XNF, S_XNG = 33, 34, 35, 36
S_A = 37
S_WO = 41
S_WQ = 89
S_KV = 113
S_XT, S_XU = 125, 127
N_SEM = 129
NT = 2
XT = XR // NT
VMEM_LIMIT = 63 * 2 ** 20 - 3328 * 1024


def nn(a, b):
    return lax.dot_general(a, b, (((1,), (0,)), ((), ())), preferred_element_type=F32)


def nt(a, b):
    return lax.dot_general(a, b, (((1,), (1,)), ((), ())), preferred_element_type=F32)


def step_kernel(x_in, dy_in, wq_in, wk_in, wv_in, wo_in, dxo, wqo, dko, dvo, woo,
                xg, dyg, wq8, wst, wqkv, wo, qkv, kt, vt, prob, pbuf, ot, dout, at, am, dkv, pw, pkv,
                kvs, kvr, so, ro, sq, rq, skv, rkv, sx, rx, sy, ry, xn, xta, xtb, abuf, ssem, rsem, lsem):
    pod = lax.axis_index("pod")
    z = lax.axis_index("data")
    m = lax.axis_index("model")
    y = m // 2
    c = m % 2
    core_m = 2 * y + 1 - c
    far_m = (m + 2) % 4
    diag_m = (core_m + 2) % 4
    core_dev = (pod, z, core_m)
    far_dev = (pod, z, far_m)

    inner = ((z + 1) // 2) % 2
    pair_dev = (pod, z + 1 - 2 * (z % 2), m)
    other_dev = (pod, 3 - z, m)
    x_off = CH * (1 - z // 2)

    def rows(block, n=BLK, off=0):
        return pl.ds(pl.multiple_of(block * BLK + off, n), n)

    def chunk(i):
        return i + (1 - z // 2) * (3 - 2 * i)

    def col(i):
        return pl.ds(pl.multiple_of(chunk(i) * CH, CH), CH)

    def dcol(i):
        if i < 2:
            return pl.ds(pl.multiple_of(chunk(0) * CH + i * SC, SC), SC)
        return col(i - 1)

    def remote(src, dst, sem, dev):
        return pltpu.make_async_remote_copy(src_ref=src, dst_ref=dst, send_sem=ssem.at[sem], recv_sem=rsem.at[sem],
                                            device_id=dev, device_id_type=MESH)

    def head_rows(h):
        return pl.ds(pl.multiple_of(h * HD, HD), HD)

    loads = [
        pltpu.make_async_copy(x_in.at[0], xg.at[rows(m)], lsem.at[0]),
        pltpu.make_async_copy(dy_in.at[0], dyg.at[rows(m)], lsem.at[1]),
        pltpu.make_async_copy(wk_in.at[y], wqkv.at[:, pl.ds(HE, HD)], lsem.at[2]),
        pltpu.make_async_copy(wv_in.at[y], wqkv.at[:, pl.ds(HE + HD, HD)], lsem.at[3]),
        pltpu.make_async_copy(wo_in, wo, lsem.at[4]),
    ]
    def wq_load(i):
        return pltpu.make_async_copy(wq_in.at[pl.ds(pl.multiple_of(i * WR, WR), WR)], wq8.at[i % 2], lsem.at[5 + i % 2])

    for ld in loads:
        ld.start()
    wq_load(0).start()
    wq_load(1).start()

    barrier = pltpu.get_barrier_semaphore()
    for dev in (far_dev, core_dev, pair_dev):
        pl.semaphore_signal(barrier, inc=1, device_id=dev, device_id_type=MESH)

    @pl.when(inner == 1)
    def _():
        pl.semaphore_signal(barrier, inc=1, device_id=other_dev, device_id_type=MESH)

    pl.semaphore_wait(barrier, 3 + inner)

    def x_far(i, block):
        r = rows(block, XR, i * XR)
        return remote(xg.at[r], xg.at[r], S_XY + i, far_dev)

    def x_fwd(i, block):
        r = rows(block, XR, i * XR)
        return remote(xg.at[r], xg.at[r], S_XF + i, core_dev)

    def x_core(block):
        return remote(xg.at[rows(block)], xg.at[rows(block)], S_XC, core_dev)

    def dy_far(i, block):
        return remote(dyg.at[rows(block), dcol(i)], dyg.at[rows(block), dcol(i)], S_DY + i, far_dev)

    def dy_fwd(i, block):
        return remote(dyg.at[rows(block), dcol(i)], dyg.at[rows(block), dcol(i)], S_DF + i, core_dev)

    def dy_core(block):
        return remote(dyg.at[rows(block)], dyg.at[rows(block)], S_DC, core_dev)

    def xn_edge(block):
        return remote(xg.at[rows(block), pl.ds(pl.multiple_of(x_off, CH), 3 * CH)], xn.at[rows(block)], S_XN, pair_dev)

    def xn_send(block, sem, dev):
        return remote(xn.at[rows(block)], xn.at[rows(block)], sem, dev)

    def xt_edge(j):
        return remote(xg.at[rows(m, XT, (NX - 1) * XR + j * XT)], xta.at[pl.ds(j * XT, XT)], S_XT + j, pair_dev)

    def xt_far(j):
        return remote(xta.at[pl.ds(j * XT, XT)], xtb.at[pl.ds(j * XT, XT)], S_XU + j, far_dev)

    def xt_back():
        return remote(xtb, xg.at[rows(far_m, XR, (NX - 1) * XR)], S_XY + NX - 1, pair_dev)

    loads[0].wait()
    x_far(0, m).start()

    @pl.when(inner == 0)
    def _():
        for j in range(NT):
            xt_edge(j).start()
        xn_edge(m).start()
        for i in range(1, NX - 1):
            x_far(i, m).start()

    x_core(m).start()
    loads[1].wait()

    @pl.when(inner == 0)
    def _():
        for i in range(5):
            dy_far(i, m).start()

    dy_core(m).start()
    for ld in loads[2:]:
        ld.wait()

    def wq_block(i, carry):
        wq_load(i).wait()
        wst[...] = wq8[i % 2].astype(F32)

        @pl.when(i + 2 < DIM * NH // WR)
        def _():
            wq_load(i + 2).start()

        for h in range(NH):
            wqkv[pl.ds(pl.multiple_of(i * (WR // NH), WR // NH), WR // NH), pl.ds(h * HD, HD)] = wst[pl.ds(h, WR // NH, stride=NH), :].astype(BF16)
        return carry

    lax.fori_loop(0, DIM * NH // WR, wq_block, 0)

    @pl.when(inner == 1)
    def _():
        for j in range(NT):
            xt_edge(j).wait_recv()
            xt_far(j).start()
        for i in range(1, NX):
            x_far(i, m).start()
        for i in range(5):
            dy_far(i, m).start()

    def project(r):
        qkv[r, :] = nn(xg[r, :], wqkv[...]).astype(BF16)

    def flip(block):
        r = rows(block)
        kt[:, r] = qkv[r, pl.ds(HE, HD)].T
        vt[:, r] = qkv[r, pl.ds(HE + HD, HD)].T

    project(rows(m))
    x_core(core_m).wait_recv()
    project(rows(core_m))
    flip(m)
    flip(core_m)

    @pl.when(inner == 1)
    def _():
        for j in range(NT):
            xt_far(j).wait_recv()
        xt_back().start()

    def x_piece(i, carry):
        x_far(i, far_m).wait_recv()
        x_fwd(i, far_m).start()
        project(rows(far_m, XR, i * XR))
        x_fwd(i, diag_m).wait_recv()
        project(rows(diag_m, XR, i * XR))
        return carry

    lax.fori_loop(0, NX, x_piece, 0)

    flip(far_m)
    flip(diag_m)
    dy_core(core_m).wait_recv()

    def take_dy(i):
        dy_far(i, far_m).wait_recv()
        dy_fwd(i, far_m).start()

    def wo_sem(slot, s, h):
        return S_WO + slot * 8 + s * 4 + h

    def wo_edge(k, s, h):
        return remote(so.at[k, s, h], ro.at[k, s, h], wo_sem(k, s, h), pair_dev)

    def wo_swap(k, s, h):
        return remote(so.at[k, s, h], ro.at[3 + k, s, h], wo_sem(3 + k, s, h), other_dev)

    def wo_back(s, h):
        return remote(so.at[2, s, h], ro.at[3, s, h], wo_sem(5, s, h), pair_dev)

    def half_col(s):
        return pl.ds(s * SC, SC)

    def wo_pass(k, h):
        for s in range(2):
            wo_edge(k, s, h).wait_recv()
            so[k, s, h] = (pw[k, head_rows(h), half_col(s)] + ro[k, s, h].astype(F32)).astype(BF16)
            wo_swap(k, s, h).start()

    def wo_first(s, h):
        v = nn(ot[pl.ds(h * HD, HD), :], dyg[:, dcol(s)])

        @pl.when(inner == 0)
        def _():
            so[0, s, h] = v.astype(BF16)
            wo_edge(0, s, h).start()

        @pl.when(inner == 1)
        def _():
            pw[0, head_rows(h), half_col(s)] = v

    @pl.when(inner == 1)
    def _():
        xn_edge(m).wait_recv()
        xn_send(m, S_XNF, far_dev).start()
        xn_send(m, S_XNC, core_dev).start()

    scale = HD ** -0.5
    exp_scale = scale * math.log2(math.e)
    diag_mask = lax.broadcasted_iota(jnp.int32, (BLK, BLK), 0) <= lax.broadcasted_iota(jnp.int32, (BLK, BLK), 1)

    def prow(qi, kj):
        return pl.ds(BLK * (qi * (qi + 1) // 2 + kj), BLK)

    def fwd_head(h, first_q, last_q):
        hr = pl.ds(h * HD, HD)
        for qi in range(first_q, last_q):
            qb = qkv[pl.ds(qi * BLK, BLK), hr]
            mx = None
            for kj in range(qi + 1):
                s = nt(qkv[pl.ds(kj * BLK, BLK), pl.ds(HE, HD)], qb)
                if kj == qi:
                    s = jnp.where(diag_mask, s, -jnp.inf)
                prob[h, prow(qi, kj), :] = s
                bm = jnp.max(s, axis=0, keepdims=True)
                mx = bm if mx is None else jnp.maximum(mx, bm)
            tot = None
            for kj in range(qi + 1):
                e = jnp.exp2((prob[h, prow(qi, kj), :] - mx) * exp_scale)
                prob[h, prow(qi, kj), :] = e
                bs = jnp.sum(e, axis=0, keepdims=True)
                tot = bs if tot is None else tot + bs
            inv = 1.0 / tot
            for kj in range(qi + 1):
                p = prob[h, prow(qi, kj), :] * inv
                prob[h, prow(qi, kj), :] = p
                pbuf[pl.ds(kj * BLK, BLK), :] = p.astype(BF16)
            n = (qi + 1) * BLK
            ot[hr, pl.ds(qi * BLK, BLK)] = nn(vt[:, pl.ds(0, n)], pbuf[pl.ds(0, n), :]).astype(BF16)

    fwd_head(0, 0, 3)
    take_dy(0)
    fwd_head(0, 3, NB)
    dy_fwd(0, diag_m).wait_recv()
    wo_first(0, 0)
    fwd_head(1, 0, 2)
    take_dy(1)
    fwd_head(1, 2, 3)
    dy_fwd(1, diag_m).wait_recv()
    wo_first(1, 0)
    fwd_head(1, 3, NB)
    wo_first(0, 1)
    wo_first(1, 1)
    for h in range(2, NH):
        fwd_head(h, 0, 3)
        if h == 3:
            take_dy(2)
        fwd_head(h, 3, NB)
        for s in range(2):
            wo_first(s, h)

        @pl.when(inner == 1)
        def _(h=h):
            wo_pass(0, h - 2)

    def wo_return(h):
        for s in range(2):
            wo_swap(0, s, h).wait_recv()
            so[2, s, h] = (pw[3, head_rows(h), half_col(s)] + ro[3, s, h].astype(F32)).astype(BF16)
            wo_back(s, h).start()

    def wo_send(k):
        for h in range(NH):
            for s in range(2):
                so[k, s, h] = pw[k, head_rows(h), half_col(s)].astype(BF16)
                wo_edge(k, s, h).start()

    for i in range(1, 4):
        if i > 1:
            take_dy(i + 1)
        dy_fwd(i + 1, diag_m).wait_recv()
        pw[i] = nn(ot[...], dyg[:, col(i)])
        if i < 3:
            @pl.when(inner == 0)
            def _(i=i):
                wo_send(i)

            @pl.when(inner == 1)
            def _(i=i):
                wo_pass(0, i + 1)

    def a_copy(h):
        r = head_rows(h)
        return remote(at.at[r], abuf.at[r], S_A + h, pair_dev)

    def wq_swap(k, s, h):
        return remote(sq.at[k, s, h], rq.at[k, s, h], S_WQ + k * 8 + s * 4 + h, other_dev)

    def wq_back(s, h):
        return remote(sq.at[2, s, h], rq.at[2, s, h], S_WQ + 16 + s * 4 + h, pair_dev)

    def ncol(k):
        return pl.ds(pl.multiple_of(chunk(k) * CH - x_off, CH), CH)

    def spot(k, s, h=0, n=1):
        return prob.at[1 + k // 2, pl.ds(((k % 2) * 2 + s) * HE + h * HD, n * HD)]

    def wq_own(k, q):
        v = nn(at[pl.ds(0, HE), :], xg[:, pl.ds(pl.multiple_of(q * CH, CH), CH)])
        for s in range(2):
            spot(k, s, 0, NH)[...] = v[:, s * SC:(s + 1) * SC]

    def combine(h, ks=(0, 1)):
        if 0 in ks:
            a_copy(h).wait_recv()
        for k in ks:
            v = nn(abuf[head_rows(h), :], xn[:, ncol(k)])
            for s in range(2):
                sq[k, s, h] = (spot(k, s, h)[...] + v[:, s * SC:(s + 1) * SC]).astype(BF16)
                wq_swap(k, s, h).start()

    def outer(h):
        for s in range(2):
            wq_swap(0, s, h).wait_recv()
            sq[2, s, h] = (spot(3, s, h)[...] + rq[0, s, h].astype(F32)).astype(BF16)
            wq_back(s, h).start()

    def dout_block(b, carry):
        r = rows(b)
        dout[r, :] = nt(dyg[r, :], wo[...]).astype(BF16)
        return carry

    lax.fori_loop(0, NB, dout_block, 0)

    dkv[...] = jnp.zeros_like(dkv)

    def bwd_head(h, carry):
        hr = head_rows(h)
        for qi in range(NB):
            qr = pl.ds(qi * BLK, BLK)
            dob = dout[qr, hr]
            qb = qkv[qr, hr]
            delta = jnp.sum(dob.astype(F32).T * ot[hr, qr].astype(F32), axis=0, keepdims=True)
            for kj in range(qi + 1):
                kr = pl.ds(kj * BLK, BLK)
                p = prob[h, prow(qi, kj), :]
                dp = nt(qkv[kr, pl.ds(HE + HD, HD)], dob)
                ds = (p * (dp - delta)).astype(BF16)
                pbuf[kr, :] = ds
                dkv[kr, pl.ds(0, HD)] += nn(ds, qb)
                dkv[kr, pl.ds(HD, HD)] += nn(p.astype(BF16), dob)
            n = (qi + 1) * BLK
            dq = (nn(kt[:, pl.ds(0, n)], pbuf[pl.ds(0, n), :]) * scale).astype(BF16)
            at[hr, qr] = dq
            am[qr, hr] = dq.T

        @pl.when(inner == 0)
        def _():
            a_copy(h).start()

        @pl.when(inner == 1)
        def _():
            wo_pass(1, h)
            wo_return(h)

        return carry

    lax.fori_loop(0, NH, bwd_head, 0)

    dkb = (dkv[:, pl.ds(0, HD)] * scale).astype(BF16)
    dvb = dkv[:, pl.ds(HD, HD)].astype(BF16)
    am[:, pl.ds(HE, HD)] = dkb
    am[:, pl.ds(HE + HD, HD)] = dvb
    at[pl.ds(HE, HD), :] = dkb.T
    at[pl.ds(HE + HD, HD), :] = dvb.T

    def dx_part(block, put):
        def piece(i, carry):
            cs = pl.ds(pl.multiple_of(i * CH, CH), CH)
            put(i, cs, nt(am[rows(block), :], wqkv[cs, :]))
            return carry

        lax.fori_loop(0, DIM // CH, piece, 0)

    def px_copy(i):
        return remote(sx.at[i], rx.at[i], S_PX + i, core_dev)

    def py_copy(i):
        r = pl.ds(i * (BLK // 2), BLK // 2)
        return remote(sy.at[r], ry.at[r], S_PY + i, far_dev)

    def put_sx(j):
        def put(i, cs, v):
            sx[j, :, cs] = v.astype(BF16)
        return put

    def pxo(i, s):
        return prob.at[0, pl.ds(pl.multiple_of((2 * i + s) * BLK, BLK), BLK)]

    def put_own(i, cs, v):
        for s in range(2):
            pxo(i, s)[...] = v[:, s * SC:(s + 1) * SC]

    half = DIM // 2

    def kv_half(which):
        return nn(at[pl.ds(HE, 2 * HD), :], xg[:, pl.ds(pl.multiple_of(which * half, half), half)])

    def kcol(k):
        return pl.ds(pl.multiple_of(chunk(k) * KC, KC), KC)

    def kv_part(ref, slot, t):
        return ref.at[slot, pl.ds(t * HD, HD)]

    def kv_edge(k, t):
        return remote(kv_part(skv, k, t), kv_part(rkv, k, t), S_KV + 2 * k + t, pair_dev)

    def kv_swap(k, t):
        return remote(kv_part(skv, k, t), kv_part(rkv, 3 + k, t), S_KV + 2 * (3 + k) + t, other_dev)

    def kv_back(t):
        return remote(kv_part(skv, 2, t), kv_part(rkv, 3, t), S_KV + 10 + t, pair_dev)

    def kv_own(k, t):
        return pkv[pl.ds(t * HD, HD), kcol(k)]

    def kv_pass(k):
        for t in range(2):
            kv_edge(k, t).wait_recv()
            kv_part(skv, k, t)[...] = (kv_own(k, t) + kv_part(rkv, k, t)[...].astype(F32)).astype(BF16)
            kv_swap(k, t).start()

    kvs[...] = kv_half(1 - c).astype(BF16)
    kp_copy = remote(kvs, kvr, S_KP, core_dev)
    kp_copy.start()
    dx_part(diag_m, put_sx(0))
    px_copy(0).start()
    pkv[...] = kv_half(c)
    kp_copy.wait_recv()
    pkv[...] += kvr[...].astype(F32)

    @pl.when(inner == 0)
    def _():
        for k in range(3):
            for t in range(2):
                kv_part(skv, k, t)[...] = kv_own(k, t).astype(BF16)
                kv_edge(k, t).start()
    @pl.when(inner == 1)
    def _():
        xn_send(far_m, S_XNF, far_dev).wait_recv()
        xn_send(far_m, S_XNG, core_dev).start()
        wq_own(0, chunk(0))
        wq_own(1, chunk(1))

    dx_part(far_m, put_own)
    px_copy(0).wait_recv()
    for i in range(2):
        r = pl.ds(i * (BLK // 2), BLK // 2)
        for j in range(DIM // SC):
            cs = pl.ds(j * SC, SC)
            own = prob[0, pl.ds(j * BLK + i * (BLK // 2), BLK // 2), :]
            sy[r, cs] = (own + rx[0, r, cs].astype(F32)).astype(BF16)
        py_copy(i).start()

    @pl.when(inner == 1)
    def _():
        xn_send(core_m, S_XNC, core_dev).wait_recv()
        xn_send(diag_m, S_XNG, core_dev).wait_recv()
        combine(0)
        wq_own(3, chunk(3))
        combine(1)
        outer(0)

    dx_part(core_m, put_sx(1))
    px_copy(1).start()
    dx_part(m, put_own)
    wq_own(2, z)

    @pl.when(inner == 1)
    def _():
        combine(2)
        outer(1)
        combine(3, (0,))
        outer(2)
        v = nn(abuf[...], xn[:, ncol(2)])
        for s in range(2):
            spot(2, s, 0, NH)[...] += v[:, s * SC:(s + 1) * SC]
        kv_pass(0)
        combine(3, (1,))
        outer(3)
        kv_pass(1)
        for t in range(2):
            kv_swap(0, t).wait_recv()
            kv_part(skv, 2, t)[...] = (kv_own(3, t) + kv_part(rkv, 3, t)[...].astype(F32)).astype(BF16)
            kv_back(t).start()
        for h in range(NH):
            for s in range(2):
                wo_edge(2, s, h).wait_recv()
                wo_swap(1, s, h).wait_recv()
                woo[head_rows(h), half_col(s)] = pw[2, head_rows(h), half_col(s)] + ro[2, s, h].astype(F32) + ro[4, s, h].astype(F32)

    @pl.when(inner == 0)
    def _():
        for h in range(NH):
            for s in range(2):
                wo_back(s, h).wait_recv()
                woo[head_rows(h), half_col(s)] = pw[3, head_rows(h), half_col(s)] + ro[3, s, h].astype(F32)

    px_copy(1).wait_recv()
    for i in range(2):
        r = pl.ds(i * (BLK // 2), BLK // 2)
        py_copy(i).wait_recv()
        for j in range(DIM // SC):
            cs = pl.ds(j * SC, SC)
            own = prob[0, pl.ds(j * BLK + i * (BLK // 2), BLK // 2), :]
            dxo[r, cs] = (own + rx[1, r, cs].astype(F32) + ry[r, cs].astype(F32)).astype(BF16)

    def wq_put(h, s, got):
        wqo[pl.ds(s * SC * NH + h, SC, stride=NH), :] = (spot(2, s, h)[...] + got.astype(F32)).T

    kv_out = (dko, dvo)

    @pl.when(inner == 1)
    def _():
        for h in range(NH):
            for s in range(2):
                wq_swap(1, s, h).wait_recv()
                wq_put(h, s, rq[1, s, h])
        for t in range(2):
            kv_edge(2, t).wait_recv()
            kv_swap(1, t).wait_recv()
            kv_out[t][...] = (kv_own(2, t) + kv_part(rkv, 2, t)[...].astype(F32) + kv_part(rkv, 4, t)[...].astype(F32)).T

    @pl.when(inner == 0)
    def _():
        for h in range(NH):
            for s in range(2):
                wq_back(s, h).wait_recv()
                wq_put(h, s, rq[2, s, h])
        for t in range(2):
            kv_back(t).wait_recv()
            kv_out[t][...] = (kv_own(3, t) + kv_part(rkv, 3, t)[...].astype(F32)).T

    for i in range(NX - 1):
        x_far(i, m).wait_send()
    for i in range(NX):
        x_fwd(i, far_m).wait_send()
    x_core(m).wait_send()
    for i in range(5):
        dy_far(i, m).wait_send()
        dy_fwd(i, far_m).wait_send()
    dy_core(m).wait_send()
    @pl.when(inner == 0)
    def _():
        for j in range(NT):
            xt_edge(j).wait_send()
        xn_edge(m).wait_send()
        for h in range(NH):
            a_copy(h).wait_send()
        for k in range(3):
            for t in range(2):
                kv_edge(k, t).wait_send()
            for s in range(2):
                for h in range(NH):
                    wo_edge(k, s, h).wait_send()

    @pl.when(inner == 1)
    def _():
        x_far(NX - 1, m).wait_send()
        for j in range(NT):
            xt_far(j).wait_send()
        xt_back().wait_send()
        xn_send(m, S_XNF, far_dev).wait_send()
        xn_send(m, S_XNC, core_dev).wait_send()
        xn_send(far_m, S_XNG, core_dev).wait_send()
        for t in range(2):
            for k in range(2):
                kv_swap(k, t).wait_send()
            kv_back(t).wait_send()
        for s in range(2):
            for h in range(NH):
                for k in range(2):
                    wo_swap(k, s, h).wait_send()
                    wq_swap(k, s, h).wait_send()
                wo_back(s, h).wait_send()
                wq_back(s, h).wait_send()

    kp_copy.wait_send()
    for i in range(2):
        px_copy(i).wait_send()
        py_copy(i).wait_send()


def store_kernel(*refs):
    n = len(refs) // 2
    sem = refs[-1]
    copies = [pltpu.make_async_copy(refs[i], refs[n + i], sem.at[i]) for i in range(n)]
    for cp in copies:
        cp.start()
    for cp in copies:
        cp.wait()


def solution(mesh):
    tok_spec = P(('pod', 'data'), 'model', None)

    def device_step(x_loc, dy_loc, w_q, w_k, w_v, w_o):
        any_spec = pl.BlockSpec(memory_space=pl.ANY)
        vmem_spec = pl.BlockSpec(memory_space=pltpu.VMEM)
        outs = (((BLK, DIM), BF16), ((CH * NH, HD), F32), ((KC, HD), F32), ((KC, HD), F32), ((HE, CH), F32))
        dx, dwq, dwk, dwv, dwo = pl.pallas_call(
            step_kernel,
            out_shape=tuple(pltpu.VMEM(shape, dtype) for shape, dtype in outs),
            in_specs=[any_spec] * 6,
            out_specs=[vmem_spec] * 5,
            scratch_shapes=[
                pltpu.VMEM((SEQ, DIM), BF16),
                pltpu.VMEM((SEQ, DIM), BF16),
                pltpu.VMEM((2, WR, HD), BF16),
                pltpu.VMEM((WR, HD), F32),
                pltpu.VMEM((DIM, QKV), BF16),
                pltpu.VMEM((HE, DIM), BF16),
                pltpu.VMEM((SEQ, QKV), BF16),
                pltpu.VMEM((HD, SEQ), BF16),
                pltpu.VMEM((HD, SEQ), BF16),
                pltpu.VMEM((NH, CAUSAL_ROWS, BLK), F32),
                pltpu.VMEM((SEQ, BLK), BF16),
                pltpu.VMEM((HE, SEQ), BF16),
                pltpu.VMEM((SEQ, HE), BF16),
                pltpu.VMEM((QKV, SEQ), BF16),
                pltpu.VMEM((SEQ, QKV), BF16),
                pltpu.VMEM((SEQ, 2 * HD), F32),
                pltpu.VMEM((4, HE, CH), F32),
                pltpu.VMEM((2 * HD, DIM // 2), F32),
                pltpu.VMEM((2 * HD, DIM // 2), BF16),
                pltpu.VMEM((2 * HD, DIM // 2), BF16),
                pltpu.VMEM((3, 2, NH, HD, SC), BF16),
                pltpu.VMEM((5, 2, NH, HD, SC), BF16),
                pltpu.VMEM((3, 2, NH, HD, SC), BF16),
                pltpu.VMEM((3, 2, NH, HD, SC), BF16),
                pltpu.VMEM((3, 2 * HD, KC), BF16),
                pltpu.VMEM((5, 2 * HD, KC), BF16),
                pltpu.VMEM((2, BLK, DIM), BF16),
                pltpu.VMEM((2, BLK, DIM), BF16),
                pltpu.VMEM((BLK, DIM), BF16),
                pltpu.VMEM((BLK, DIM), BF16),
                pltpu.VMEM((SEQ, 3 * CH), BF16),
                pltpu.VMEM((XR, DIM), BF16),
                pltpu.VMEM((XR, DIM), BF16),
                pltpu.VMEM((HE, SEQ), BF16),
                pltpu.SemaphoreType.DMA((N_SEM,)),
                pltpu.SemaphoreType.DMA((N_SEM,)),
                pltpu.SemaphoreType.DMA((7,)),
            ],
            compiler_params=pltpu.CompilerParams(collective_id=0, has_side_effects=True, vmem_limit_bytes=VMEM_LIMIT),
        )(x_loc, dy_loc, w_q.reshape(DIM * NH, HD), w_k, w_v, w_o.reshape(HE, DIM))
        dx, dwq, dwk, dwv, dwo = pl.pallas_call(
            store_kernel,
            out_shape=tuple(jax.ShapeDtypeStruct(shape, dtype) for shape, dtype in outs),
            in_specs=[any_spec] * 5,
            out_specs=[any_spec] * 5,
            scratch_shapes=[pltpu.SemaphoreType.DMA((5,))],
            compiler_params=pltpu.CompilerParams(vmem_limit_bytes=2 ** 20),
        )(dx, dwq, dwk, dwv, dwo)
        return dx.reshape(1, BLK, DIM), dwq.reshape(CH, NH, HD), dwk, dwv, dwo.reshape(NH, HD, CH)

    kv_rows = P(('pod', 'model', 'data'), None)
    return jax.shard_map(device_step, mesh=mesh,
                         in_specs=(tok_spec, tok_spec, P(None, 'model', None), P(), P(), P('model', None, None)),
                         out_specs=(tok_spec, P(('pod', 'data'), 'model', None), kv_rows, kv_rows, P(('pod', 'model'), None, 'data')),
                         check_vma=False)
```

```python
import functools
import math

import jax
import jax.numpy as jnp
from jax import lax
from jax.experimental import pallas as pl
from jax.experimental.pallas import tpu as pltpu
from jax.sharding import PartitionSpec as P

MESH = pl.DeviceIdType.MESH
F32 = jnp.float32
BF16 = jnp.bfloat16

SEQ = 1024
BLK = 256
DIM = 2048
HD = 128
NH = 4
HE = NH * HD
QKV = HE + 2 * HD
CH = 512
SC = CH // 2
WR = 1024
KC = 256
NX = 8
XR = BLK // NX
NB = SEQ // BLK
CAUSAL_ROWS = BLK * NB * (NB + 1) // 2

S_XY, S_XF, S_XC = 0, 8, 16
S_DY, S_DF, S_DC = 17, 22, 27
S_KP = 28
S_PX = 29
S_PY = 31
S_XN, S_XNC, S_XNF, S_XNG = 33, 36, 37, 40
S_A = 43
S_WO = 47
S_WQ = 95
S_KV = 119
N_SEM = 131
VMEM_LIMIT = 63 * 2 ** 20 - 3328 * 1024


def nn(a, b):
    return lax.dot_general(a, b, (((1,), (0,)), ((), ())), preferred_element_type=F32)


def nt(a, b):
    return lax.dot_general(a, b, (((1,), (1,)), ((), ())), preferred_element_type=F32)


def step_kernel(x_in, dy_in, wq_in, wk_in, wv_in, wo_in, dxo, wqo, dko, dvo, woo,
                xg, dyg, wq8, wst, wqkv, wo, qkv, kt, vt, prob, pbuf, ot, dout, at, am, dkv, pw, pkv,
                kvs, kvr, so, ro, sq, rq, skv, rkv, sx, rx, sy, ry, xn, abuf, ssem, rsem, lsem):
    pod = lax.axis_index("pod")
    z = lax.axis_index("data")
    m = lax.axis_index("model")
    y = m // 2
    c = m % 2
    core_m = 2 * y + 1 - c
    far_m = (m + 2) % 4
    diag_m = (core_m + 2) % 4
    core_dev = (pod, z, core_m)
    far_dev = (pod, z, far_m)

    inner = ((z + 1) // 2) % 2
    pair_dev = (pod, z + 1 - 2 * (z % 2), m)
    other_dev = (pod, 3 - z, m)
    x_off = CH * (1 - z // 2)

    def rows(block, n=BLK, off=0):
        return pl.ds(pl.multiple_of(block * BLK + off, n), n)

    def chunk(i):
        return i + (1 - z // 2) * (3 - 2 * i)

    def col(i):
        return pl.ds(pl.multiple_of(chunk(i) * CH, CH), CH)

    def dcol(i):
        if i < 2:
            return pl.ds(pl.multiple_of(chunk(0) * CH + i * SC, SC), SC)
        return col(i - 1)

    def remote(src, dst, sem, dev):
        return pltpu.make_async_remote_copy(src_ref=src, dst_ref=dst, send_sem=ssem.at[sem], recv_sem=rsem.at[sem],
                                            device_id=dev, device_id_type=MESH)

    def head_rows(h):
        return pl.ds(pl.multiple_of(h * HD, HD), HD)

    loads = [
        pltpu.make_async_copy(x_in.at[0], xg.at[rows(m)], lsem.at[0]),
        pltpu.make_async_copy(dy_in.at[0], dyg.at[rows(m)], lsem.at[1]),
        pltpu.make_async_copy(wk_in.at[y], wqkv.at[:, pl.ds(HE, HD)], lsem.at[2]),
        pltpu.make_async_copy(wv_in.at[y], wqkv.at[:, pl.ds(HE + HD, HD)], lsem.at[3]),
        pltpu.make_async_copy(wo_in, wo, lsem.at[4]),
    ]
    def wq_load(i):
        return pltpu.make_async_copy(wq_in.at[pl.ds(pl.multiple_of(i * WR, WR), WR)], wq8.at[i % 2], lsem.at[5 + i % 2])

    for ld in loads:
        ld.start()
    wq_load(0).start()
    wq_load(1).start()

    barrier = pltpu.get_barrier_semaphore()
    for dev in (far_dev, core_dev, pair_dev):
        pl.semaphore_signal(barrier, inc=1, device_id=dev, device_id_type=MESH)

    @pl.when(inner == 1)
    def _():
        pl.semaphore_signal(barrier, inc=1, device_id=other_dev, device_id_type=MESH)

    pl.semaphore_wait(barrier, 3 + inner)

    def x_far(i, block):
        r = rows(block, XR, i * XR)
        return remote(xg.at[r], xg.at[r], S_XY + i, far_dev)

    def x_fwd(i, block):
        r = rows(block, XR, i * XR)
        return remote(xg.at[r], xg.at[r], S_XF + i, core_dev)

    def x_core(block):
        return remote(xg.at[rows(block)], xg.at[rows(block)], S_XC, core_dev)

    def dy_far(i, block):
        return remote(dyg.at[rows(block), dcol(i)], dyg.at[rows(block), dcol(i)], S_DY + i, far_dev)

    def dy_fwd(i, block):
        return remote(dyg.at[rows(block), dcol(i)], dyg.at[rows(block), dcol(i)], S_DF + i, core_dev)

    def dy_core(block):
        return remote(dyg.at[rows(block)], dyg.at[rows(block)], S_DC, core_dev)

    def ncol(k):
        return pl.ds(pl.multiple_of(chunk(k) * CH - x_off, CH), CH)

    def xn_edge(k):
        return remote(xg.at[rows(m), col(k)], xn.at[rows(m), ncol(k)], S_XN + k, pair_dev)

    def xn_core(block):
        return remote(xn.at[rows(block)], xn.at[rows(block)], S_XNC, core_dev)

    def xn_far(k, block):
        return remote(xn.at[rows(block), ncol(k)], xn.at[rows(block), ncol(k)], S_XNF + k, far_dev)

    def xn_fwd(k, block):
        return remote(xn.at[rows(block), ncol(k)], xn.at[rows(block), ncol(k)], S_XNG + k, core_dev)

    def take_xn(k):
        xn_far(k, far_m).wait_recv()
        xn_fwd(k, far_m).start()

    loads[0].wait()
    for i in range(NX):
        x_far(i, m).start()

    @pl.when(inner == 0)
    def _():
        for k in range(3):
            xn_edge(k).start()

    x_core(m).start()
    loads[1].wait()
    for i in range(5):
        dy_far(i, m).start()
    dy_core(m).start()
    for ld in loads[2:]:
        ld.wait()

    def wq_block(i, carry):
        wq_load(i).wait()
        wst[...] = wq8[i % 2].astype(F32)

        @pl.when(i + 2 < DIM * NH // WR)
        def _():
            wq_load(i + 2).start()

        for h in range(NH):
            wqkv[pl.ds(pl.multiple_of(i * (WR // NH), WR // NH), WR // NH), pl.ds(h * HD, HD)] = wst[pl.ds(h, WR // NH, stride=NH), :].astype(BF16)
        return carry

    lax.fori_loop(0, DIM * NH // WR, wq_block, 0)

    def project(r):
        qkv[r, :] = nn(xg[r, :], wqkv[...]).astype(BF16)

    def flip(block):
        r = rows(block)
        kt[:, r] = qkv[r, pl.ds(HE, HD)].T
        vt[:, r] = qkv[r, pl.ds(HE + HD, HD)].T

    project(rows(m))
    x_core(core_m).wait_recv()
    project(rows(core_m))
    flip(m)
    flip(core_m)

    def x_piece(i, carry):
        x_far(i, far_m).wait_recv()
        x_fwd(i, far_m).start()
        project(rows(far_m, XR, i * XR))
        x_fwd(i, diag_m).wait_recv()
        project(rows(diag_m, XR, i * XR))
        return carry

    lax.fori_loop(0, NX, x_piece, 0)

    flip(far_m)
    flip(diag_m)
    dy_core(core_m).wait_recv()

    def take_dy(i):
        dy_far(i, far_m).wait_recv()
        dy_fwd(i, far_m).start()

    def wo_sem(slot, s, h):
        return S_WO + slot * 8 + s * 4 + h

    def wo_edge(k, s, h):
        return remote(so.at[k, s, h], ro.at[k, s, h], wo_sem(k, s, h), pair_dev)

    def wo_swap(k, s, h):
        return remote(so.at[k, s, h], ro.at[3 + k, s, h], wo_sem(3 + k, s, h), other_dev)

    def wo_back(s, h):
        return remote(so.at[2, s, h], ro.at[3, s, h], wo_sem(5, s, h), pair_dev)

    def half_col(s):
        return pl.ds(s * SC, SC)

    def wo_pass(k, h):
        for s in range(2):
            wo_edge(k, s, h).wait_recv()
            so[k, s, h] = (pw[k, head_rows(h), half_col(s)] + ro[k, s, h].astype(F32)).astype(BF16)
            wo_swap(k, s, h).start()

    def wo_first(s, h):
        v = nn(ot[pl.ds(h * HD, HD), :], dyg[:, dcol(s)])

        @pl.when(inner == 0)
        def _():
            so[0, s, h] = v.astype(BF16)
            wo_edge(0, s, h).start()

        @pl.when(inner == 1)
        def _():
            pw[0, head_rows(h), half_col(s)] = v

    @pl.when(inner == 1)
    def _():
        for k in range(3):
            xn_edge(k).wait_recv()
            xn_far(k, m).start()
        xn_core(m).start()

    scale = HD ** -0.5
    exp_scale = scale * math.log2(math.e)
    diag_mask = lax.broadcasted_iota(jnp.int32, (BLK, BLK), 0) <= lax.broadcasted_iota(jnp.int32, (BLK, BLK), 1)

    def prow(qi, kj):
        return pl.ds(BLK * (qi * (qi + 1) // 2 + kj), BLK)

    def fwd_head(h, first_q, last_q):
        hr = pl.ds(h * HD, HD)
        for qi in range(first_q, last_q):
            qb = qkv[pl.ds(qi * BLK, BLK), hr]
            mx = None
            for kj in range(qi + 1):
                s = nt(qkv[pl.ds(kj * BLK, BLK), pl.ds(HE, HD)], qb)
                if kj == qi:
                    s = jnp.where(diag_mask, s, -jnp.inf)
                prob[h, prow(qi, kj), :] = s
                bm = jnp.max(s, axis=0, keepdims=True)
                mx = bm if mx is None else jnp.maximum(mx, bm)
            tot = None
            for kj in range(qi + 1):
                e = jnp.exp2((prob[h, prow(qi, kj), :] - mx) * exp_scale)
                prob[h, prow(qi, kj), :] = e
                bs = jnp.sum(e, axis=0, keepdims=True)
                tot = bs if tot is None else tot + bs
            inv = 1.0 / tot
            for kj in range(qi + 1):
                p = prob[h, prow(qi, kj), :] * inv
                prob[h, prow(qi, kj), :] = p
                pbuf[pl.ds(kj * BLK, BLK), :] = p.astype(BF16)
            n = (qi + 1) * BLK
            ot[hr, pl.ds(qi * BLK, BLK)] = nn(vt[:, pl.ds(0, n)], pbuf[pl.ds(0, n), :]).astype(BF16)

    fwd_head(0, 0, 3)
    take_dy(0)
    fwd_head(0, 3, NB)
    dy_fwd(0, diag_m).wait_recv()
    wo_first(0, 0)
    fwd_head(1, 0, 2)
    take_dy(1)
    fwd_head(1, 2, 3)
    dy_fwd(1, diag_m).wait_recv()
    wo_first(1, 0)
    fwd_head(1, 3, NB)
    wo_first(0, 1)
    wo_first(1, 1)
    for h in range(2, NH):
        fwd_head(h, 0, 3)
        if h == 3:
            take_dy(2)
        fwd_head(h, 3, NB)
        for s in range(2):
            wo_first(s, h)

        @pl.when(inner == 1)
        def _(h=h):
            wo_pass(0, h - 2)

    def wo_return(h):
        for s in range(2):
            wo_swap(0, s, h).wait_recv()
            so[2, s, h] = (pw[3, head_rows(h), half_col(s)] + ro[3, s, h].astype(F32)).astype(BF16)
            wo_back(s, h).start()

    def wo_send(k):
        for h in range(NH):
            for s in range(2):
                so[k, s, h] = pw[k, head_rows(h), half_col(s)].astype(BF16)
                wo_edge(k, s, h).start()

    for i in range(1, 4):
        if i > 1:
            take_dy(i + 1)
        dy_fwd(i + 1, diag_m).wait_recv()
        pw[i] = nn(ot[...], dyg[:, col(i)])
        if i < 3:
            if i == 1:
                @pl.when(inner == 0)
                def _():
                    wo_send(1)

            @pl.when(inner == 1)
            def _(i=i):
                wo_pass(0, i + 1)

    def a_copy(h):
        r = head_rows(h)
        return remote(at.at[r], abuf.at[r], S_A + h, pair_dev)

    def wq_swap(k, s, h):
        return remote(sq.at[k, s, h], rq.at[k, s, h], S_WQ + k * 8 + s * 4 + h, other_dev)

    def wq_back(s, h):
        return remote(sq.at[2, s, h], rq.at[2, s, h], S_WQ + 16 + s * 4 + h, pair_dev)

    def spot(k, s, h=0, n=1):
        return prob.at[1 + k // 2, pl.ds(((k % 2) * 2 + s) * HE + h * HD, n * HD)]

    def wq_own(k, q):
        v = nn(at[pl.ds(0, HE), :], xg[:, pl.ds(pl.multiple_of(q * CH, CH), CH)])
        for s in range(2):
            spot(k, s, 0, NH)[...] = v[:, s * SC:(s + 1) * SC]

    def combine(h, ks=(0, 1)):
        if 0 in ks:
            a_copy(h).wait_recv()
        for k in ks:
            v = nn(abuf[head_rows(h), :], xn[:, ncol(k)])
            for s in range(2):
                sq[k, s, h] = (spot(k, s, h)[...] + v[:, s * SC:(s + 1) * SC]).astype(BF16)
                wq_swap(k, s, h).start()

    def outer(h):
        for s in range(2):
            wq_swap(0, s, h).wait_recv()
            sq[2, s, h] = (spot(3, s, h)[...] + rq[0, s, h].astype(F32)).astype(BF16)
            wq_back(s, h).start()

    def dout_block(b, carry):
        r = rows(b)
        dout[r, :] = nt(dyg[r, :], wo[...]).astype(BF16)
        return carry

    lax.fori_loop(0, NB, dout_block, 0)

    dkv[...] = jnp.zeros_like(dkv)

    def bwd_head(h, carry):
        hr = head_rows(h)
        for qi in range(NB):
            qr = pl.ds(qi * BLK, BLK)
            dob = dout[qr, hr]
            qb = qkv[qr, hr]
            delta = jnp.sum(dob.astype(F32).T * ot[hr, qr].astype(F32), axis=0, keepdims=True)
            for kj in range(qi + 1):
                kr = pl.ds(kj * BLK, BLK)
                p = prob[h, prow(qi, kj), :]
                dp = nt(qkv[kr, pl.ds(HE + HD, HD)], dob)
                ds = (p * (dp - delta)).astype(BF16)
                pbuf[kr, :] = ds
                dkv[kr, pl.ds(0, HD)] += nn(ds, qb)
                dkv[kr, pl.ds(HD, HD)] += nn(p.astype(BF16), dob)
            n = (qi + 1) * BLK
            dq = (nn(kt[:, pl.ds(0, n)], pbuf[pl.ds(0, n), :]) * scale).astype(BF16)
            at[hr, qr] = dq
            am[qr, hr] = dq.T

        @pl.when(inner == 0)
        def _():
            a_copy(h).start()

        @pl.when(inner == 1)
        def _():
            wo_pass(1, h)
            wo_return(h)

            for at_h, piece in ((1, 0), (3, 1)):
                @pl.when(h == at_h)
                def _(piece=piece):
                    take_xn(piece)

        return carry

    lax.fori_loop(0, NH, bwd_head, 0)

    dkb = (dkv[:, pl.ds(0, HD)] * scale).astype(BF16)
    dvb = dkv[:, pl.ds(HD, HD)].astype(BF16)
    am[:, pl.ds(HE, HD)] = dkb
    am[:, pl.ds(HE + HD, HD)] = dvb
    at[pl.ds(HE, HD), :] = dkb.T
    at[pl.ds(HE + HD, HD), :] = dvb.T

    def dx_part(block, put):
        def piece(i, carry):
            cs = pl.ds(pl.multiple_of(i * CH, CH), CH)
            put(i, cs, nt(am[rows(block), :], wqkv[cs, :]))
            return carry

        lax.fori_loop(0, DIM // CH, piece, 0)

    def px_copy(i):
        return remote(sx.at[i], rx.at[i], S_PX + i, core_dev)

    def py_copy(i):
        r = pl.ds(i * (BLK // 2), BLK // 2)
        return remote(sy.at[r], ry.at[r], S_PY + i, far_dev)

    def put_sx(j):
        def put(i, cs, v):
            sx[j, :, cs] = v.astype(BF16)
        return put

    def pxo(i, s):
        return prob.at[0, pl.ds(pl.multiple_of((2 * i + s) * BLK, BLK), BLK)]

    def put_own(i, cs, v):
        for s in range(2):
            pxo(i, s)[...] = v[:, s * SC:(s + 1) * SC]

    half = DIM // 2

    def kv_half(which):
        return nn(at[pl.ds(HE, 2 * HD), :], xg[:, pl.ds(pl.multiple_of(which * half, half), half)])

    def kcol(k):
        return pl.ds(pl.multiple_of(chunk(k) * KC, KC), KC)

    def kv_part(ref, slot, t):
        return ref.at[slot, pl.ds(t * HD, HD)]

    def kv_edge(k, t):
        return remote(kv_part(skv, k, t), kv_part(rkv, k, t), S_KV + 2 * k + t, pair_dev)

    def kv_swap(k, t):
        return remote(kv_part(skv, k, t), kv_part(rkv, 3 + k, t), S_KV + 2 * (3 + k) + t, other_dev)

    def kv_back(t):
        return remote(kv_part(skv, 2, t), kv_part(rkv, 3, t), S_KV + 10 + t, pair_dev)

    def kv_own(k, t):
        return pkv[pl.ds(t * HD, HD), kcol(k)]

    def kv_pass(k):
        for t in range(2):
            kv_edge(k, t).wait_recv()
            kv_part(skv, k, t)[...] = (kv_own(k, t) + kv_part(rkv, k, t)[...].astype(F32)).astype(BF16)
            kv_swap(k, t).start()

    kvs[...] = kv_half(1 - c).astype(BF16)
    kp_copy = remote(kvs, kvr, S_KP, core_dev)
    kp_copy.start()
    dx_part(diag_m, put_sx(0))
    px_copy(0).start()
    pkv[...] = kv_half(c)
    kp_copy.wait_recv()
    pkv[...] += kvr[...].astype(F32)

    @pl.when(inner == 0)
    def _():
        for k in range(3):
            for t in range(2):
                kv_part(skv, k, t)[...] = kv_own(k, t).astype(BF16)
                kv_edge(k, t).start()
        wo_send(2)
    @pl.when(inner == 1)
    def _():
        wq_own(0, chunk(0))
        xn_core(core_m).wait_recv()
        xn_fwd(0, diag_m).wait_recv()
        combine(0, (0,))
        wq_own(1, chunk(1))
        xn_fwd(1, diag_m).wait_recv()
        combine(0, (1,))

    dx_part(far_m, put_own)
    px_copy(0).wait_recv()
    for i in range(2):
        r = pl.ds(i * (BLK // 2), BLK // 2)
        for j in range(DIM // SC):
            cs = pl.ds(j * SC, SC)
            own = prob[0, pl.ds(j * BLK + i * (BLK // 2), BLK // 2), :]
            sy[r, cs] = (own + rx[0, r, cs].astype(F32)).astype(BF16)
        py_copy(i).start()

    @pl.when(inner == 1)
    def _():
        combine(1)
        take_xn(2)
        wq_own(3, chunk(3))
        outer(0)
        combine(2)
        outer(1)

    dx_part(core_m, put_sx(1))
    px_copy(1).start()
    dx_part(m, put_own)
    wq_own(2, z)

    @pl.when(inner == 1)
    def _():
        combine(3, (0,))
        outer(2)
        kv_pass(0)
        combine(3, (1,))
        xn_fwd(2, diag_m).wait_recv()
        v = nn(abuf[...], xn[:, ncol(2)])
        for s in range(2):
            spot(2, s, 0, NH)[...] += v[:, s * SC:(s + 1) * SC]
        kv_pass(1)
        outer(3)
        for t in range(2):
            kv_swap(0, t).wait_recv()
            kv_part(skv, 2, t)[...] = (kv_own(3, t) + kv_part(rkv, 3, t)[...].astype(F32)).astype(BF16)
            kv_back(t).start()

    @pl.when(inner == 0)
    def _():
        for h in range(NH):
            for s in range(2):
                wo_back(s, h).wait_recv()
                woo[head_rows(h), half_col(s)] = pw[3, head_rows(h), half_col(s)] + ro[3, s, h].astype(F32)

    px_copy(1).wait_recv()
    for i in range(2):
        r = pl.ds(i * (BLK // 2), BLK // 2)
        py_copy(i).wait_recv()
        for j in range(DIM // SC):
            cs = pl.ds(j * SC, SC)
            own = prob[0, pl.ds(j * BLK + i * (BLK // 2), BLK // 2), :]
            dxo[r, cs] = (own + rx[1, r, cs].astype(F32) + ry[r, cs].astype(F32)).astype(BF16)

    def wq_put(h, s, got):
        wqo[pl.ds(s * SC * NH + h, SC, stride=NH), :] = (spot(2, s, h)[...] + got.astype(F32)).T

    kv_out = (dko, dvo)

    @pl.when(inner == 1)
    def _():
        for h in range(NH):
            for s in range(2):
                wq_swap(1, s, h).wait_recv()
                wq_put(h, s, rq[1, s, h])
        for t in range(2):
            kv_edge(2, t).wait_recv()
            kv_swap(1, t).wait_recv()
            kv_out[t][...] = (kv_own(2, t) + kv_part(rkv, 2, t)[...].astype(F32) + kv_part(rkv, 4, t)[...].astype(F32)).T
        for h in range(NH):
            for s in range(2):
                wo_edge(2, s, h).wait_recv()
                wo_swap(1, s, h).wait_recv()
                woo[head_rows(h), half_col(s)] = pw[2, head_rows(h), half_col(s)] + ro[2, s, h].astype(F32) + ro[4, s, h].astype(F32)

    @pl.when(inner == 0)
    def _():
        for h in range(NH):
            for s in range(2):
                wq_back(s, h).wait_recv()
                wq_put(h, s, rq[2, s, h])
        for t in range(2):
            kv_back(t).wait_recv()
            kv_out[t][...] = (kv_own(3, t) + kv_part(rkv, 3, t)[...].astype(F32)).T

    for i in range(NX):
        x_far(i, m).wait_send()
        x_fwd(i, far_m).wait_send()
    x_core(m).wait_send()
    for i in range(5):
        dy_far(i, m).wait_send()
        dy_fwd(i, far_m).wait_send()
    dy_core(m).wait_send()
    @pl.when(inner == 0)
    def _():
        for k in range(3):
            xn_edge(k).wait_send()
        for h in range(NH):
            a_copy(h).wait_send()
        for k in range(3):
            for t in range(2):
                kv_edge(k, t).wait_send()
            for s in range(2):
                for h in range(NH):
                    wo_edge(k, s, h).wait_send()

    @pl.when(inner == 1)
    def _():
        xn_core(m).wait_send()
        for k in range(3):
            xn_far(k, m).wait_send()
            xn_fwd(k, far_m).wait_send()
        for t in range(2):
            for k in range(2):
                kv_swap(k, t).wait_send()
            kv_back(t).wait_send()
        for s in range(2):
            for h in range(NH):
                for k in range(2):
                    wo_swap(k, s, h).wait_send()
                    wq_swap(k, s, h).wait_send()
                wo_back(s, h).wait_send()
                wq_back(s, h).wait_send()

    kp_copy.wait_send()
    for i in range(2):
        px_copy(i).wait_send()
        py_copy(i).wait_send()


def store_kernel(*refs):
    n = len(refs) // 2
    sem = refs[-1]
    copies = [pltpu.make_async_copy(refs[i], refs[n + i], sem.at[i]) for i in range(n)]
    for cp in copies:
        cp.start()
    for cp in copies:
        cp.wait()


def solution(mesh):
    tok_spec = P(('pod', 'data'), 'model', None)

    def device_step(x_loc, dy_loc, w_q, w_k, w_v, w_o):
        any_spec = pl.BlockSpec(memory_space=pl.ANY)
        vmem_spec = pl.BlockSpec(memory_space=pltpu.VMEM)
        outs = (((BLK, DIM), BF16), ((CH * NH, HD), F32), ((KC, HD), F32), ((KC, HD), F32), ((HE, CH), F32))
        dx, dwq, dwk, dwv, dwo = pl.pallas_call(
            step_kernel,
            out_shape=tuple(pltpu.VMEM(shape, dtype) for shape, dtype in outs),
            in_specs=[any_spec] * 6,
            out_specs=[vmem_spec] * 5,
            scratch_shapes=[
                pltpu.VMEM((SEQ, DIM), BF16),
                pltpu.VMEM((SEQ, DIM), BF16),
                pltpu.VMEM((2, WR, HD), BF16),
                pltpu.VMEM((WR, HD), F32),
                pltpu.VMEM((DIM, QKV), BF16),
                pltpu.VMEM((HE, DIM), BF16),
                pltpu.VMEM((SEQ, QKV), BF16),
                pltpu.VMEM((HD, SEQ), BF16),
                pltpu.VMEM((HD, SEQ), BF16),
                pltpu.VMEM((NH, CAUSAL_ROWS, BLK), F32),
                pltpu.VMEM((SEQ, BLK), BF16),
                pltpu.VMEM((HE, SEQ), BF16),
                pltpu.VMEM((SEQ, HE), BF16),
                pltpu.VMEM((QKV, SEQ), BF16),
                pltpu.VMEM((SEQ, QKV), BF16),
                pltpu.VMEM((SEQ, 2 * HD), F32),
                pltpu.VMEM((4, HE, CH), F32),
                pltpu.VMEM((2 * HD, DIM // 2), F32),
                pltpu.VMEM((2 * HD, DIM // 2), BF16),
                pltpu.VMEM((2 * HD, DIM // 2), BF16),
                pltpu.VMEM((3, 2, NH, HD, SC), BF16),
                pltpu.VMEM((5, 2, NH, HD, SC), BF16),
                pltpu.VMEM((3, 2, NH, HD, SC), BF16),
                pltpu.VMEM((3, 2, NH, HD, SC), BF16),
                pltpu.VMEM((3, 2 * HD, KC), BF16),
                pltpu.VMEM((5, 2 * HD, KC), BF16),
                pltpu.VMEM((2, BLK, DIM), BF16),
                pltpu.VMEM((2, BLK, DIM), BF16),
                pltpu.VMEM((BLK, DIM), BF16),
                pltpu.VMEM((BLK, DIM), BF16),
                pltpu.VMEM((SEQ, 3 * CH), BF16),
                pltpu.VMEM((HE, SEQ), BF16),
                pltpu.SemaphoreType.DMA((N_SEM,)),
                pltpu.SemaphoreType.DMA((N_SEM,)),
                pltpu.SemaphoreType.DMA((7,)),
            ],
            compiler_params=pltpu.CompilerParams(collective_id=0, has_side_effects=True, vmem_limit_bytes=VMEM_LIMIT),
        )(x_loc, dy_loc, w_q.reshape(DIM * NH, HD), w_k, w_v, w_o.reshape(HE, DIM))
        dx, dwq, dwk, dwv, dwo = pl.pallas_call(
            store_kernel,
            out_shape=tuple(jax.ShapeDtypeStruct(shape, dtype) for shape, dtype in outs),
            in_specs=[any_spec] * 5,
            out_specs=[any_spec] * 5,
            scratch_shapes=[pltpu.SemaphoreType.DMA((5,))],
            compiler_params=pltpu.CompilerParams(vmem_limit_bytes=2 ** 20),
        )(dx, dwq, dwk, dwv, dwo)
        return dx.reshape(1, BLK, DIM), dwq.reshape(CH, NH, HD), dwk, dwv, dwo.reshape(NH, HD, CH)

    kv_rows = P(('pod', 'model', 'data'), None)
    return jax.shard_map(device_step, mesh=mesh,
                         in_specs=(tok_spec, tok_spec, P(None, 'model', None), P(), P(), P('model', None, None)),
                         out_specs=(tok_spec, P(('pod', 'data'), 'model', None), kv_rows, kv_rows, P(('pod', 'model'), None, 'data')),
                         check_vma=False)
```

```python
import functools
import math

import jax
import jax.numpy as jnp
from jax import lax
from jax.experimental import pallas as pl
from jax.experimental.pallas import tpu as pltpu
from jax.sharding import PartitionSpec as P

MESH = pl.DeviceIdType.MESH
F32 = jnp.float32
BF16 = jnp.bfloat16

SEQ = 1024
BLK = 256
DIM = 2048
HD = 128
NH = 4
HE = NH * HD
QKV = HE + 2 * HD
CH = 512
SC = CH // 2
WR = 1024
KC = 256
NX = 8
XR = BLK // NX
NB = SEQ // BLK
CAUSAL_ROWS = BLK * NB * (NB + 1) // 2

S_XY, S_XF, S_XC = 0, 8, 16
S_DY, S_DF, S_DC = 17, 22, 27
S_KP = 28
S_PX = 29
S_PY = 31
S_XN, S_XNC, S_XNF, S_XNG = 33, 36, 37, 40
S_A = 43
S_WO = 47
S_WQ = 95
S_KV = 119
S_XT, S_XU = 131, 133
N_SEM = 135
NT = 2
XT = XR // NT
VMEM_LIMIT = 63 * 2 ** 20 - 3328 * 1024


def nn(a, b):
    return lax.dot_general(a, b, (((1,), (0,)), ((), ())), preferred_element_type=F32)


def nt(a, b):
    return lax.dot_general(a, b, (((1,), (1,)), ((), ())), preferred_element_type=F32)


def step_kernel(x_in, dy_in, wq_in, wk_in, wv_in, wo_in, dxo, wqo, dko, dvo, woo,
                xg, dyg, wq8, wst, wqkv, wo, qkv, kt, vt, prob, pbuf, ot, dout, at, am, dkv, pw, pkv,
                kvs, kvr, so, ro, sq, rq, skv, rkv, sx, rx, sy, ry, xn, xta, xtb, abuf, ssem, rsem, lsem):
    pod = lax.axis_index("pod")
    z = lax.axis_index("data")
    m = lax.axis_index("model")
    y = m // 2
    c = m % 2
    core_m = 2 * y + 1 - c
    far_m = (m + 2) % 4
    diag_m = (core_m + 2) % 4
    core_dev = (pod, z, core_m)
    far_dev = (pod, z, far_m)

    inner = ((z + 1) // 2) % 2
    pair_dev = (pod, z + 1 - 2 * (z % 2), m)
    other_dev = (pod, 3 - z, m)
    x_off = CH * (1 - z // 2)

    def rows(block, n=BLK, off=0):
        return pl.ds(pl.multiple_of(block * BLK + off, n), n)

    def chunk(i):
        return i + (1 - z // 2) * (3 - 2 * i)

    def col(i):
        return pl.ds(pl.multiple_of(chunk(i) * CH, CH), CH)

    def dcol(i):
        if i < 2:
            return pl.ds(pl.multiple_of(chunk(0) * CH + i * SC, SC), SC)
        return col(i - 1)

    def remote(src, dst, sem, dev):
        return pltpu.make_async_remote_copy(src_ref=src, dst_ref=dst, send_sem=ssem.at[sem], recv_sem=rsem.at[sem],
                                            device_id=dev, device_id_type=MESH)

    def head_rows(h):
        return pl.ds(pl.multiple_of(h * HD, HD), HD)

    loads = [
        pltpu.make_async_copy(x_in.at[0], xg.at[rows(m)], lsem.at[0]),
        pltpu.make_async_copy(dy_in.at[0], dyg.at[rows(m)], lsem.at[1]),
        pltpu.make_async_copy(wk_in.at[y], wqkv.at[:, pl.ds(HE, HD)], lsem.at[2]),
        pltpu.make_async_copy(wv_in.at[y], wqkv.at[:, pl.ds(HE + HD, HD)], lsem.at[3]),
        pltpu.make_async_copy(wo_in, wo, lsem.at[4]),
    ]
    def wq_load(i):
        return pltpu.make_async_copy(wq_in.at[pl.ds(pl.multiple_of(i * WR, WR), WR)], wq8.at[i % 2], lsem.at[5 + i % 2])

    for ld in loads:
        ld.start()
    wq_load(0).start()
    wq_load(1).start()

    barrier = pltpu.get_barrier_semaphore()
    for dev in (far_dev, core_dev, pair_dev):
        pl.semaphore_signal(barrier, inc=1, device_id=dev, device_id_type=MESH)

    @pl.when(inner == 1)
    def _():
        pl.semaphore_signal(barrier, inc=1, device_id=other_dev, device_id_type=MESH)

    pl.semaphore_wait(barrier, 3 + inner)

    def x_far(i, block):
        r = rows(block, XR, i * XR)
        return remote(xg.at[r], xg.at[r], S_XY + i, far_dev)

    def x_fwd(i, block):
        r = rows(block, XR, i * XR)
        return remote(xg.at[r], xg.at[r], S_XF + i, core_dev)

    def x_core(block):
        return remote(xg.at[rows(block)], xg.at[rows(block)], S_XC, core_dev)

    def dy_far(i, block):
        return remote(dyg.at[rows(block), dcol(i)], dyg.at[rows(block), dcol(i)], S_DY + i, far_dev)

    def dy_fwd(i, block):
        return remote(dyg.at[rows(block), dcol(i)], dyg.at[rows(block), dcol(i)], S_DF + i, core_dev)

    def dy_core(block):
        return remote(dyg.at[rows(block)], dyg.at[rows(block)], S_DC, core_dev)

    def ncol(k):
        return pl.ds(pl.multiple_of(chunk(k) * CH - x_off, CH), CH)

    def xn_edge(k):
        return remote(xg.at[rows(m), col(k)], xn.at[rows(m), ncol(k)], S_XN + k, pair_dev)

    def xn_core(block):
        return remote(xn.at[rows(block)], xn.at[rows(block)], S_XNC, core_dev)

    def xn_far(k, block):
        return remote(xn.at[rows(block), ncol(k)], xn.at[rows(block), ncol(k)], S_XNF + k, far_dev)

    def xn_fwd(k, block):
        return remote(xn.at[rows(block), ncol(k)], xn.at[rows(block), ncol(k)], S_XNG + k, core_dev)

    def take_xn(k):
        xn_far(k, far_m).wait_recv()
        xn_fwd(k, far_m).start()

    def xt_edge(j):
        return remote(xg.at[rows(m, XT, (NX - 1) * XR + j * XT)], xta.at[pl.ds(j * XT, XT)], S_XT + j, pair_dev)

    def xt_far(j):
        return remote(xta.at[pl.ds(j * XT, XT)], xtb.at[pl.ds(j * XT, XT)], S_XU + j, far_dev)

    def xt_back():
        return remote(xtb, xg.at[rows(far_m, XR, (NX - 1) * XR)], S_XY + NX - 1, pair_dev)

    loads[0].wait()
    for i in range(2):
        x_far(i, m).start()

    @pl.when(inner == 0)
    def _():
        for j in range(NT):
            xt_edge(j).start()
        for k in range(3):
            xn_edge(k).start()
        for i in range(2, NX - 1):
            x_far(i, m).start()

    x_core(m).start()
    loads[1].wait()

    @pl.when(inner == 0)
    def _():
        for i in range(5):
            dy_far(i, m).start()

    dy_core(m).start()
    for ld in loads[2:]:
        ld.wait()

    def wq_block(i, carry):
        wq_load(i).wait()
        wst[...] = wq8[i % 2].astype(F32)

        @pl.when(i + 2 < DIM * NH // WR)
        def _():
            wq_load(i + 2).start()

        for h in range(NH):
            wqkv[pl.ds(pl.multiple_of(i * (WR // NH), WR // NH), WR // NH), pl.ds(h * HD, HD)] = wst[pl.ds(h, WR // NH, stride=NH), :].astype(BF16)
        return carry

    lax.fori_loop(0, DIM * NH // WR, wq_block, 0)

    @pl.when(inner == 1)
    def _():
        for j in range(NT):
            xt_edge(j).wait_recv()
            xt_far(j).start()
        for i in range(2, NX):
            x_far(i, m).start()
        for i in range(5):
            dy_far(i, m).start()

    def project(r):
        qkv[r, :] = nn(xg[r, :], wqkv[...]).astype(BF16)

    def flip(block):
        r = rows(block)
        kt[:, r] = qkv[r, pl.ds(HE, HD)].T
        vt[:, r] = qkv[r, pl.ds(HE + HD, HD)].T

    project(rows(m))
    x_core(core_m).wait_recv()
    project(rows(core_m))
    flip(m)
    flip(core_m)

    @pl.when(inner == 1)
    def _():
        for j in range(NT):
            xt_far(j).wait_recv()
        xt_back().start()

    def x_piece(step, carry):
        i = step + (1 - inner) * (step // (NX - 2)) * (1 - 2 * (step % 2))
        x_far(i, far_m).wait_recv()
        x_fwd(i, far_m).start()
        project(rows(far_m, XR, i * XR))
        x_fwd(i, diag_m).wait_recv()
        project(rows(diag_m, XR, i * XR))
        return carry

    lax.fori_loop(0, NX, x_piece, 0)

    flip(far_m)
    flip(diag_m)
    dy_core(core_m).wait_recv()

    def take_dy(i):
        dy_far(i, far_m).wait_recv()
        dy_fwd(i, far_m).start()

    def wo_sem(slot, s, h):
        return S_WO + slot * 8 + s * 4 + h

    def wo_edge(k, s, h):
        return remote(so.at[k, s, h], ro.at[k, s, h], wo_sem(k, s, h), pair_dev)

    def wo_swap(k, s, h):
        return remote(so.at[k, s, h], ro.at[3 + k, s, h], wo_sem(3 + k, s, h), other_dev)

    def wo_back(s, h):
        return remote(so.at[2, s, h], ro.at[3, s, h], wo_sem(5, s, h), pair_dev)

    def half_col(s):
        return pl.ds(s * SC, SC)

    def wo_pass(k, h):
        for s in range(2):
            wo_edge(k, s, h).wait_recv()
            so[k, s, h] = (pw[k, head_rows(h), half_col(s)] + ro[k, s, h].astype(F32)).astype(BF16)
            wo_swap(k, s, h).start()

    def wo_first(s, h):
        v = nn(ot[pl.ds(h * HD, HD), :], dyg[:, dcol(s)])

        @pl.when(inner == 0)
        def _():
            so[0, s, h] = v.astype(BF16)
            wo_edge(0, s, h).start()

        @pl.when(inner == 1)
        def _():
            pw[0, head_rows(h), half_col(s)] = v

    @pl.when(inner == 1)
    def _():
        for k in range(3):
            xn_edge(k).wait_recv()
            xn_far(k, m).start()
        xn_core(m).start()

    scale = HD ** -0.5
    exp_scale = scale * math.log2(math.e)
    diag_mask = lax.broadcasted_iota(jnp.int32, (BLK, BLK), 0) <= lax.broadcasted_iota(jnp.int32, (BLK, BLK), 1)

    def prow(qi, kj):
        return pl.ds(BLK * (qi * (qi + 1) // 2 + kj), BLK)

    def fwd_head(h, first_q, last_q):
        hr = pl.ds(h * HD, HD)
        for qi in range(first_q, last_q):
            qb = qkv[pl.ds(qi * BLK, BLK), hr]
            mx = None
            for kj in range(qi + 1):
                s = nt(qkv[pl.ds(kj * BLK, BLK), pl.ds(HE, HD)], qb)
                if kj == qi:
                    s = jnp.where(diag_mask, s, -jnp.inf)
                prob[h, prow(qi, kj), :] = s
                bm = jnp.max(s, axis=0, keepdims=True)
                mx = bm if mx is None else jnp.maximum(mx, bm)
            tot = None
            for kj in range(qi + 1):
                e = jnp.exp2((prob[h, prow(qi, kj), :] - mx) * exp_scale)
                prob[h, prow(qi, kj), :] = e
                bs = jnp.sum(e, axis=0, keepdims=True)
                tot = bs if tot is None else tot + bs
            inv = 1.0 / tot
            for kj in range(qi + 1):
                p = prob[h, prow(qi, kj), :] * inv
                prob[h, prow(qi, kj), :] = p
                pbuf[pl.ds(kj * BLK, BLK), :] = p.astype(BF16)
            n = (qi + 1) * BLK
            ot[hr, pl.ds(qi * BLK, BLK)] = nn(vt[:, pl.ds(0, n)], pbuf[pl.ds(0, n), :]).astype(BF16)

    fwd_head(0, 0, 3)
    take_dy(0)
    fwd_head(0, 3, NB)
    dy_fwd(0, diag_m).wait_recv()
    wo_first(0, 0)
    fwd_head(1, 0, 2)
    take_dy(1)
    fwd_head(1, 2, 3)
    dy_fwd(1, diag_m).wait_recv()
    wo_first(1, 0)
    fwd_head(1, 3, NB)
    wo_first(0, 1)
    wo_first(1, 1)
    for h in range(2, NH):
        fwd_head(h, 0, 3)
        if h == 3:
            take_dy(2)
        fwd_head(h, 3, NB)
        for s in range(2):
            wo_first(s, h)

        @pl.when(inner == 1)
        def _(h=h):
            wo_pass(0, h - 2)

    def wo_return(h):
        for s in range(2):
            wo_swap(0, s, h).wait_recv()
            so[2, s, h] = (pw[3, head_rows(h), half_col(s)] + ro[3, s, h].astype(F32)).astype(BF16)
            wo_back(s, h).start()

    def wo_send(k):
        for h in range(NH):
            for s in range(2):
                so[k, s, h] = pw[k, head_rows(h), half_col(s)].astype(BF16)
                wo_edge(k, s, h).start()

    for i in range(1, 4):
        if i > 1:
            take_dy(i + 1)
        dy_fwd(i + 1, diag_m).wait_recv()
        pw[i] = nn(ot[...], dyg[:, col(i)])
        if i < 3:
            if i == 1:
                @pl.when(inner == 0)
                def _():
                    wo_send(1)

            @pl.when(inner == 1)
            def _(i=i):
                wo_pass(0, i + 1)

    def a_copy(h):
        r = head_rows(h)
        return remote(at.at[r], abuf.at[r], S_A + h, pair_dev)

    def wq_swap(k, s, h):
        return remote(sq.at[k, s, h], rq.at[k, s, h], S_WQ + k * 8 + s * 4 + h, other_dev)

    def wq_back(s, h):
        return remote(sq.at[2, s, h], rq.at[2, s, h], S_WQ + 16 + s * 4 + h, pair_dev)

    def spot(k, s, h=0, n=1):
        return prob.at[1 + k // 2, pl.ds(((k % 2) * 2 + s) * HE + h * HD, n * HD)]

    def wq_own(k, q):
        v = nn(at[pl.ds(0, HE), :], xg[:, pl.ds(pl.multiple_of(q * CH, CH), CH)])
        for s in range(2):
            spot(k, s, 0, NH)[...] = v[:, s * SC:(s + 1) * SC]

    def combine(h, ks=(0, 1)):
        if 0 in ks:
            a_copy(h).wait_recv()
        for k in ks:
            v = nn(abuf[head_rows(h), :], xn[:, ncol(k)])
            for s in range(2):
                sq[k, s, h] = (spot(k, s, h)[...] + v[:, s * SC:(s + 1) * SC]).astype(BF16)
                wq_swap(k, s, h).start()

    def outer(h):
        for s in range(2):
            wq_swap(0, s, h).wait_recv()
            sq[2, s, h] = (spot(3, s, h)[...] + rq[0, s, h].astype(F32)).astype(BF16)
            wq_back(s, h).start()

    def dout_block(b, carry):
        r = rows(b)
        dout[r, :] = nt(dyg[r, :], wo[...]).astype(BF16)
        return carry

    lax.fori_loop(0, NB, dout_block, 0)

    dkv[...] = jnp.zeros_like(dkv)

    def bwd_head(h, carry):
        hr = head_rows(h)
        for qi in range(NB):
            qr = pl.ds(qi * BLK, BLK)
            dob = dout[qr, hr]
            qb = qkv[qr, hr]
            delta = jnp.sum(dob.astype(F32).T * ot[hr, qr].astype(F32), axis=0, keepdims=True)
            for kj in range(qi + 1):
                kr = pl.ds(kj * BLK, BLK)
                p = prob[h, prow(qi, kj), :]
                dp = nt(qkv[kr, pl.ds(HE + HD, HD)], dob)
                ds = (p * (dp - delta)).astype(BF16)
                pbuf[kr, :] = ds
                dkv[kr, pl.ds(0, HD)] += nn(ds, qb)
                dkv[kr, pl.ds(HD, HD)] += nn(p.astype(BF16), dob)
            n = (qi + 1) * BLK
            dq = (nn(kt[:, pl.ds(0, n)], pbuf[pl.ds(0, n), :]) * scale).astype(BF16)
            at[hr, qr] = dq
            am[qr, hr] = dq.T

        @pl.when(inner == 0)
        def _():
            a_copy(h).start()

        @pl.when(inner == 1)
        def _():
            wo_pass(1, h)
            wo_return(h)

            @pl.when(h == 2)
            def _():
                take_xn(0)

        return carry

    lax.fori_loop(0, NH, bwd_head, 0)

    @pl.when(inner == 1)
    def _():
        take_xn(1)
        wq_own(0, chunk(0))
        xn_core(core_m).wait_recv()
        xn_fwd(0, diag_m).wait_recv()
        combine(0, (0,))

    dkb = (dkv[:, pl.ds(0, HD)] * scale).astype(BF16)
    dvb = dkv[:, pl.ds(HD, HD)].astype(BF16)
    am[:, pl.ds(HE, HD)] = dkb
    am[:, pl.ds(HE + HD, HD)] = dvb
    at[pl.ds(HE, HD), :] = dkb.T
    at[pl.ds(HE + HD, HD), :] = dvb.T

    def dx_part(block, put):
        def piece(i, carry):
            cs = pl.ds(pl.multiple_of(i * CH, CH), CH)
            put(i, cs, nt(am[rows(block), :], wqkv[cs, :]))
            return carry

        lax.fori_loop(0, DIM // CH, piece, 0)

    def px_copy(i):
        return remote(sx.at[i], rx.at[i], S_PX + i, core_dev)

    def py_copy(i):
        r = pl.ds(i * (BLK // 2), BLK // 2)
        return remote(sy.at[r], ry.at[r], S_PY + i, far_dev)

    def put_sx(j):
        def put(i, cs, v):
            sx[j, :, cs] = v.astype(BF16)
        return put

    def pxo(i, s):
        return prob.at[0, pl.ds(pl.multiple_of((2 * i + s) * BLK, BLK), BLK)]

    def put_own(i, cs, v):
        for s in range(2):
            pxo(i, s)[...] = v[:, s * SC:(s + 1) * SC]

    half = DIM // 2

    def kv_half(which):
        return nn(at[pl.ds(HE, 2 * HD), :], xg[:, pl.ds(pl.multiple_of(which * half, half), half)])

    def kcol(k):
        return pl.ds(pl.multiple_of(chunk(k) * KC, KC), KC)

    def kv_part(ref, slot, t):
        return ref.at[slot, pl.ds(t * HD, HD)]

    def kv_edge(k, t):
        return remote(kv_part(skv, k, t), kv_part(rkv, k, t), S_KV + 2 * k + t, pair_dev)

    def kv_swap(k, t):
        return remote(kv_part(skv, k, t), kv_part(rkv, 3 + k, t), S_KV + 2 * (3 + k) + t, other_dev)

    def kv_back(t):
        return remote(kv_part(skv, 2, t), kv_part(rkv, 3, t), S_KV + 10 + t, pair_dev)

    def kv_own(k, t):
        return pkv[pl.ds(t * HD, HD), kcol(k)]

    def kv_pass(k):
        for t in range(2):
            kv_edge(k, t).wait_recv()
            kv_part(skv, k, t)[...] = (kv_own(k, t) + kv_part(rkv, k, t)[...].astype(F32)).astype(BF16)
            kv_swap(k, t).start()

    kvs[...] = kv_half(1 - c).astype(BF16)
    kp_copy = remote(kvs, kvr, S_KP, core_dev)
    kp_copy.start()
    dx_part(diag_m, put_sx(0))
    px_copy(0).start()
    pkv[...] = kv_half(c)
    kp_copy.wait_recv()
    pkv[...] += kvr[...].astype(F32)

    @pl.when(inner == 0)
    def _():
        for k in range(3):
            for t in range(2):
                kv_part(skv, k, t)[...] = kv_own(k, t).astype(BF16)
                kv_edge(k, t).start()
        wo_send(2)
    @pl.when(inner == 1)
    def _():
        wq_own(1, chunk(1))
        xn_fwd(1, diag_m).wait_recv()
        combine(0, (1,))

    dx_part(far_m, put_own)
    px_copy(0).wait_recv()
    for i in range(2):
        r = pl.ds(i * (BLK // 2), BLK // 2)
        for j in range(DIM // SC):
            cs = pl.ds(j * SC, SC)
            own = prob[0, pl.ds(j * BLK + i * (BLK // 2), BLK // 2), :]
            sy[r, cs] = (own + rx[0, r, cs].astype(F32)).astype(BF16)
        py_copy(i).start()

    @pl.when(inner == 1)
    def _():
        combine(1)
        take_xn(2)
        wq_own(3, chunk(3))
        outer(0)
        combine(2)
        outer(1)

    dx_part(core_m, put_sx(1))
    px_copy(1).start()
    dx_part(m, put_own)
    wq_own(2, z)

    @pl.when(inner == 1)
    def _():
        combine(3, (0,))
        outer(2)
        kv_pass(0)
        combine(3, (1,))
        xn_fwd(2, diag_m).wait_recv()
        v = nn(abuf[...], xn[:, ncol(2)])
        for s in range(2):
            spot(2, s, 0, NH)[...] += v[:, s * SC:(s + 1) * SC]
        kv_pass(1)
        outer(3)
        for t in range(2):
            kv_swap(0, t).wait_recv()
            kv_part(skv, 2, t)[...] = (kv_own(3, t) + kv_part(rkv, 3, t)[...].astype(F32)).astype(BF16)
            kv_back(t).start()

    @pl.when(inner == 0)
    def _():
        for h in range(NH):
            for s in range(2):
                wo_back(s, h).wait_recv()
                woo[head_rows(h), half_col(s)] = pw[3, head_rows(h), half_col(s)] + ro[3, s, h].astype(F32)

    px_copy(1).wait_recv()
    for i in range(2):
        r = pl.ds(i * (BLK // 2), BLK // 2)
        py_copy(i).wait_recv()
        for j in range(DIM // SC):
            cs = pl.ds(j * SC, SC)
            own = prob[0, pl.ds(j * BLK + i * (BLK // 2), BLK // 2), :]
            dxo[r, cs] = (own + rx[1, r, cs].astype(F32) + ry[r, cs].astype(F32)).astype(BF16)

    def wq_put(h, s, got):
        wqo[pl.ds(s * SC * NH + h, SC, stride=NH), :] = (spot(2, s, h)[...] + got.astype(F32)).T

    kv_out = (dko, dvo)

    @pl.when(inner == 1)
    def _():
        for h in range(NH):
            for s in range(2):
                wq_swap(1, s, h).wait_recv()
                wq_put(h, s, rq[1, s, h])
        for t in range(2):
            kv_edge(2, t).wait_recv()
            kv_swap(1, t).wait_recv()
            kv_out[t][...] = (kv_own(2, t) + kv_part(rkv, 2, t)[...].astype(F32) + kv_part(rkv, 4, t)[...].astype(F32)).T
        for h in range(NH):
            for s in range(2):
                wo_edge(2, s, h).wait_recv()
                wo_swap(1, s, h).wait_recv()
                woo[head_rows(h), half_col(s)] = pw[2, head_rows(h), half_col(s)] + ro[2, s, h].astype(F32) + ro[4, s, h].astype(F32)

    @pl.when(inner == 0)
    def _():
        for h in range(NH):
            for s in range(2):
                wq_back(s, h).wait_recv()
                wq_put(h, s, rq[2, s, h])
        for t in range(2):
            kv_back(t).wait_recv()
            kv_out[t][...] = (kv_own(3, t) + kv_part(rkv, 3, t)[...].astype(F32)).T

    for i in range(NX - 1):
        x_far(i, m).wait_send()
    for i in range(NX):
        x_fwd(i, far_m).wait_send()
    x_core(m).wait_send()
    for i in range(5):
        dy_far(i, m).wait_send()
        dy_fwd(i, far_m).wait_send()
    dy_core(m).wait_send()
    @pl.when(inner == 0)
    def _():
        for j in range(NT):
            xt_edge(j).wait_send()
        for k in range(3):
            xn_edge(k).wait_send()
        for h in range(NH):
            a_copy(h).wait_send()
        for k in range(3):
            for t in range(2):
                kv_edge(k, t).wait_send()
            for s in range(2):
                for h in range(NH):
                    wo_edge(k, s, h).wait_send()

    @pl.when(inner == 1)
    def _():
        x_far(NX - 1, m).wait_send()
        for j in range(NT):
            xt_far(j).wait_send()
        xt_back().wait_send()
        xn_core(m).wait_send()
        for k in range(3):
            xn_far(k, m).wait_send()
            xn_fwd(k, far_m).wait_send()
        for t in range(2):
            for k in range(2):
                kv_swap(k, t).wait_send()
            kv_back(t).wait_send()
        for s in range(2):
            for h in range(NH):
                for k in range(2):
                    wo_swap(k, s, h).wait_send()
                    wq_swap(k, s, h).wait_send()
                wo_back(s, h).wait_send()
                wq_back(s, h).wait_send()

    kp_copy.wait_send()
    for i in range(2):
        px_copy(i).wait_send()
        py_copy(i).wait_send()


def store_kernel(*refs):
    n = len(refs) // 2
    sem = refs[-1]
    copies = [pltpu.make_async_copy(refs[i], refs[n + i], sem.at[i]) for i in range(n)]
    for cp in copies:
        cp.start()
    for cp in copies:
        cp.wait()


def solution(mesh):
    tok_spec = P(('pod', 'data'), 'model', None)

    def device_step(x_loc, dy_loc, w_q, w_k, w_v, w_o):
        any_spec = pl.BlockSpec(memory_space=pl.ANY)
        vmem_spec = pl.BlockSpec(memory_space=pltpu.VMEM)
        outs = (((BLK, DIM), BF16), ((CH * NH, HD), F32), ((KC, HD), F32), ((KC, HD), F32), ((HE, CH), F32))
        dx, dwq, dwk, dwv, dwo = pl.pallas_call(
            step_kernel,
            out_shape=tuple(pltpu.VMEM(shape, dtype) for shape, dtype in outs),
            in_specs=[any_spec] * 6,
            out_specs=[vmem_spec] * 5,
            scratch_shapes=[
                pltpu.VMEM((SEQ, DIM), BF16),
                pltpu.VMEM((SEQ, DIM), BF16),
                pltpu.VMEM((2, WR, HD), BF16),
                pltpu.VMEM((WR, HD), F32),
                pltpu.VMEM((DIM, QKV), BF16),
                pltpu.VMEM((HE, DIM), BF16),
                pltpu.VMEM((SEQ, QKV), BF16),
                pltpu.VMEM((HD, SEQ), BF16),
                pltpu.VMEM((HD, SEQ), BF16),
                pltpu.VMEM((NH, CAUSAL_ROWS, BLK), F32),
                pltpu.VMEM((SEQ, BLK), BF16),
                pltpu.VMEM((HE, SEQ), BF16),
                pltpu.VMEM((SEQ, HE), BF16),
                pltpu.VMEM((QKV, SEQ), BF16),
                pltpu.VMEM((SEQ, QKV), BF16),
                pltpu.VMEM((SEQ, 2 * HD), F32),
                pltpu.VMEM((4, HE, CH), F32),
                pltpu.VMEM((2 * HD, DIM // 2), F32),
                pltpu.VMEM((2 * HD, DIM // 2), BF16),
                pltpu.VMEM((2 * HD, DIM // 2), BF16),
                pltpu.VMEM((3, 2, NH, HD, SC), BF16),
                pltpu.VMEM((5, 2, NH, HD, SC), BF16),
                pltpu.VMEM((3, 2, NH, HD, SC), BF16),
                pltpu.VMEM((3, 2, NH, HD, SC), BF16),
                pltpu.VMEM((3, 2 * HD, KC), BF16),
                pltpu.VMEM((5, 2 * HD, KC), BF16),
                pltpu.VMEM((2, BLK, DIM), BF16),
                pltpu.VMEM((2, BLK, DIM), BF16),
                pltpu.VMEM((BLK, DIM), BF16),
                pltpu.VMEM((BLK, DIM), BF16),
                pltpu.VMEM((SEQ, 3 * CH), BF16),
                pltpu.VMEM((XR, DIM), BF16),
                pltpu.VMEM((XR, DIM), BF16),
                pltpu.VMEM((HE, SEQ), BF16),
                pltpu.SemaphoreType.DMA((N_SEM,)),
                pltpu.SemaphoreType.DMA((N_SEM,)),
                pltpu.SemaphoreType.DMA((7,)),
            ],
            compiler_params=pltpu.CompilerParams(collective_id=0, has_side_effects=True, vmem_limit_bytes=VMEM_LIMIT),
        )(x_loc, dy_loc, w_q.reshape(DIM * NH, HD), w_k, w_v, w_o.reshape(HE, DIM))
        dx, dwq, dwk, dwv, dwo = pl.pallas_call(
            store_kernel,
            out_shape=tuple(jax.ShapeDtypeStruct(shape, dtype) for shape, dtype in outs),
            in_specs=[any_spec] * 5,
            out_specs=[any_spec] * 5,
            scratch_shapes=[pltpu.SemaphoreType.DMA((5,))],
            compiler_params=pltpu.CompilerParams(vmem_limit_bytes=2 ** 20),
        )(dx, dwq, dwk, dwv, dwo)
        return dx.reshape(1, BLK, DIM), dwq.reshape(CH, NH, HD), dwk, dwv, dwo.reshape(NH, HD, CH)

    kv_rows = P(('pod', 'model', 'data'), None)
    return jax.shard_map(device_step, mesh=mesh,
                         in_specs=(tok_spec, tok_spec, P(None, 'model', None), P(), P(), P('model', None, None)),
                         out_specs=(tok_spec, P(('pod', 'data'), 'model', None), kv_rows, kv_rows, P(('pod', 'model'), None, 'data')),
                         check_vma=False)
```

```python
import functools
import math

import jax
import jax.numpy as jnp
from jax import lax
from jax.experimental import pallas as pl
from jax.experimental.pallas import tpu as pltpu
from jax.sharding import PartitionSpec as P

MESH = pl.DeviceIdType.MESH
F32 = jnp.float32
BF16 = jnp.bfloat16

SEQ = 1024
BLK = 256
DIM = 2048
HD = 128
NH = 4
HE = NH * HD
QKV = HE + 2 * HD
CH = 512
SC = CH // 2
WR = 1024
KC = 256
NX = 8
XR = BLK // NX
NB = SEQ // BLK
CAUSAL_ROWS = BLK * NB * (NB + 1) // 2

S_XY, S_XF, S_XC = 0, 8, 16
S_DY, S_DF, S_DC = 17, 22, 27
S_KP = 28
S_PX = 29
S_PY = 31
S_XN, S_XNC, S_XNF, S_XNG = 33, 36, 37, 40
S_A = 43
S_WO = 47
S_WQ = 95
S_KV = 119
S_XT, S_XU = 131, 133
N_SEM = 135
NT = 2
XT = XR // NT
VMEM_LIMIT = 63 * 2 ** 20 - 3328 * 1024


def nn(a, b):
    return lax.dot_general(a, b, (((1,), (0,)), ((), ())), preferred_element_type=F32)


def nt(a, b):
    return lax.dot_general(a, b, (((1,), (1,)), ((), ())), preferred_element_type=F32)


def step_kernel(x_in, dy_in, wq_in, wk_in, wv_in, wo_in, dxo, wqo, dko, dvo, woo,
                xg, dyg, wq8, wst, wqkv, wo, qkv, kt, vt, prob, pbuf, ot, dout, at, am, dkv, pw, pkv,
                kvs, kvr, so, ro, sq, rq, skv, rkv, sx, rx, sy, ry, xn, xta, xtb, abuf, ssem, rsem, lsem):
    pod = lax.axis_index("pod")
    z = lax.axis_index("data")
    m = lax.axis_index("model")
    y = m // 2
    c = m % 2
    core_m = 2 * y + 1 - c
    far_m = (m + 2) % 4
    diag_m = (core_m + 2) % 4
    core_dev = (pod, z, core_m)
    far_dev = (pod, z, far_m)

    inner = ((z + 1) // 2) % 2
    pair_dev = (pod, z + 1 - 2 * (z % 2), m)
    other_dev = (pod, 3 - z, m)
    x_off = CH * (1 - z // 2)

    def rows(block, n=BLK, off=0):
        return pl.ds(pl.multiple_of(block * BLK + off, n), n)

    def chunk(i):
        return i + (1 - z // 2) * (3 - 2 * i)

    def col(i):
        return pl.ds(pl.multiple_of(chunk(i) * CH, CH), CH)

    def dcol(i):
        if i < 2:
            return pl.ds(pl.multiple_of(chunk(0) * CH + i * SC, SC), SC)
        return col(i - 1)

    def remote(src, dst, sem, dev):
        return pltpu.make_async_remote_copy(src_ref=src, dst_ref=dst, send_sem=ssem.at[sem], recv_sem=rsem.at[sem],
                                            device_id=dev, device_id_type=MESH)

    def head_rows(h):
        return pl.ds(pl.multiple_of(h * HD, HD), HD)

    loads = [
        pltpu.make_async_copy(x_in.at[0], xg.at[rows(m)], lsem.at[0]),
        pltpu.make_async_copy(dy_in.at[0], dyg.at[rows(m)], lsem.at[1]),
        pltpu.make_async_copy(wk_in.at[y], wqkv.at[:, pl.ds(HE, HD)], lsem.at[2]),
        pltpu.make_async_copy(wv_in.at[y], wqkv.at[:, pl.ds(HE + HD, HD)], lsem.at[3]),
        pltpu.make_async_copy(wo_in, wo, lsem.at[4]),
    ]
    def wq_load(i):
        return pltpu.make_async_copy(wq_in.at[pl.ds(pl.multiple_of(i * WR, WR), WR)], wq8.at[i % 2], lsem.at[5 + i % 2])

    for ld in loads:
        ld.start()
    wq_load(0).start()
    wq_load(1).start()

    barrier = pltpu.get_barrier_semaphore()
    for dev in (far_dev, core_dev, pair_dev):
        pl.semaphore_signal(barrier, inc=1, device_id=dev, device_id_type=MESH)

    @pl.when(inner == 1)
    def _():
        pl.semaphore_signal(barrier, inc=1, device_id=other_dev, device_id_type=MESH)

    pl.semaphore_wait(barrier, 3 + inner)

    def x_far(i, block):
        r = rows(block, XR, i * XR)
        return remote(xg.at[r], xg.at[r], S_XY + i, far_dev)

    def x_fwd(i, block):
        r = rows(block, XR, i * XR)
        return remote(xg.at[r], xg.at[r], S_XF + i, core_dev)

    def x_core(block):
        return remote(xg.at[rows(block)], xg.at[rows(block)], S_XC, core_dev)

    def dy_far(i, block):
        return remote(dyg.at[rows(block), dcol(i)], dyg.at[rows(block), dcol(i)], S_DY + i, far_dev)

    def dy_fwd(i, block):
        return remote(dyg.at[rows(block), dcol(i)], dyg.at[rows(block), dcol(i)], S_DF + i, core_dev)

    def dy_core(block):
        return remote(dyg.at[rows(block)], dyg.at[rows(block)], S_DC, core_dev)

    def ncol(k):
        return pl.ds(pl.multiple_of(chunk(k) * CH - x_off, CH), CH)

    def xn_edge(k):
        return remote(xg.at[rows(m), col(k)], xn.at[rows(m), ncol(k)], S_XN + k, pair_dev)

    def xn_core(block):
        return remote(xn.at[rows(block)], xn.at[rows(block)], S_XNC, core_dev)

    def xn_far(k, block):
        return remote(xn.at[rows(block), ncol(k)], xn.at[rows(block), ncol(k)], S_XNF + k, far_dev)

    def xn_fwd(k, block):
        return remote(xn.at[rows(block), ncol(k)], xn.at[rows(block), ncol(k)], S_XNG + k, core_dev)

    def take_xn(k):
        xn_far(k, far_m).wait_recv()
        xn_fwd(k, far_m).start()

    def xt_edge(j):
        return remote(xg.at[rows(m, XT, (NX - 1) * XR + j * XT)], xta.at[pl.ds(j * XT, XT)], S_XT + j, pair_dev)

    def xt_far(j):
        return remote(xta.at[pl.ds(j * XT, XT)], xtb.at[pl.ds(j * XT, XT)], S_XU + j, far_dev)

    def xt_back():
        return remote(xtb, xg.at[rows(far_m, XR, (NX - 1) * XR)], S_XY + NX - 1, pair_dev)

    loads[0].wait()
    for i in range(2):
        x_far(i, m).start()

    @pl.when(inner == 0)
    def _():
        for j in range(NT):
            xt_edge(j).start()
        for k in range(3):
            xn_edge(k).start()
        for i in range(2, NX - 1):
            x_far(i, m).start()

    x_core(m).start()
    loads[1].wait()

    @pl.when(inner == 0)
    def _():
        for i in range(5):
            dy_far(i, m).start()

    dy_core(m).start()
    for ld in loads[2:]:
        ld.wait()

    def wq_block(i, carry):
        wq_load(i).wait()
        wst[...] = wq8[i % 2].astype(F32)

        @pl.when(i + 2 < DIM * NH // WR)
        def _():
            wq_load(i + 2).start()

        for h in range(NH):
            wqkv[pl.ds(pl.multiple_of(i * (WR // NH), WR // NH), WR // NH), pl.ds(h * HD, HD)] = wst[pl.ds(h, WR // NH, stride=NH), :].astype(BF16)
        return carry

    lax.fori_loop(0, DIM * NH // WR, wq_block, 0)

    @pl.when(inner == 1)
    def _():
        for j in range(NT):
            xt_edge(j).wait_recv()
            xt_far(j).start()
        for i in range(2, NX):
            x_far(i, m).start()
        for i in range(5):
            dy_far(i, m).start()

    def project(r):
        qkv[r, :] = nn(xg[r, :], wqkv[...]).astype(BF16)

    def flip(block):
        r = rows(block)
        kt[:, r] = qkv[r, pl.ds(HE, HD)].T
        vt[:, r] = qkv[r, pl.ds(HE + HD, HD)].T

    project(rows(m))
    x_core(core_m).wait_recv()
    project(rows(core_m))
    flip(m)
    flip(core_m)

    @pl.when(inner == 1)
    def _():
        for j in range(NT):
            xt_far(j).wait_recv()
        xt_back().start()

    def x_piece(step, carry):
        i = step + (1 - inner) * (step // (NX - 2)) * (1 - 2 * (step % 2))
        x_far(i, far_m).wait_recv()
        x_fwd(i, far_m).start()
        project(rows(far_m, XR, i * XR))
        x_fwd(i, diag_m).wait_recv()
        project(rows(diag_m, XR, i * XR))
        return carry

    lax.fori_loop(0, NX, x_piece, 0)

    flip(far_m)
    flip(diag_m)
    dy_core(core_m).wait_recv()

    def take_dy(i):
        dy_far(i, far_m).wait_recv()
        dy_fwd(i, far_m).start()

    def wo_sem(slot, s, h):
        return S_WO + slot * 8 + s * 4 + h

    def wo_edge(k, s, h):
        return remote(so.at[k, s, h], ro.at[k, s, h], wo_sem(k, s, h), pair_dev)

    def wo_swap(k, s, h):
        return remote(so.at[k, s, h], ro.at[3 + k, s, h], wo_sem(3 + k, s, h), other_dev)

    def wo_back(s, h):
        return remote(so.at[2, s, h], ro.at[3, s, h], wo_sem(5, s, h), pair_dev)

    def half_col(s):
        return pl.ds(s * SC, SC)

    def wo_pass(k, h):
        for s in range(2):
            wo_edge(k, s, h).wait_recv()
            so[k, s, h] = (pw[k, head_rows(h), half_col(s)] + ro[k, s, h].astype(F32)).astype(BF16)
            wo_swap(k, s, h).start()

    def wo_first(s, h):
        v = nn(ot[pl.ds(h * HD, HD), :], dyg[:, dcol(s)])

        @pl.when(inner == 0)
        def _():
            so[0, s, h] = v.astype(BF16)
            wo_edge(0, s, h).start()

        @pl.when(inner == 1)
        def _():
            pw[0, head_rows(h), half_col(s)] = v

    @pl.when(inner == 1)
    def _():
        for k in range(3):
            xn_edge(k).wait_recv()
            xn_far(k, m).start()
        xn_core(m).start()

    scale = HD ** -0.5
    exp_scale = scale * math.log2(math.e)
    diag_mask = lax.broadcasted_iota(jnp.int32, (BLK, BLK), 0) <= lax.broadcasted_iota(jnp.int32, (BLK, BLK), 1)

    def prow(qi, kj):
        return pl.ds(BLK * (qi * (qi + 1) // 2 + kj), BLK)

    def fwd_head(h, first_q, last_q):
        hr = pl.ds(h * HD, HD)
        for qi in range(first_q, last_q):
            qb = qkv[pl.ds(qi * BLK, BLK), hr]
            mx = None
            for kj in range(qi + 1):
                s = nt(qkv[pl.ds(kj * BLK, BLK), pl.ds(HE, HD)], qb)
                if kj == qi:
                    s = jnp.where(diag_mask, s, -jnp.inf)
                prob[h, prow(qi, kj), :] = s
                bm = jnp.max(s, axis=0, keepdims=True)
                mx = bm if mx is None else jnp.maximum(mx, bm)
            tot = None
            for kj in range(qi + 1):
                e = jnp.exp2((prob[h, prow(qi, kj), :] - mx) * exp_scale)
                prob[h, prow(qi, kj), :] = e
                bs = jnp.sum(e, axis=0, keepdims=True)
                tot = bs if tot is None else tot + bs
            inv = 1.0 / tot
            for kj in range(qi + 1):
                p = prob[h, prow(qi, kj), :] * inv
                prob[h, prow(qi, kj), :] = p
                pbuf[pl.ds(kj * BLK, BLK), :] = p.astype(BF16)
            n = (qi + 1) * BLK
            ot[hr, pl.ds(qi * BLK, BLK)] = nn(vt[:, pl.ds(0, n)], pbuf[pl.ds(0, n), :]).astype(BF16)

    fwd_head(0, 0, 3)
    take_dy(0)
    fwd_head(0, 3, NB)
    dy_fwd(0, diag_m).wait_recv()
    wo_first(0, 0)
    fwd_head(1, 0, 2)
    take_dy(1)
    fwd_head(1, 2, 3)
    dy_fwd(1, diag_m).wait_recv()
    wo_first(1, 0)
    fwd_head(1, 3, NB)
    wo_first(0, 1)
    wo_first(1, 1)
    for h in range(2, NH):
        fwd_head(h, 0, 3)
        if h == 3:
            take_dy(2)
        fwd_head(h, 3, NB)
        for s in range(2):
            wo_first(s, h)

        @pl.when(inner == 1)
        def _(h=h):
            wo_pass(0, h - 2)

    def wo_return(h):
        for s in range(2):
            wo_swap(0, s, h).wait_recv()
            so[2, s, h] = (pw[3, head_rows(h), half_col(s)] + ro[3, s, h].astype(F32)).astype(BF16)
            wo_back(s, h).start()

    def wo_send(k):
        for h in range(NH):
            for s in range(2):
                so[k, s, h] = pw[k, head_rows(h), half_col(s)].astype(BF16)
                wo_edge(k, s, h).start()

    for i in range(1, 4):
        if i > 1:
            take_dy(i + 1)
        dy_fwd(i + 1, diag_m).wait_recv()
        pw[i] = nn(ot[...], dyg[:, col(i)])
        if i < 3:
            if i == 1:
                @pl.when(inner == 0)
                def _():
                    wo_send(1)

            @pl.when(inner == 1)
            def _(i=i):
                wo_pass(0, i + 1)

    def a_copy(h):
        r = head_rows(h)
        return remote(at.at[r], abuf.at[r], S_A + h, pair_dev)

    def wq_swap(k, s, h):
        return remote(sq.at[k, s, h], rq.at[k, s, h], S_WQ + k * 8 + s * 4 + h, other_dev)

    def wq_back(s, h):
        return remote(sq.at[2, s, h], rq.at[2, s, h], S_WQ + 16 + s * 4 + h, pair_dev)

    def spot(k, s, h=0, n=1):
        return prob.at[1 + k // 2, pl.ds(((k % 2) * 2 + s) * HE + h * HD, n * HD)]

    def wq_own(k, q):
        v = nn(at[pl.ds(0, HE), :], xg[:, pl.ds(pl.multiple_of(q * CH, CH), CH)])
        for s in range(2):
            spot(k, s, 0, NH)[...] = v[:, s * SC:(s + 1) * SC]

    def combine(h, ks=(0, 1)):
        if 0 in ks:
            a_copy(h).wait_recv()
        for k in ks:
            v = nn(abuf[head_rows(h), :], xn[:, ncol(k)])
            for s in range(2):
                sq[k, s, h] = (spot(k, s, h)[...] + v[:, s * SC:(s + 1) * SC]).astype(BF16)
                wq_swap(k, s, h).start()

    def outer(h):
        for s in range(2):
            wq_swap(0, s, h).wait_recv()
            sq[2, s, h] = (spot(3, s, h)[...] + rq[0, s, h].astype(F32)).astype(BF16)
            wq_back(s, h).start()

    def dout_block(b, carry):
        r = rows(b)
        dout[r, :] = nt(dyg[r, :], wo[...]).astype(BF16)
        return carry

    lax.fori_loop(0, NB, dout_block, 0)

    dkv[...] = jnp.zeros_like(dkv)

    def bwd_head(h, carry):
        hr = head_rows(h)
        for qi in range(NB):
            qr = pl.ds(qi * BLK, BLK)
            dob = dout[qr, hr]
            qb = qkv[qr, hr]
            delta = jnp.sum(dob.astype(F32).T * ot[hr, qr].astype(F32), axis=0, keepdims=True)
            for kj in range(qi + 1):
                kr = pl.ds(kj * BLK, BLK)
                p = prob[h, prow(qi, kj), :]
                dp = nt(qkv[kr, pl.ds(HE + HD, HD)], dob)
                ds = (p * (dp - delta)).astype(BF16)
                pbuf[kr, :] = ds
                dkv[kr, pl.ds(0, HD)] += nn(ds, qb)
                dkv[kr, pl.ds(HD, HD)] += nn(p.astype(BF16), dob)
            n = (qi + 1) * BLK
            dq = (nn(kt[:, pl.ds(0, n)], pbuf[pl.ds(0, n), :]) * scale).astype(BF16)
            at[hr, qr] = dq
            am[qr, hr] = dq.T

        @pl.when(inner == 0)
        def _():
            a_copy(h).start()

        @pl.when(inner == 1)
        def _():
            wo_pass(1, h)
            wo_return(h)

            @pl.when(h == 2)
            def _():
                take_xn(0)

        return carry

    lax.fori_loop(0, NH, bwd_head, 0)

    @pl.when(inner == 1)
    def _():
        take_xn(1)
        wq_own(0, chunk(0))
        xn_core(core_m).wait_recv()
        xn_fwd(0, diag_m).wait_recv()
        combine(0, (0,))
        combine(1, (0,))

    dkb = (dkv[:, pl.ds(0, HD)] * scale).astype(BF16)
    dvb = dkv[:, pl.ds(HD, HD)].astype(BF16)
    am[:, pl.ds(HE, HD)] = dkb
    am[:, pl.ds(HE + HD, HD)] = dvb
    at[pl.ds(HE, HD), :] = dkb.T
    at[pl.ds(HE + HD, HD), :] = dvb.T

    def dx_part(block, put):
        def piece(i, carry):
            cs = pl.ds(pl.multiple_of(i * CH, CH), CH)
            put(i, cs, nt(am[rows(block), :], wqkv[cs, :]))
            return carry

        lax.fori_loop(0, DIM // CH, piece, 0)

    def px_copy(i):
        return remote(sx.at[i], rx.at[i], S_PX + i, core_dev)

    def py_copy(i):
        r = pl.ds(i * (BLK // 2), BLK // 2)
        return remote(sy.at[r], ry.at[r], S_PY + i, far_dev)

    def put_sx(j):
        def put(i, cs, v):
            sx[j, :, cs] = v.astype(BF16)
        return put

    def pxo(i, s):
        return prob.at[0, pl.ds(pl.multiple_of((2 * i + s) * BLK, BLK), BLK)]

    def put_own(i, cs, v):
        for s in range(2):
            pxo(i, s)[...] = v[:, s * SC:(s + 1) * SC]

    half = DIM // 2

    def kv_half(which):
        return nn(at[pl.ds(HE, 2 * HD), :], xg[:, pl.ds(pl.multiple_of(which * half, half), half)])

    def kcol(k):
        return pl.ds(pl.multiple_of(chunk(k) * KC, KC), KC)

    def kv_part(ref, slot, t):
        return ref.at[slot, pl.ds(t * HD, HD)]

    def kv_edge(k, t):
        return remote(kv_part(skv, k, t), kv_part(rkv, k, t), S_KV + 2 * k + t, pair_dev)

    def kv_swap(k, t):
        return remote(kv_part(skv, k, t), kv_part(rkv, 3 + k, t), S_KV + 2 * (3 + k) + t, other_dev)

    def kv_back(t):
        return remote(kv_part(skv, 2, t), kv_part(rkv, 3, t), S_KV + 10 + t, pair_dev)

    def kv_own(k, t):
        return pkv[pl.ds(t * HD, HD), kcol(k)]

    def kv_pass(k):
        for t in range(2):
            kv_edge(k, t).wait_recv()
            kv_part(skv, k, t)[...] = (kv_own(k, t) + kv_part(rkv, k, t)[...].astype(F32)).astype(BF16)
            kv_swap(k, t).start()

    dx_part(diag_m, put_sx(0))
    px_copy(0).start()
    dx_part(far_m, put_own)
    px_copy(0).wait_recv()
    for i in range(2):
        r = pl.ds(i * (BLK // 2), BLK // 2)
        for j in range(DIM // SC):
            cs = pl.ds(j * SC, SC)
            own = prob[0, pl.ds(j * BLK + i * (BLK // 2), BLK // 2), :]
            sy[r, cs] = (own + rx[0, r, cs].astype(F32)).astype(BF16)
        py_copy(i).start()

    @pl.when(inner == 1)
    def _():
        wq_own(1, chunk(1))
        xn_fwd(1, diag_m).wait_recv()
        combine(0, (1,))
        combine(1, (1,))

    kvs[...] = kv_half(1 - c).astype(BF16)
    kp_copy = remote(kvs, kvr, S_KP, core_dev)
    kp_copy.start()
    pkv[...] = kv_half(c)
    kp_copy.wait_recv()
    pkv[...] += kvr[...].astype(F32)

    @pl.when(inner == 0)
    def _():
        for k in range(3):
            for t in range(2):
                kv_part(skv, k, t)[...] = kv_own(k, t).astype(BF16)
                kv_edge(k, t).start()
        wo_send(2)
    @pl.when(inner == 1)
    def _():
        combine(2)
        take_xn(2)
        wq_own(3, chunk(3))
        outer(0)
        outer(1)

    dx_part(core_m, put_sx(1))
    px_copy(1).start()
    dx_part(m, put_own)
    wq_own(2, z)

    @pl.when(inner == 1)
    def _():
        combine(3, (0,))
        outer(2)
        kv_pass(0)
        combine(3, (1,))
        xn_fwd(2, diag_m).wait_recv()
        v = nn(abuf[...], xn[:, ncol(2)])
        for s in range(2):
            spot(2, s, 0, NH)[...] += v[:, s * SC:(s + 1) * SC]
        kv_pass(1)
        outer(3)
        for t in range(2):
            kv_swap(0, t).wait_recv()
            kv_part(skv, 2, t)[...] = (kv_own(3, t) + kv_part(rkv, 3, t)[...].astype(F32)).astype(BF16)
            kv_back(t).start()

    @pl.when(inner == 0)
    def _():
        for h in range(NH):
            for s in range(2):
                wo_back(s, h).wait_recv()
                woo[head_rows(h), half_col(s)] = pw[3, head_rows(h), half_col(s)] + ro[3, s, h].astype(F32)

    px_copy(1).wait_recv()
    for i in range(2):
        r = pl.ds(i * (BLK // 2), BLK // 2)
        py_copy(i).wait_recv()
        for j in range(DIM // SC):
            cs = pl.ds(j * SC, SC)
            own = prob[0, pl.ds(j * BLK + i * (BLK // 2), BLK // 2), :]
            dxo[r, cs] = (own + rx[1, r, cs].astype(F32) + ry[r, cs].astype(F32)).astype(BF16)

    def wq_put(h, s, got):
        wqo[pl.ds(s * SC * NH + h, SC, stride=NH), :] = (spot(2, s, h)[...] + got.astype(F32)).T

    kv_out = (dko, dvo)

    @pl.when(inner == 1)
    def _():
        for h in range(NH):
            for s in range(2):
                wq_swap(1, s, h).wait_recv()
                wq_put(h, s, rq[1, s, h])
        for t in range(2):
            kv_edge(2, t).wait_recv()
            kv_swap(1, t).wait_recv()
            kv_out[t][...] = (kv_own(2, t) + kv_part(rkv, 2, t)[...].astype(F32) + kv_part(rkv, 4, t)[...].astype(F32)).T
        for h in range(NH):
            for s in range(2):
                wo_edge(2, s, h).wait_recv()
                wo_swap(1, s, h).wait_recv()
                woo[head_rows(h), half_col(s)] = pw[2, head_rows(h), half_col(s)] + ro[2, s, h].astype(F32) + ro[4, s, h].astype(F32)

    @pl.when(inner == 0)
    def _():
        for h in range(NH):
            for s in range(2):
                wq_back(s, h).wait_recv()
                wq_put(h, s, rq[2, s, h])
        for t in range(2):
            kv_back(t).wait_recv()
            kv_out[t][...] = (kv_own(3, t) + kv_part(rkv, 3, t)[...].astype(F32)).T

    for i in range(NX - 1):
        x_far(i, m).wait_send()
    for i in range(NX):
        x_fwd(i, far_m).wait_send()
    x_core(m).wait_send()
    for i in range(5):
        dy_far(i, m).wait_send()
        dy_fwd(i, far_m).wait_send()
    dy_core(m).wait_send()
    @pl.when(inner == 0)
    def _():
        for j in range(NT):
            xt_edge(j).wait_send()
        for k in range(3):
            xn_edge(k).wait_send()
        for h in range(NH):
            a_copy(h).wait_send()
        for k in range(3):
            for t in range(2):
                kv_edge(k, t).wait_send()
            for s in range(2):
                for h in range(NH):
                    wo_edge(k, s, h).wait_send()

    @pl.when(inner == 1)
    def _():
        x_far(NX - 1, m).wait_send()
        for j in range(NT):
            xt_far(j).wait_send()
        xt_back().wait_send()
        xn_core(m).wait_send()
        for k in range(3):
            xn_far(k, m).wait_send()
            xn_fwd(k, far_m).wait_send()
        for t in range(2):
            for k in range(2):
                kv_swap(k, t).wait_send()
            kv_back(t).wait_send()
        for s in range(2):
            for h in range(NH):
                for k in range(2):
                    wo_swap(k, s, h).wait_send()
                    wq_swap(k, s, h).wait_send()
                wo_back(s, h).wait_send()
                wq_back(s, h).wait_send()

    kp_copy.wait_send()
    for i in range(2):
        px_copy(i).wait_send()
        py_copy(i).wait_send()


def store_kernel(*refs):
    n = len(refs) // 2
    sem = refs[-1]
    copies = [pltpu.make_async_copy(refs[i], refs[n + i], sem.at[i]) for i in range(n)]
    for cp in copies:
        cp.start()
    for cp in copies:
        cp.wait()


def solution(mesh):
    tok_spec = P(('pod', 'data'), 'model', None)

    def device_step(x_loc, dy_loc, w_q, w_k, w_v, w_o):
        any_spec = pl.BlockSpec(memory_space=pl.ANY)
        vmem_spec = pl.BlockSpec(memory_space=pltpu.VMEM)
        outs = (((BLK, DIM), BF16), ((CH * NH, HD), F32), ((KC, HD), F32), ((KC, HD), F32), ((HE, CH), F32))
        dx, dwq, dwk, dwv, dwo = pl.pallas_call(
            step_kernel,
            out_shape=tuple(pltpu.VMEM(shape, dtype) for shape, dtype in outs),
            in_specs=[any_spec] * 6,
            out_specs=[vmem_spec] * 5,
            scratch_shapes=[
                pltpu.VMEM((SEQ, DIM), BF16),
                pltpu.VMEM((SEQ, DIM), BF16),
                pltpu.VMEM((2, WR, HD), BF16),
                pltpu.VMEM((WR, HD), F32),
                pltpu.VMEM((DIM, QKV), BF16),
                pltpu.VMEM((HE, DIM), BF16),
                pltpu.VMEM((SEQ, QKV), BF16),
                pltpu.VMEM((HD, SEQ), BF16),
                pltpu.VMEM((HD, SEQ), BF16),
                pltpu.VMEM((NH, CAUSAL_ROWS, BLK), F32),
                pltpu.VMEM((SEQ, BLK), BF16),
                pltpu.VMEM((HE, SEQ), BF16),
                pltpu.VMEM((SEQ, HE), BF16),
                pltpu.VMEM((QKV, SEQ), BF16),
                pltpu.VMEM((SEQ, QKV), BF16),
                pltpu.VMEM((SEQ, 2 * HD), F32),
                pltpu.VMEM((4, HE, CH), F32),
                pltpu.VMEM((2 * HD, DIM // 2), F32),
                pltpu.VMEM((2 * HD, DIM // 2), BF16),
                pltpu.VMEM((2 * HD, DIM // 2), BF16),
                pltpu.VMEM((3, 2, NH, HD, SC), BF16),
                pltpu.VMEM((5, 2, NH, HD, SC), BF16),
                pltpu.VMEM((3, 2, NH, HD, SC), BF16),
                pltpu.VMEM((3, 2, NH, HD, SC), BF16),
                pltpu.VMEM((3, 2 * HD, KC), BF16),
                pltpu.VMEM((5, 2 * HD, KC), BF16),
                pltpu.VMEM((2, BLK, DIM), BF16),
                pltpu.VMEM((2, BLK, DIM), BF16),
                pltpu.VMEM((BLK, DIM), BF16),
                pltpu.VMEM((BLK, DIM), BF16),
                pltpu.VMEM((SEQ, 3 * CH), BF16),
                pltpu.VMEM((XR, DIM), BF16),
                pltpu.VMEM((XR, DIM), BF16),
                pltpu.VMEM((HE, SEQ), BF16),
                pltpu.SemaphoreType.DMA((N_SEM,)),
                pltpu.SemaphoreType.DMA((N_SEM,)),
                pltpu.SemaphoreType.DMA((7,)),
            ],
            compiler_params=pltpu.CompilerParams(collective_id=0, has_side_effects=True, vmem_limit_bytes=VMEM_LIMIT),
        )(x_loc, dy_loc, w_q.reshape(DIM * NH, HD), w_k, w_v, w_o.reshape(HE, DIM))
        dx, dwq, dwk, dwv, dwo = pl.pallas_call(
            store_kernel,
            out_shape=tuple(jax.ShapeDtypeStruct(shape, dtype) for shape, dtype in outs),
            in_specs=[any_spec] * 5,
            out_specs=[any_spec] * 5,
            scratch_shapes=[pltpu.SemaphoreType.DMA((5,))],
            compiler_params=pltpu.CompilerParams(vmem_limit_bytes=2 ** 20),
        )(dx, dwq, dwk, dwv, dwo)
        return dx.reshape(1, BLK, DIM), dwq.reshape(CH, NH, HD), dwk, dwv, dwo.reshape(NH, HD, CH)

    kv_rows = P(('pod', 'model', 'data'), None)
    return jax.shard_map(device_step, mesh=mesh,
                         in_specs=(tok_spec, tok_spec, P(None, 'model', None), P(), P(), P('model', None, None)),
                         out_specs=(tok_spec, P(('pod', 'data'), 'model', None), kv_rows, kv_rows, P(('pod', 'model'), None, 'data')),
                         check_vma=False)
```

```python
import functools
import math

import jax
import jax.numpy as jnp
from jax import lax
from jax.experimental import pallas as pl
from jax.experimental.pallas import tpu as pltpu
from jax.sharding import PartitionSpec as P

MESH = pl.DeviceIdType.MESH
F32 = jnp.float32
BF16 = jnp.bfloat16

SEQ = 1024
BLK = 256
DIM = 2048
HD = 128
NH = 4
HE = NH * HD
QKV = HE + 2 * HD
CH = 512
SC = CH // 2
WR = 1024
KC = 256
NX = 8
XR = BLK // NX
NB = SEQ // BLK
CAUSAL_ROWS = BLK * NB * (NB + 1) // 2

S_XY, S_XF, S_XC = 0, 8, 16
S_DY, S_DF, S_DC = 17, 22, 27
S_KP = 28
S_PX = 29
S_PY = 31
S_XN, S_XNC, S_XNF, S_XNG = 33, 36, 37, 40
S_A = 43
S_WO = 47
S_WQ = 95
S_KV = 119
S_XT, S_XU, S_XV = 131, 132, 133
N_SEM = 134
NT = 1
XT = XR // 2
VMEM_LIMIT = 63 * 2 ** 20 - 3328 * 1024


def nn(a, b):
    return lax.dot_general(a, b, (((1,), (0,)), ((), ())), preferred_element_type=F32)


def nt(a, b):
    return lax.dot_general(a, b, (((1,), (1,)), ((), ())), preferred_element_type=F32)


def step_kernel(x_in, dy_in, wq_in, wk_in, wv_in, wo_in, dxo, wqo, dko, dvo, woo,
                xg, dyg, wq8, wst, wqkv, wo, qkv, kt, vt, prob, pbuf, ot, dout, at, am, dkv, pw, pkv,
                kvs, kvr, so, ro, sq, rq, skv, rkv, sx, rx, sy, ry, xn, xta, xtb, abuf, ssem, rsem, lsem):
    pod = lax.axis_index("pod")
    z = lax.axis_index("data")
    m = lax.axis_index("model")
    y = m // 2
    c = m % 2
    core_m = 2 * y + 1 - c
    far_m = (m + 2) % 4
    diag_m = (core_m + 2) % 4
    core_dev = (pod, z, core_m)
    far_dev = (pod, z, far_m)

    inner = ((z + 1) // 2) % 2
    pair_dev = (pod, z + 1 - 2 * (z % 2), m)
    other_dev = (pod, 3 - z, m)
    x_off = CH * (1 - z // 2)

    def rows(block, n=BLK, off=0):
        return pl.ds(pl.multiple_of(block * BLK + off, n), n)

    def chunk(i):
        return i + (1 - z // 2) * (3 - 2 * i)

    def col(i):
        return pl.ds(pl.multiple_of(chunk(i) * CH, CH), CH)

    def dcol(i):
        if i < 2:
            return pl.ds(pl.multiple_of(chunk(0) * CH + i * SC, SC), SC)
        return col(i - 1)

    def remote(src, dst, sem, dev):
        return pltpu.make_async_remote_copy(src_ref=src, dst_ref=dst, send_sem=ssem.at[sem], recv_sem=rsem.at[sem],
                                            device_id=dev, device_id_type=MESH)

    def head_rows(h):
        return pl.ds(pl.multiple_of(h * HD, HD), HD)

    loads = [
        pltpu.make_async_copy(x_in.at[0], xg.at[rows(m)], lsem.at[0]),
        pltpu.make_async_copy(dy_in.at[0], dyg.at[rows(m)], lsem.at[1]),
        pltpu.make_async_copy(wk_in.at[y], wqkv.at[:, pl.ds(HE, HD)], lsem.at[2]),
        pltpu.make_async_copy(wv_in.at[y], wqkv.at[:, pl.ds(HE + HD, HD)], lsem.at[3]),
        pltpu.make_async_copy(wo_in, wo, lsem.at[4]),
    ]
    def wq_load(i):
        return pltpu.make_async_copy(wq_in.at[pl.ds(pl.multiple_of(i * WR, WR), WR)], wq8.at[i % 2], lsem.at[5 + i % 2])

    for ld in loads:
        ld.start()
    wq_load(0).start()
    wq_load(1).start()

    barrier = pltpu.get_barrier_semaphore()
    for dev in (far_dev, core_dev, pair_dev):
        pl.semaphore_signal(barrier, inc=1, device_id=dev, device_id_type=MESH)

    @pl.when(inner == 1)
    def _():
        pl.semaphore_signal(barrier, inc=1, device_id=other_dev, device_id_type=MESH)

    pl.semaphore_wait(barrier, 3 + inner)

    def x_far(i, block):
        r = rows(block, XR, i * XR)
        return remote(xg.at[r], xg.at[r], S_XY + i, far_dev)

    def x_fwd(i, block):
        r = rows(block, XR, i * XR)
        return remote(xg.at[r], xg.at[r], S_XF + i, core_dev)

    def x_core(block):
        return remote(xg.at[rows(block)], xg.at[rows(block)], S_XC, core_dev)

    def dy_far(i, block):
        return remote(dyg.at[rows(block), dcol(i)], dyg.at[rows(block), dcol(i)], S_DY + i, far_dev)

    def dy_fwd(i, block):
        return remote(dyg.at[rows(block), dcol(i)], dyg.at[rows(block), dcol(i)], S_DF + i, core_dev)

    def dy_core(block):
        return remote(dyg.at[rows(block)], dyg.at[rows(block)], S_DC, core_dev)

    def ncol(k):
        return pl.ds(pl.multiple_of(chunk(k) * CH - x_off, CH), CH)

    def xn_edge(k):
        return remote(xg.at[rows(m), col(k)], xn.at[rows(m), ncol(k)], S_XN + k, pair_dev)

    def xn_core(block):
        return remote(xn.at[rows(block)], xn.at[rows(block)], S_XNC, core_dev)

    def xn_far(k, block):
        return remote(xn.at[rows(block), ncol(k)], xn.at[rows(block), ncol(k)], S_XNF + k, far_dev)

    def xn_fwd(k, block):
        return remote(xn.at[rows(block), ncol(k)], xn.at[rows(block), ncol(k)], S_XNG + k, core_dev)

    def take_xn(k):
        xn_far(k, far_m).wait_recv()
        xn_fwd(k, far_m).start()

    def xt_edge(j):
        return remote(xg.at[rows(m, XT, (NX - 1) * XR + XT)], xta.at[pl.ds(j * XT, XT)], S_XT + j, pair_dev)

    def xt_far(j):
        return remote(xta.at[pl.ds(j * XT, XT)], xtb.at[pl.ds(j * XT, XT)], S_XU + j, far_dev)

    def xt_back():
        return remote(xtb, xg.at[rows(far_m, XT, (NX - 1) * XR + XT)], S_XV, pair_dev)

    def x_last(block):
        r = rows(block, XT, (NX - 1) * XR)
        return remote(xg.at[r], xg.at[r], S_XY + NX - 1, far_dev)

    loads[0].wait()
    for i in range(2):
        x_far(i, m).start()

    @pl.when(inner == 0)
    def _():
        for j in range(NT):
            xt_edge(j).start()
        for k in range(3):
            xn_edge(k).start()
        for i in range(2, NX - 1):
            x_far(i, m).start()
        x_last(m).start()

    x_core(m).start()
    loads[1].wait()

    @pl.when(inner == 0)
    def _():
        for i in range(5):
            dy_far(i, m).start()

    dy_core(m).start()
    for ld in loads[2:]:
        ld.wait()

    def wq_block(i, carry):
        wq_load(i).wait()
        wst[...] = wq8[i % 2].astype(F32)

        @pl.when(i + 2 < DIM * NH // WR)
        def _():
            wq_load(i + 2).start()

        for h in range(NH):
            wqkv[pl.ds(pl.multiple_of(i * (WR // NH), WR // NH), WR // NH), pl.ds(h * HD, HD)] = wst[pl.ds(h, WR // NH, stride=NH), :].astype(BF16)
        return carry

    lax.fori_loop(0, DIM * NH // WR, wq_block, 0)

    @pl.when(inner == 1)
    def _():
        for j in range(NT):
            xt_edge(j).wait_recv()
            xt_far(j).start()
        for i in range(2, NX):
            x_far(i, m).start()
        for i in range(5):
            dy_far(i, m).start()

    def project(r):
        qkv[r, :] = nn(xg[r, :], wqkv[...]).astype(BF16)

    def flip(block):
        r = rows(block)
        kt[:, r] = qkv[r, pl.ds(HE, HD)].T
        vt[:, r] = qkv[r, pl.ds(HE + HD, HD)].T

    project(rows(m))
    x_core(core_m).wait_recv()
    project(rows(core_m))
    flip(m)
    flip(core_m)

    @pl.when(inner == 1)
    def _():
        for j in range(NT):
            xt_far(j).wait_recv()
        xt_back().start()

    def x_piece(i, carry):
        split = (1 - inner) * (i // (NX - 1))

        @pl.when(split == 0)
        def _():
            x_far(i, far_m).wait_recv()

        @pl.when(split == 1)
        def _():
            x_last(far_m).wait_recv()
            xt_back().wait_recv()

        x_fwd(i, far_m).start()
        project(rows(far_m, XR, i * XR))
        x_fwd(i, diag_m).wait_recv()
        project(rows(diag_m, XR, i * XR))
        return carry

    lax.fori_loop(0, NX, x_piece, 0)

    flip(far_m)
    flip(diag_m)
    dy_core(core_m).wait_recv()

    def take_dy(i):
        dy_far(i, far_m).wait_recv()
        dy_fwd(i, far_m).start()

    def wo_sem(slot, s, h):
        return S_WO + slot * 8 + s * 4 + h

    def wo_edge(k, s, h):
        return remote(so.at[k, s, h], ro.at[k, s, h], wo_sem(k, s, h), pair_dev)

    def wo_swap(k, s, h):
        return remote(so.at[k, s, h], ro.at[3 + k, s, h], wo_sem(3 + k, s, h), other_dev)

    def wo_back(s, h):
        return remote(so.at[2, s, h], ro.at[3, s, h], wo_sem(5, s, h), pair_dev)

    def half_col(s):
        return pl.ds(s * SC, SC)

    def wo_pass(k, h):
        for s in range(2):
            wo_edge(k, s, h).wait_recv()
            so[k, s, h] = (pw[k, head_rows(h), half_col(s)] + ro[k, s, h].astype(F32)).astype(BF16)
            wo_swap(k, s, h).start()

    def wo_first(s, h):
        v = nn(ot[pl.ds(h * HD, HD), :], dyg[:, dcol(s)])

        @pl.when(inner == 0)
        def _():
            so[0, s, h] = v.astype(BF16)
            wo_edge(0, s, h).start()

        @pl.when(inner == 1)
        def _():
            pw[0, head_rows(h), half_col(s)] = v

    @pl.when(inner == 1)
    def _():
        for k in range(3):
            xn_edge(k).wait_recv()
            xn_far(k, m).start()
        xn_core(m).start()

    scale = HD ** -0.5
    exp_scale = scale * math.log2(math.e)
    diag_mask = lax.broadcasted_iota(jnp.int32, (BLK, BLK), 0) <= lax.broadcasted_iota(jnp.int32, (BLK, BLK), 1)

    def prow(qi, kj):
        return pl.ds(BLK * (qi * (qi + 1) // 2 + kj), BLK)

    def fwd_head(h, first_q, last_q):
        hr = pl.ds(h * HD, HD)
        for qi in range(first_q, last_q):
            qb = qkv[pl.ds(qi * BLK, BLK), hr]
            mx = None
            for kj in range(qi + 1):
                s = nt(qkv[pl.ds(kj * BLK, BLK), pl.ds(HE, HD)], qb)
                if kj == qi:
                    s = jnp.where(diag_mask, s, -jnp.inf)
                prob[h, prow(qi, kj), :] = s
                bm = jnp.max(s, axis=0, keepdims=True)
                mx = bm if mx is None else jnp.maximum(mx, bm)
            tot = None
            for kj in range(qi + 1):
                e = jnp.exp2((prob[h, prow(qi, kj), :] - mx) * exp_scale)
                prob[h, prow(qi, kj), :] = e
                bs = jnp.sum(e, axis=0, keepdims=True)
                tot = bs if tot is None else tot + bs
            inv = 1.0 / tot
            for kj in range(qi + 1):
                p = prob[h, prow(qi, kj), :] * inv
                prob[h, prow(qi, kj), :] = p
                pbuf[pl.ds(kj * BLK, BLK), :] = p.astype(BF16)
            n = (qi + 1) * BLK
            ot[hr, pl.ds(qi * BLK, BLK)] = nn(vt[:, pl.ds(0, n)], pbuf[pl.ds(0, n), :]).astype(BF16)

    fwd_head(0, 0, 3)
    take_dy(0)
    fwd_head(0, 3, NB)
    dy_fwd(0, diag_m).wait_recv()
    wo_first(0, 0)
    fwd_head(1, 0, 2)
    take_dy(1)
    fwd_head(1, 2, 3)
    dy_fwd(1, diag_m).wait_recv()
    wo_first(1, 0)
    fwd_head(1, 3, NB)
    wo_first(0, 1)
    wo_first(1, 1)
    for h in range(2, NH):
        fwd_head(h, 0, 3)
        if h == 3:
            take_dy(2)
        fwd_head(h, 3, NB)
        for s in range(2):
            wo_first(s, h)

        @pl.when(inner == 1)
        def _(h=h):
            wo_pass(0, h - 2)

    def wo_return(h):
        for s in range(2):
            wo_swap(0, s, h).wait_recv()
            so[2, s, h] = (pw[3, head_rows(h), half_col(s)] + ro[3, s, h].astype(F32)).astype(BF16)
            wo_back(s, h).start()

    def wo_send(k):
        for h in range(NH):
            for s in range(2):
                so[k, s, h] = pw[k, head_rows(h), half_col(s)].astype(BF16)
                wo_edge(k, s, h).start()

    for i in range(1, 4):
        if i > 1:
            take_dy(i + 1)
        dy_fwd(i + 1, diag_m).wait_recv()
        pw[i] = nn(ot[...], dyg[:, col(i)])
        if i < 3:
            if i == 1:
                @pl.when(inner == 0)
                def _():
                    wo_send(1)

            @pl.when(inner == 1)
            def _(i=i):
                wo_pass(0, i + 1)

    def a_copy(h):
        r = head_rows(h)
        return remote(at.at[r], abuf.at[r], S_A + h, pair_dev)

    def wq_swap(k, s, h):
        return remote(sq.at[k, s, h], rq.at[k, s, h], S_WQ + k * 8 + s * 4 + h, other_dev)

    def wq_back(s, h):
        return remote(sq.at[2, s, h], rq.at[2, s, h], S_WQ + 16 + s * 4 + h, pair_dev)

    def spot(k, s, h=0, n=1):
        return prob.at[1 + k // 2, pl.ds(((k % 2) * 2 + s) * HE + h * HD, n * HD)]

    def wq_own(k, q):
        v = nn(at[pl.ds(0, HE), :], xg[:, pl.ds(pl.multiple_of(q * CH, CH), CH)])
        for s in range(2):
            spot(k, s, 0, NH)[...] = v[:, s * SC:(s + 1) * SC]

    def combine(h, ks=(0, 1)):
        if 0 in ks:
            a_copy(h).wait_recv()
        for k in ks:
            v = nn(abuf[head_rows(h), :], xn[:, ncol(k)])
            for s in range(2):
                sq[k, s, h] = (spot(k, s, h)[...] + v[:, s * SC:(s + 1) * SC]).astype(BF16)
                wq_swap(k, s, h).start()

    def outer(h):
        for s in range(2):
            wq_swap(0, s, h).wait_recv()
            sq[2, s, h] = (spot(3, s, h)[...] + rq[0, s, h].astype(F32)).astype(BF16)
            wq_back(s, h).start()

    def dout_block(b, carry):
        r = rows(b)
        dout[r, :] = nt(dyg[r, :], wo[...]).astype(BF16)
        return carry

    lax.fori_loop(0, NB, dout_block, 0)

    dkv[...] = jnp.zeros_like(dkv)

    def bwd_head(h, carry):
        hr = head_rows(h)
        for qi in range(NB):
            qr = pl.ds(qi * BLK, BLK)
            dob = dout[qr, hr]
            qb = qkv[qr, hr]
            delta = jnp.sum(dob.astype(F32).T * ot[hr, qr].astype(F32), axis=0, keepdims=True)
            for kj in range(qi + 1):
                kr = pl.ds(kj * BLK, BLK)
                p = prob[h, prow(qi, kj), :]
                dp = nt(qkv[kr, pl.ds(HE + HD, HD)], dob)
                ds = (p * (dp - delta)).astype(BF16)
                pbuf[kr, :] = ds
                dkv[kr, pl.ds(0, HD)] += nn(ds, qb)
                dkv[kr, pl.ds(HD, HD)] += nn(p.astype(BF16), dob)
            n = (qi + 1) * BLK
            dq = (nn(kt[:, pl.ds(0, n)], pbuf[pl.ds(0, n), :]) * scale).astype(BF16)
            at[hr, qr] = dq
            am[qr, hr] = dq.T

        @pl.when(inner == 0)
        def _():
            a_copy(h).start()

        @pl.when(inner == 1)
        def _():
            wo_pass(1, h)
            wo_return(h)

            @pl.when(h == 2)
            def _():
                take_xn(0)

        return carry

    lax.fori_loop(0, NH, bwd_head, 0)

    @pl.when(inner == 1)
    def _():
        take_xn(1)
        wq_own(0, chunk(0))
        xn_core(core_m).wait_recv()
        xn_fwd(0, diag_m).wait_recv()
        combine(0, (0,))
        combine(1, (0,))

    dkb = (dkv[:, pl.ds(0, HD)] * scale).astype(BF16)
    dvb = dkv[:, pl.ds(HD, HD)].astype(BF16)
    am[:, pl.ds(HE, HD)] = dkb
    am[:, pl.ds(HE + HD, HD)] = dvb
    at[pl.ds(HE, HD), :] = dkb.T
    at[pl.ds(HE + HD, HD), :] = dvb.T

    def dx_part(block, put):
        def piece(i, carry):
            cs = pl.ds(pl.multiple_of(i * CH, CH), CH)
            put(i, cs, nt(am[rows(block), :], wqkv[cs, :]))
            return carry

        lax.fori_loop(0, DIM // CH, piece, 0)

    def px_copy(i):
        return remote(sx.at[i], rx.at[i], S_PX + i, core_dev)

    def py_copy(i):
        r = pl.ds(i * (BLK // 2), BLK // 2)
        return remote(sy.at[r], ry.at[r], S_PY + i, far_dev)

    def put_sx(j):
        def put(i, cs, v):
            sx[j, :, cs] = v.astype(BF16)
        return put

    def pxo(i, s):
        return prob.at[0, pl.ds(pl.multiple_of((2 * i + s) * BLK, BLK), BLK)]

    def put_own(i, cs, v):
        for s in range(2):
            pxo(i, s)[...] = v[:, s * SC:(s + 1) * SC]

    half = DIM // 2

    def kv_half(which):
        return nn(at[pl.ds(HE, 2 * HD), :], xg[:, pl.ds(pl.multiple_of(which * half, half), half)])

    def kcol(k):
        return pl.ds(pl.multiple_of(chunk(k) * KC, KC), KC)

    def kv_part(ref, slot, t):
        return ref.at[slot, pl.ds(t * HD, HD)]

    def kv_edge(k, t):
        return remote(kv_part(skv, k, t), kv_part(rkv, k, t), S_KV + 2 * k + t, pair_dev)

    def kv_swap(k, t):
        return remote(kv_part(skv, k, t), kv_part(rkv, 3 + k, t), S_KV + 2 * (3 + k) + t, other_dev)

    def kv_back(t):
        return remote(kv_part(skv, 2, t), kv_part(rkv, 3, t), S_KV + 10 + t, pair_dev)

    def kv_own(k, t):
        return pkv[pl.ds(t * HD, HD), kcol(k)]

    def kv_pass(k):
        for t in range(2):
            kv_edge(k, t).wait_recv()
            kv_part(skv, k, t)[...] = (kv_own(k, t) + kv_part(rkv, k, t)[...].astype(F32)).astype(BF16)
            kv_swap(k, t).start()

    dx_part(diag_m, put_sx(0))
    px_copy(0).start()
    dx_part(far_m, put_own)
    px_copy(0).wait_recv()
    for i in range(2):
        r = pl.ds(i * (BLK // 2), BLK // 2)
        for j in range(DIM // SC):
            cs = pl.ds(j * SC, SC)
            own = prob[0, pl.ds(j * BLK + i * (BLK // 2), BLK // 2), :]
            sy[r, cs] = (own + rx[0, r, cs].astype(F32)).astype(BF16)
        py_copy(i).start()

    @pl.when(inner == 1)
    def _():
        wq_own(1, chunk(1))
        xn_fwd(1, diag_m).wait_recv()
        combine(0, (1,))
        combine(1, (1,))

    kvs[...] = kv_half(1 - c).astype(BF16)
    kp_copy = remote(kvs, kvr, S_KP, core_dev)
    kp_copy.start()
    pkv[...] = kv_half(c)
    kp_copy.wait_recv()
    pkv[...] += kvr[...].astype(F32)

    @pl.when(inner == 0)
    def _():
        for k in range(3):
            for t in range(2):
                kv_part(skv, k, t)[...] = kv_own(k, t).astype(BF16)
                kv_edge(k, t).start()
        wo_send(2)
    @pl.when(inner == 1)
    def _():
        combine(2)
        take_xn(2)
        wq_own(3, chunk(3))
        outer(0)
        outer(1)

    dx_part(core_m, put_sx(1))
    px_copy(1).start()
    dx_part(m, put_own)
    wq_own(2, z)

    @pl.when(inner == 1)
    def _():
        combine(3, (0,))
        outer(2)
        kv_pass(0)
        combine(3, (1,))
        xn_fwd(2, diag_m).wait_recv()
        v = nn(abuf[...], xn[:, ncol(2)])
        for s in range(2):
            spot(2, s, 0, NH)[...] += v[:, s * SC:(s + 1) * SC]
        kv_pass(1)
        outer(3)
        for t in range(2):
            kv_swap(0, t).wait_recv()
            kv_part(skv, 2, t)[...] = (kv_own(3, t) + kv_part(rkv, 3, t)[...].astype(F32)).astype(BF16)
            kv_back(t).start()

    @pl.when(inner == 0)
    def _():
        for h in range(NH):
            for s in range(2):
                wo_back(s, h).wait_recv()
                woo[head_rows(h), half_col(s)] = pw[3, head_rows(h), half_col(s)] + ro[3, s, h].astype(F32)

    px_copy(1).wait_recv()
    for i in range(2):
        r = pl.ds(i * (BLK // 2), BLK // 2)
        py_copy(i).wait_recv()
        for j in range(DIM // SC):
            cs = pl.ds(j * SC, SC)
            own = prob[0, pl.ds(j * BLK + i * (BLK // 2), BLK // 2), :]
            dxo[r, cs] = (own + rx[1, r, cs].astype(F32) + ry[r, cs].astype(F32)).astype(BF16)

    def wq_put(h, s, got):
        wqo[pl.ds(s * SC * NH + h, SC, stride=NH), :] = (spot(2, s, h)[...] + got.astype(F32)).T

    kv_out = (dko, dvo)

    @pl.when(inner == 1)
    def _():
        for h in range(NH):
            for s in range(2):
                wq_swap(1, s, h).wait_recv()
                wq_put(h, s, rq[1, s, h])
        for t in range(2):
            kv_edge(2, t).wait_recv()
            kv_swap(1, t).wait_recv()
            kv_out[t][...] = (kv_own(2, t) + kv_part(rkv, 2, t)[...].astype(F32) + kv_part(rkv, 4, t)[...].astype(F32)).T
        for h in range(NH):
            for s in range(2):
                wo_edge(2, s, h).wait_recv()
                wo_swap(1, s, h).wait_recv()
                woo[head_rows(h), half_col(s)] = pw[2, head_rows(h), half_col(s)] + ro[2, s, h].astype(F32) + ro[4, s, h].astype(F32)

    @pl.when(inner == 0)
    def _():
        for h in range(NH):
            for s in range(2):
                wq_back(s, h).wait_recv()
                wq_put(h, s, rq[2, s, h])
        for t in range(2):
            kv_back(t).wait_recv()
            kv_out[t][...] = (kv_own(3, t) + kv_part(rkv, 3, t)[...].astype(F32)).T

    for i in range(NX - 1):
        x_far(i, m).wait_send()
    for i in range(NX):
        x_fwd(i, far_m).wait_send()
    x_core(m).wait_send()
    for i in range(5):
        dy_far(i, m).wait_send()
        dy_fwd(i, far_m).wait_send()
    dy_core(m).wait_send()
    @pl.when(inner == 0)
    def _():
        x_last(m).wait_send()
        for j in range(NT):
            xt_edge(j).wait_send()
        for k in range(3):
            xn_edge(k).wait_send()
        for h in range(NH):
            a_copy(h).wait_send()
        for k in range(3):
            for t in range(2):
                kv_edge(k, t).wait_send()
            for s in range(2):
                for h in range(NH):
                    wo_edge(k, s, h).wait_send()

    @pl.when(inner == 1)
    def _():
        x_far(NX - 1, m).wait_send()
        for j in range(NT):
            xt_far(j).wait_send()
        xt_back().wait_send()
        xn_core(m).wait_send()
        for k in range(3):
            xn_far(k, m).wait_send()
            xn_fwd(k, far_m).wait_send()
        for t in range(2):
            for k in range(2):
                kv_swap(k, t).wait_send()
            kv_back(t).wait_send()
        for s in range(2):
            for h in range(NH):
                for k in range(2):
                    wo_swap(k, s, h).wait_send()
                    wq_swap(k, s, h).wait_send()
                wo_back(s, h).wait_send()
                wq_back(s, h).wait_send()

    kp_copy.wait_send()
    for i in range(2):
        px_copy(i).wait_send()
        py_copy(i).wait_send()


def store_kernel(*refs):
    n = len(refs) // 2
    sem = refs[-1]
    copies = [pltpu.make_async_copy(refs[i], refs[n + i], sem.at[i]) for i in range(n)]
    for cp in copies:
        cp.start()
    for cp in copies:
        cp.wait()


def solution(mesh):
    tok_spec = P(('pod', 'data'), 'model', None)

    def device_step(x_loc, dy_loc, w_q, w_k, w_v, w_o):
        any_spec = pl.BlockSpec(memory_space=pl.ANY)
        vmem_spec = pl.BlockSpec(memory_space=pltpu.VMEM)
        outs = (((BLK, DIM), BF16), ((CH * NH, HD), F32), ((KC, HD), F32), ((KC, HD), F32), ((HE, CH), F32))
        dx, dwq, dwk, dwv, dwo = pl.pallas_call(
            step_kernel,
            out_shape=tuple(pltpu.VMEM(shape, dtype) for shape, dtype in outs),
            in_specs=[any_spec] * 6,
            out_specs=[vmem_spec] * 5,
            scratch_shapes=[
                pltpu.VMEM((SEQ, DIM), BF16),
                pltpu.VMEM((SEQ, DIM), BF16),
                pltpu.VMEM((2, WR, HD), BF16),
                pltpu.VMEM((WR, HD), F32),
                pltpu.VMEM((DIM, QKV), BF16),
                pltpu.VMEM((HE, DIM), BF16),
                pltpu.VMEM((SEQ, QKV), BF16),
                pltpu.VMEM((HD, SEQ), BF16),
                pltpu.VMEM((HD, SEQ), BF16),
                pltpu.VMEM((NH, CAUSAL_ROWS, BLK), F32),
                pltpu.VMEM((SEQ, BLK), BF16),
                pltpu.VMEM((HE, SEQ), BF16),
                pltpu.VMEM((SEQ, HE), BF16),
                pltpu.VMEM((QKV, SEQ), BF16),
                pltpu.VMEM((SEQ, QKV), BF16),
                pltpu.VMEM((SEQ, 2 * HD), F32),
                pltpu.VMEM((4, HE, CH), F32),
                pltpu.VMEM((2 * HD, DIM // 2), F32),
                pltpu.VMEM((2 * HD, DIM // 2), BF16),
                pltpu.VMEM((2 * HD, DIM // 2), BF16),
                pltpu.VMEM((3, 2, NH, HD, SC), BF16),
                pltpu.VMEM((5, 2, NH, HD, SC), BF16),
                pltpu.VMEM((3, 2, NH, HD, SC), BF16),
                pltpu.VMEM((3, 2, NH, HD, SC), BF16),
                pltpu.VMEM((3, 2 * HD, KC), BF16),
                pltpu.VMEM((5, 2 * HD, KC), BF16),
                pltpu.VMEM((2, BLK, DIM), BF16),
                pltpu.VMEM((2, BLK, DIM), BF16),
                pltpu.VMEM((BLK, DIM), BF16),
                pltpu.VMEM((BLK, DIM), BF16),
                pltpu.VMEM((SEQ, 3 * CH), BF16),
                pltpu.VMEM((XT, DIM), BF16),
                pltpu.VMEM((XT, DIM), BF16),
                pltpu.VMEM((HE, SEQ), BF16),
                pltpu.SemaphoreType.DMA((N_SEM,)),
                pltpu.SemaphoreType.DMA((N_SEM,)),
                pltpu.SemaphoreType.DMA((7,)),
            ],
            compiler_params=pltpu.CompilerParams(collective_id=0, has_side_effects=True, vmem_limit_bytes=VMEM_LIMIT),
        )(x_loc, dy_loc, w_q.reshape(DIM * NH, HD), w_k, w_v, w_o.reshape(HE, DIM))
        dx, dwq, dwk, dwv, dwo = pl.pallas_call(
            store_kernel,
            out_shape=tuple(jax.ShapeDtypeStruct(shape, dtype) for shape, dtype in outs),
            in_specs=[any_spec] * 5,
            out_specs=[any_spec] * 5,
            scratch_shapes=[pltpu.SemaphoreType.DMA((5,))],
            compiler_params=pltpu.CompilerParams(vmem_limit_bytes=2 ** 20),
        )(dx, dwq, dwk, dwv, dwo)
        return dx.reshape(1, BLK, DIM), dwq.reshape(CH, NH, HD), dwk, dwv, dwo.reshape(NH, HD, CH)

    kv_rows = P(('pod', 'model', 'data'), None)
    return jax.shard_map(device_step, mesh=mesh,
                         in_specs=(tok_spec, tok_spec, P(None, 'model', None), P(), P(), P('model', None, None)),
                         out_specs=(tok_spec, P(('pod', 'data'), 'model', None), kv_rows, kv_rows, P(('pod', 'model'), None, 'data')),
                         check_vma=False)
```
